32 devices in a mesh: grp: 8 (over z, core), sub: 4 (over y, x).
Axes of the slice: x: 2, y: 2, z: 4, core: 2. Of those that a mesh axis runs over, the one named last changes fastest.
Arguments:
- coarse_op: float32 [256, 64, 576], P(('grp', 'sub'))
- right_side: float32 [256, 64, 64], P(('grp', 'sub')), may hold values from -6 to 6
- owner_map: int32 [256], replicated, may hold values from 0 to 255, as said below
- neighbor_table: int32 [256, 8], replicated, may hold values from 0 to 255, as said below
Outputs:
- solution: float32 [256, 64, 64], P(('grp', 'sub'))
The draws below stay inside these ranges and needn't reach their ends.
Inputs may be any that keep to these rules, and one draw needn't show every extreme that they name: `owner_map`: a permutation of 0 .. 255. `neighbor_table`: row t lists the neighbours of coarse site t on a periodic 4^4 lattice in the order +x, -x, +y, -y, +z, -z, +t, -t; lattice positions carry the site numbers in a permuted order.
All inputs are finite; a program needn't handle non-finite values.
Results may differ from the reference program's by a relative error of at most 0.0001.
Values sent between devices are 32-bit elements; how exact they have to be, the bound alone decides.
No kernel may reach another device: no remote copies, remote signals or barrier semaphores. Data moves between devices by JAX's collectives and lax.ppermute only.
A program may use at most 64 MiB of HBM per device.

```python
import jax
import jax.numpy as jnp
from jax import lax

LAT = 4
DOF = 64
RHS = 64
ITERS = 3
HOPS = 8
SITES = 256


def draw_coarse_op(key, part):
    noise_key = jax.random.fold_in(key, 11)
    diag_key = jax.random.fold_in(key, 12)
    spread = 0.6 / (9.0 * DOF) ** 0.5
    noise = jax.random.normal(noise_key, (SITES, DOF, 9 * DOF), jnp.float32) * spread
    diag = jnp.exp(jax.random.uniform(diag_key, (SITES, DOF), jnp.float32, 0.0, 1.0986123))
    unit = jnp.eye(DOF, 9 * DOF, dtype=jnp.float32)
    return noise + diag[:, :, None] * unit[None]


def draw_owner_map(key, part):
    return jax.random.permutation(jax.random.fold_in(key, 21), SITES).astype(jnp.int32)


def draw_neighbor_table(key, part):
    relabel = jax.random.permutation(jax.random.fold_in(key, 31), SITES).astype(jnp.int32)
    position = jnp.arange(SITES, dtype=jnp.int32)
    columns = []
    for axis_dim in range(4):
        stride = LAT ** axis_dim
        coord = position // stride % LAT
        for offset in (1, -1):
            moved = position + ((coord + offset) % LAT - coord) * stride
            columns.append(relabel[moved])
    table = jnp.stack(columns, axis=1).astype(jnp.int32)
    return jnp.zeros((SITES, HOPS), jnp.int32).at[relabel].set(table)


def shard_levels(rng, dims, split, smallest, high):
    level, own = 1.0, jax.random.fold_in(rng, 6)
    for dim, shards_of in split:
        heights = jnp.exp(jax.random.uniform(jax.random.fold_in(own, dim), (shards_of,), jnp.float32, smallest / len(split), high / len(split)))
        level = level * jnp.repeat(heights, dims[dim] // shards_of).reshape([-1 if axis == dim else 1 for axis in range(len(dims))])
    return level


def gaussian(stream_key, dims, scale, limit, shards=(), held_as=jnp.bfloat16):
    array = scale * jax.random.normal(stream_key, dims, jnp.float32)
    if shards:
        array = array * shard_levels(stream_key, dims, shards, -0.22, 0.18)
    return jnp.clip(array, -limit, limit).astype(held_as)


def setup_inputs(seed: int = 0) -> dict:
    key_of = jax.random.split(jax.random.key(seed), 5)
    return {
        "coarse_op": draw_coarse_op(jax.random.fold_in(key_of[4], 71), 0),
        "right_side": gaussian(key_of[1], (SITES, DOF, RHS), 1.0, 6.0, ((0, 32),), jnp.float32),
        "owner_map": draw_owner_map(jax.random.fold_in(key_of[4], 71), 0),
        "neighbor_table": draw_neighbor_table(jax.random.fold_in(key_of[4], 71), 0),
    }


def inner_product(first, second):
    return lax.optimization_barrier(jnp.sum(first * second, axis=(0, 1)))

def reference(coarse_op, right_side, owner_map, neighbor_table):
    site_ids = jnp.arange(SITES, dtype=jnp.int32)
    inverse = lax.optimization_barrier(jnp.sum(jnp.where(owner_map[None, :] == site_ids[:, None], site_ids[None, :], 0), axis=1)).astype(jnp.int32)
    link = inverse[neighbor_table[owner_map]]

    def apply_op(vector):
        stacked = jnp.concatenate([vector[:, None], vector[link]], axis=1).reshape(SITES, 9 * DOF, RHS)
        return jnp.einsum('sac,scr->sar', coarse_op, stacked, precision=lax.Precision.HIGHEST)
    beta = jnp.sqrt(inner_product(right_side, right_side))
    krylov = [right_side / beta]
    hess = jnp.zeros((ITERS + 1, ITERS, RHS), jnp.float32)
    for column in range(ITERS):
        image = apply_op(krylov[column])
        coeffs = [inner_product(vector, image) for vector in krylov]
        for index_i in range(column + 1):
            image = image - coeffs[index_i] * krylov[index_i]
            hess = hess.at[index_i, column].set(coeffs[index_i])
        norm_value = jnp.sqrt(inner_product(image, image))
        hess = hess.at[column + 1, column].set(norm_value)
        krylov.append(image / norm_value)
    gram_matrix = jnp.einsum('ijr,ikr->rjk', hess, hess, precision=lax.Precision.HIGHEST)
    projected = (beta[None, :] * hess[0]).T
    weights = jnp.linalg.solve(gram_matrix, projected[..., None])[..., 0]
    solution = jnp.zeros_like(right_side)
    for column in range(ITERS):
        solution = solution + weights[:, column][None, None, :] * krylov[column]
    return solution
```

```python
import functools

import jax
import jax.numpy as jnp
from jax import lax
from jax.experimental import pallas as pl
from jax.experimental.pallas import tpu as pltpu
from jax.sharding import Mesh
from jax.sharding import PartitionSpec as P

F32 = jnp.float32
BF16 = jnp.bfloat16
CORES = 2
VMEM = pl.BlockSpec(memory_space=pltpu.VMEM)
SMEM = pl.BlockSpec(memory_space=pltpu.SMEM)
ANY = pl.BlockSpec(memory_space=pl.ANY)
PARAMS = pltpu.CompilerParams(vmem_limit_bytes=56 * 1024 * 1024)


def low_half(shape, dof):
    return lax.broadcasted_iota(jnp.int32, shape, 1) < dof


def lane_sum(values):
    return jnp.sum(values, axis=1, keepdims=True)


def split_bf16(values):
    high = values.astype(BF16)
    return high, (values - high.astype(F32)).astype(BF16)


def place(columns, shape):
    lane = lax.broadcasted_iota(jnp.int32, shape, 1)
    packed = jnp.zeros(shape, F32)
    for index, column in enumerate(columns):
        packed = jnp.where(lane == index, column, packed)
    return packed


def position_kernel(geometry, ids, owner, table, out, where):
    per_dev, n_sub, nz, hops = geometry
    me_z, me_c, me_s = ids[0], ids[1], ids[2]
    sites = owner.shape[0]

    def locate(slot):
        dev = slot // per_dev
        grp = dev // n_sub
        block = ((grp % CORES) ^ me_c) * nz + grp // CORES
        return (block * n_sub + ((dev % n_sub) ^ me_s)) * per_dev + slot % per_dev

    def fill(slot, carry):
        where[owner[slot]] = locate(slot)
        return carry

    lax.fori_loop(0, sites, fill, 0, unroll=8)

    def look(local, carry):
        dev = (me_z * CORES + me_c) * n_sub + ((local // per_dev) ^ me_s)
        slot = dev * per_dev + local % per_dev
        base = owner[slot] * hops
        out[local * (hops + 1)] = locate(slot)
        for hop in range(hops):
            out[local * (hops + 1) + 1 + hop] = where[table[base + hop]]
        return carry

    lax.fori_loop(0, n_sub * per_dev, look, 0, unroll=2)


def spread(dup, pair, values, dof):
    mask = low_half(values.shape, dof)
    rolled = pltpu.roll(values, dof, 1)
    dup[2 * pair] = jnp.where(mask, values, rolled)
    dup[2 * pair + 1] = jnp.where(mask, rolled, values)


def site_product(op, local, pos, dup, terms, dof):
    rows = dup.shape[1]
    mask = low_half((rows, 2 * dof), dof)
    tiles = []
    for first in range(0, terms - 1, 2):
        left = dup[pos[local * terms + first]]
        right = dup[pos[local * terms + first + 1]]
        tiles.append(jnp.where(mask, left, right))
    if terms % 2:
        tiles.append(dup[pos[local * terms + terms - 1]][:, :dof])
    high, low = split_bf16(jnp.concatenate(tiles, axis=1))
    op_high, op_low = split_bf16(op)
    product = lax.dot_general(
        jnp.concatenate([high, low], axis=0),
        jnp.concatenate([op_high, op_low], axis=0),
        (((1,), (1,)), ((), ())),
        preferred_element_type=F32,
    )
    total = product[:rows] + product[rows:]
    return total + pltpu.roll(total, dof, 1)


def apply_rows(ops, pos, dup, terms, dof, put):
    per_part = ops[0].shape[0]
    rows = dup.shape[1]
    mask = low_half((rows, 2 * dof), dof)
    if per_part % 2:
        for pair in range(len(ops) * per_part // 2):
            halves = [
                site_product(ops[i // per_part][i % per_part], i, pos, dup, terms, dof)
                for i in (2 * pair, 2 * pair + 1)
            ]
            put(pair, jnp.where(mask, halves[0], halves[1]))
        return
    base = 0
    for op in ops:

        def body(inner, carry, base=base, op=op):
            first = base + 2 * inner
            even = site_product(op[2 * inner], first, pos, dup, terms, dof)
            odd = site_product(op[2 * inner + 1], first + 1, pos, dup, terms, dof)
            put(base // 2 + inner, jnp.where(mask, even, odd))
            return carry

        lax.fori_loop(0, op.shape[0] // 2, body, 0, unroll=True)
        base += op.shape[0]


def start_copies(sources, targets, sems):
    copies = [
        pltpu.make_async_copy(source, target, sems.at[index])
        for index, (source, target) in enumerate(zip(sources, targets))
    ]
    for copy in copies:
        copy.start()
    return copies


def over_pairs(fields, step, init):
    n_pair = fields[0].shape[0]
    for half in range(2):
        init = lax.fori_loop(
            0, n_pair, lambda pair, carry, half=half: step(half, pair, carry), init, unroll=8
        )
    return init


def first_kernel(count, dof, terms, pos, own, par, *rest):
    ops, out = rest[:count], rest[count]
    held, sems, dup = rest[count + 1 : 2 * count + 1], rest[2 * count + 1], rest[2 * count + 2]
    copies = start_copies(ops, held, sems)
    n_pair = own.shape[0]
    fields = (own, par)

    def build(half, pair, carry):
        spread(dup, half * n_pair + pair, fields[half][pair], dof)
        return carry

    over_pairs(fields, build, 0)
    for copy in copies:
        copy.wait()

    def put(pair, values):
        for block in range(out.shape[0]):
            out[block, pair] = values

    apply_rows(held, pos, dup, terms, dof, put)


def second_kernel(count, dof, terms, ids, pos, b_own, b_par, z_own, z_par, *rest):
    ops, (out, basis, mine, coeffs) = rest[:count], rest[count : count + 4]
    rest = rest[count + 4 :]
    held, sems, dup = rest[:count], rest[count], rest[count + 1]
    copies = start_copies(ops, held, sems)
    n_pair = b_own.shape[0]
    b_ref, z_ref = (b_own, b_par), (z_own, z_par)
    shape = b_own.shape[1:]
    zero = jnp.zeros(shape, F32)

    def dots(half, pair, carry):
        b, z = b_ref[half][pair], z_ref[half][pair]
        return carry[0] + b * b, carry[1] + b * z

    norm, cross = over_pairs(b_ref, dots, (zero, zero))
    beta_sq = lane_sum(norm)
    beta = jnp.sqrt(beta_sq)
    scale = 1.0 / beta
    h00 = lane_sum(cross) * scale * scale

    def remove(half, pair, carry):
        w = z_ref[half][pair] * scale - (h00 * scale) * b_ref[half][pair]
        basis[half * n_pair + pair] = w
        return carry + w * w

    h10 = jnp.sqrt(lane_sum(over_pairs(b_ref, remove, zero)))
    unit = 1.0 / h10

    def build(half, pair, carry):
        v = basis[half * n_pair + pair] * unit
        basis[half * n_pair + pair] = v
        spread(dup, half * n_pair + pair, v, dof)
        return carry

    over_pairs(b_ref, build, 0)
    coeffs[...] = place([beta, h00, h10], shape)
    n_mine = mine.shape[0]
    mine[...] = basis[pl.ds(ids[0] * n_mine, n_mine)]
    for copy in copies:
        copy.wait()

    def put(pair, values):
        for block in range(out.shape[0]):
            out[block, pair] = values

    apply_rows(held, pos, dup, terms, dof, put)


def third_kernel(
    count, dof, terms, ids, pos, b_own, b_par, basis, z_own, z_par, b_mine, v1_mine, coeffs, *rest
):
    ops, (sums, mine, coeffs_out) = rest[:count], rest[count : count + 3]
    rest = rest[count + 3 :]
    held, sems, dup, work, image = (
        rest[:count],
        rest[count],
        rest[count + 1],
        rest[count + 2],
        rest[count + 3],
    )
    copies = start_copies(ops, held, sems)
    n_pair = b_own.shape[0]
    b_ref, z_ref = (b_own, b_par), (z_own, z_par)
    shape = b_own.shape[1:]
    zero = jnp.zeros(shape, F32)
    known = coeffs[...]
    scale = 1.0 / known[:, 0:1]

    def dots(half, pair, carry):
        z = z_ref[half][pair]
        return carry[0] + b_ref[half][pair] * z, carry[1] + basis[half * n_pair + pair] * z

    first, second = over_pairs(b_ref, dots, (zero, zero))
    h01 = lane_sum(first) * scale
    h11 = lane_sum(second)

    def remove(half, pair, carry):
        w = (
            z_ref[half][pair]
            - (h01 * scale) * b_ref[half][pair]
            - h11 * basis[half * n_pair + pair]
        )
        work[half * n_pair + pair] = w
        return carry + w * w

    h21 = jnp.sqrt(lane_sum(over_pairs(b_ref, remove, zero)))
    unit = 1.0 / h21

    def build(half, pair, carry):
        v = work[half * n_pair + pair] * unit
        work[half * n_pair + pair] = v
        spread(dup, half * n_pair + pair, v, dof)
        return carry

    over_pairs(b_ref, build, 0)
    n_mine = mine.shape[0]
    mine[...] = work[pl.ds(ids[0] * n_mine, n_mine)]
    for copy in copies:
        copy.wait()

    def put(pair, values):
        image[pair] = values

    apply_rows(held, pos, dup, terms, dof, put)

    def last(pair, carry):
        u = image[pair]
        return (
            carry[0] + b_mine[pair] * u,
            carry[1] + v1_mine[pair] * u,
            carry[2] + mine[pair] * u,
            carry[3] + u * u,
        )

    parts = lax.fori_loop(0, n_mine, last, (zero, zero, zero, zero), unroll=True)
    packed = place([lane_sum(part) for part in parts], shape)
    for block in range(sums.shape[0]):
        sums[block] = packed
    lane = lax.broadcasted_iota(jnp.int32, shape, 1)
    merged = jnp.where(lane == 3, h01, known)
    merged = jnp.where(lane == 4, h11, merged)
    coeffs_out[...] = jnp.where(lane == 5, h21, merged)


def combine_kernel(ids, sums, coeffs, b_mine, v1_mine, v2_mine, out):
    total = sums[0]
    for block in range(1, sums.shape[0]):
        total = total + sums[block]
    known = coeffs[...]
    beta, h00, h10 = known[:, 0:1], known[:, 1:2], known[:, 2:3]
    h01, h11, h21 = known[:, 3:4], known[:, 4:5], known[:, 5:6]
    scale = 1.0 / beta
    h02, h12, h22, g22 = total[:, 0:1] * scale, total[:, 1:2], total[:, 2:3], total[:, 3:4]
    g00 = h00 * h00 + h10 * h10
    g01 = h00 * h01 + h10 * h11
    g02 = h00 * h02 + h10 * h12
    g11 = h01 * h01 + h11 * h11 + h21 * h21
    g12 = h01 * h02 + h11 * h12 + h21 * h22
    l10 = g01 / g00
    l20 = g02 / g00
    d1 = g11 - l10 * g01
    e21 = g12 - l20 * g01
    l21 = e21 / d1
    d2 = g22 - l20 * g02 - l21 * e21
    r0 = beta * h00
    r1 = beta * h01 - l10 * r0
    r2 = beta * h02 - l20 * r0 - l21 * r1
    y2 = r2 / d2
    y1 = r1 / d1 - l21 * y2
    y0 = r0 / g00 - l10 * y1 - l20 * y2
    c0 = y0 * scale
    parts, per_part = out.shape[0], out.shape[1]
    for part in range(parts):
        target = part ^ ids[2]
        for inner in range(per_part):
            pair = part * per_part + inner
            out[target, inner] = c0 * b_mine[pair] + y1 * v1_mine[pair] + y2 * v2_mine[pair]


def finish_kernel(dof, parts, out):
    for pair in range(parts.shape[1]):
        stacked = jnp.concatenate([parts[q, pair] for q in range(parts.shape[0])], axis=0)
        turned = stacked.T
        out[2 * pair] = turned[:dof]
        out[2 * pair + 1] = turned[dof:]


def per_device(coarse_op, right_side, owner_map, neighbor_table):
    nz = lax.axis_size("z")
    n_sub = lax.axis_size("sub")
    per_dev, dof, width = coarse_op.shape
    terms = width // dof
    hops = terms - 1
    rhs = right_side.shape[2] // n_sub
    n_loc = n_sub * per_dev
    n_own = n_loc // 2
    me_z, me_c, me_s = lax.axis_index("z"), lax.axis_index("core"), lax.axis_index("sub")
    ids = jnp.stack([me_z, me_c, me_s]).astype(jnp.int32)
    even = per_dev % 2 == 0
    lanes = 2 * dof
    field = (n_own, rhs, lanes)

    if n_sub == 4:
        hop_x = [(s, s ^ 1) for s in range(n_sub)]
        hop_y = [(s, s ^ 2) for s in range(n_sub)]
        op_x = lax.ppermute(coarse_op, "sub", hop_x)
        op_y = lax.ppermute(coarse_op, "sub", hop_y)
    order = jnp.arange(n_sub, dtype=jnp.int32) ^ me_s

    positions = pl.pallas_call(
        functools.partial(position_kernel, (per_dev, n_sub, nz, hops)),
        out_shape=jax.ShapeDtypeStruct((n_loc * terms,), jnp.int32),
        in_specs=[SMEM, SMEM, SMEM],
        out_specs=SMEM,
        scratch_shapes=[pltpu.SMEM((owner_map.shape[0],), jnp.int32)],
        name="positions",
    )(ids, owner_map, neighbor_table.reshape(-1))

    turned = right_side.reshape(per_dev, dof, n_sub, rhs).transpose(2, 0, 3, 1)
    if even:
        turned = turned.reshape(n_sub, per_dev // 2, 2, rhs, dof).transpose(0, 1, 3, 2, 4)
        turned = turned.reshape(n_sub, per_dev // 2, rhs, lanes)
    mine = lax.all_to_all(turned, "sub", split_axis=0, concat_axis=0, tiled=True)[order]
    if not even:
        mine = mine.reshape(n_own, 2, rhs, dof).transpose(0, 2, 1, 3)
    b_mine = mine.reshape(field)

    swap = [(c, c ^ 1) for c in range(CORES)]

    def gather(copies):
        own = lax.all_to_all(copies, "z", split_axis=0, concat_axis=0, tiled=True)
        par = lax.ppermute(own, "core", swap)
        return own.reshape((nz * n_own,) + field[1:]), par.reshape((nz * n_own,) + field[1:])

    b_own, b_par = gather(jnp.broadcast_to(b_mine[None], (nz,) + field))

    if n_sub == 4:
        op_x, op_y, b_own, b_par = lax.optimization_barrier((op_x, op_y, b_own, b_par))
        half = per_dev // 2
        op_d0 = lax.ppermute(op_y[:half], "sub", hop_x)
        op_d1 = lax.ppermute(op_x[half:], "sub", hop_y)
        ops = [coarse_op, op_x, op_y, op_d0, op_d1]
    else:
        every = lax.all_gather(coarse_op, "sub", axis=0)[order]
        ops = [every[k] for k in range(n_sub)]
    count = len(ops)
    held = [pltpu.VMEM(op.shape, F32) for op in ops]
    sems = pltpu.SemaphoreType.DMA((count,))
    dup = pltpu.VMEM((CORES * nz * n_loc, rhs, lanes), F32)
    spread_shape = jax.ShapeDtypeStruct((nz,) + field, F32)
    small = jax.ShapeDtypeStruct(field[1:], F32)
    own_shape = jax.ShapeDtypeStruct(field, F32)

    z1 = pl.pallas_call(
        functools.partial(first_kernel, count, dof, terms),
        out_shape=spread_shape,
        in_specs=[SMEM, VMEM, VMEM] + [ANY] * count,
        out_specs=VMEM,
        scratch_shapes=held + [sems, dup],
        compiler_params=PARAMS,
        name="first",
    )(positions, b_own, b_par, *ops)
    z1_own, z1_par = gather(z1)

    z2, basis, v1_mine, coeffs = pl.pallas_call(
        functools.partial(second_kernel, count, dof, terms),
        out_shape=[
            spread_shape,
            jax.ShapeDtypeStruct((CORES * nz * n_own,) + field[1:], F32),
            own_shape,
            small,
        ],
        in_specs=[SMEM, SMEM] + [VMEM] * 4 + [ANY] * count,
        out_specs=[VMEM] * 4,
        scratch_shapes=held + [sems, dup],
        compiler_params=PARAMS,
        name="second",
    )(ids, positions, b_own, b_par, z1_own, z1_par, *ops)
    z2_own, z2_par = gather(z2)

    copies = nz * CORES
    sums, v2_mine, coeffs = pl.pallas_call(
        functools.partial(third_kernel, count, dof, terms),
        out_shape=[jax.ShapeDtypeStruct((copies,) + field[1:], F32), own_shape, small],
        in_specs=[SMEM, SMEM] + [VMEM] * 8 + [ANY] * count,
        out_specs=[VMEM] * 3,
        scratch_shapes=held
        + [
            sems,
            dup,
            pltpu.VMEM((CORES * nz * n_own,) + field[1:], F32),
            pltpu.VMEM(field, F32),
        ],
        compiler_params=PARAMS,
        name="third",
    )(ids, positions, b_own, b_par, basis, z2_own, z2_par, b_mine, v1_mine, coeffs, *ops)
    sums = lax.all_to_all(sums, ("z", "core"), split_axis=0, concat_axis=0, tiled=True)

    blocks = (n_sub, per_dev // 2, rhs, lanes) if even else (1,) + field
    result = pl.pallas_call(
        combine_kernel,
        out_shape=jax.ShapeDtypeStruct(blocks, F32),
        in_specs=[SMEM] + [VMEM] * 5,
        out_specs=VMEM,
        name="combine",
    )(ids if even else ids * 0, sums, coeffs, b_mine, v1_mine, v2_mine)
    if even:
        result = lax.all_to_all(result, "sub", split_axis=0, concat_axis=0, tiled=True)
        return pl.pallas_call(
            functools.partial(finish_kernel, dof),
            out_shape=jax.ShapeDtypeStruct(right_side.shape, F32),
            in_specs=[VMEM],
            out_specs=VMEM,
            name="finish",
        )(result)
    result = result.reshape(n_own, rhs, 2, dof).transpose(0, 2, 1, 3).reshape(n_sub, per_dev, rhs, dof)
    result = lax.all_to_all(result[order], "sub", split_axis=0, concat_axis=0, tiled=True)
    return result.transpose(1, 3, 0, 2).reshape(right_side.shape)


def solution(mesh):
    n_grp, n_sub = mesh.shape["grp"], mesh.shape["sub"]
    inner = Mesh(mesh.devices.reshape(n_grp // CORES, CORES, n_sub), ("z", "core", "sub"))
    split = P(("z", "core", "sub"), None, None)
    return jax.shard_map(
        per_device,
        mesh=inner,
        in_specs=(split, split, P(), P()),
        out_specs=split,
        check_vma=False,
    )
```

```python
import functools

import jax
import jax.numpy as jnp
from jax import lax
from jax.experimental import pallas as pl
from jax.experimental.pallas import tpu as pltpu
from jax.sharding import Mesh
from jax.sharding import PartitionSpec as P


F32 = jnp.float32
BF16 = jnp.bfloat16
CORES = 2
VMEM = pl.BlockSpec(memory_space=pltpu.VMEM)
SMEM = pl.BlockSpec(memory_space=pltpu.SMEM)
ANY = pl.BlockSpec(memory_space=pl.ANY)
PARAMS = pltpu.CompilerParams(vmem_limit_bytes=20 * 1024 * 1024)
SMALL = pltpu.CompilerParams(vmem_limit_bytes=4 * 1024 * 1024)


def divide(value, size):
    if size & (size - 1):
        return lax.div(value, jnp.int32(size))
    return lax.shift_right_logical(value, jnp.int32(size.bit_length() - 1))


def remain(value, size):
    if size & (size - 1):
        return lax.rem(value, jnp.int32(size))
    return value & (size - 1)


def low_half(shape, dof):
    return lax.broadcasted_iota(jnp.int32, shape, 1) < dof


def lane_sum(values):
    return jnp.sum(values, axis=1, keepdims=True)


def split_bf16(values):
    high = values.astype(BF16)
    return high, (values - high.astype(F32)).astype(BF16)


def place(columns, shape):
    lane = lax.broadcasted_iota(jnp.int32, shape, 1)
    packed = jnp.zeros(shape, F32)
    for index, column in enumerate(columns):
        packed = jnp.where(lane == index, column, packed)
    return packed


def dense_rows(columns, shape, rows):
    size, lanes = shape
    per_row = lanes // size
    flipped = place(columns, shape).T
    lane = lax.broadcasted_iota(jnp.int32, (1, lanes), 1)
    wide = jnp.concatenate([flipped] * per_row, axis=1)
    packed = []
    for row in range(rows):
        line = jnp.zeros((1, lanes), F32)
        for inner in range(per_row):
            index = row * per_row + inner
            if index < len(columns):
                line = jnp.where(divide(lane, size) == inner, wide[index : index + 1], line)
        packed.append(line)
    return jnp.concatenate(packed, axis=0)


def position_kernel(geometry, ids, owner, table, out, where):
    per_dev, n_sub, nz, hops = geometry
    me_z, me_c, me_s = ids[0], ids[1], ids[2]
    sites = owner.shape[0]

    def locate(slot):
        dev = divide(slot, per_dev)
        grp = divide(dev, n_sub)
        block = (remain(grp, CORES) ^ me_c) * nz + divide(grp, CORES)
        return (block * n_sub + (remain(dev, n_sub) ^ me_s)) * per_dev + remain(slot, per_dev)

    def fill(slot, carry):
        where[owner[slot]] = locate(slot)
        return carry

    lax.fori_loop(0, sites, fill, 0, unroll=8)

    def look(local, carry):
        dev = (me_z * CORES + me_c) * n_sub + (divide(local, per_dev) ^ me_s)
        slot = dev * per_dev + remain(local, per_dev)
        base = owner[slot] * hops
        out[local * (hops + 1)] = locate(slot)
        for hop in range(hops):
            out[local * (hops + 1) + 1 + hop] = where[table[base + hop]]
        return carry

    lax.fori_loop(0, n_sub * per_dev, look, 0, unroll=2)


def spread(dup, pair, values, dof):
    mask = low_half(values.shape, dof)
    rolled = pltpu.roll(values, dof, 1)
    dup[2 * pair] = jnp.where(mask, values, rolled)
    dup[2 * pair + 1] = jnp.where(mask, rolled, values)


def site_product(op, local, pos, dup, terms, dof):
    rows = dup.shape[1]
    mask = low_half((rows, 2 * dof), dof)
    tiles = []
    for first in range(0, terms - 1, 2):
        left = dup[pos[local * terms + first]]
        right = dup[pos[local * terms + first + 1]]
        tiles.append(jnp.where(mask, left, right))
    if terms % 2:
        tiles.append(dup[pos[local * terms + terms - 1]][:, :dof])
    high, low = split_bf16(jnp.concatenate(tiles, axis=1))
    op_high, op_low = split_bf16(op)
    product = lax.dot_general(
        jnp.concatenate([high, low], axis=0),
        jnp.concatenate([op_high, op_low], axis=0),
        (((1,), (1,)), ((), ())),
        preferred_element_type=F32,
    )
    total = product[:rows] + product[rows:]
    return total + pltpu.roll(total, dof, 1)


def apply_rows(ops, pos, dup, terms, dof, put, base=0):
    per_part = ops[0].shape[0]
    rows = dup.shape[1]
    mask = low_half((rows, 2 * dof), dof)
    if per_part % 2:
        for pair in range(len(ops) * per_part // 2):
            halves = [
                site_product(ops[i // per_part][i % per_part], i, pos, dup, terms, dof)
                for i in (2 * pair, 2 * pair + 1)
            ]
            put(pair, jnp.where(mask, halves[0], halves[1]))
        return
    for op in ops:

        def body(inner, carry, base=base, op=op):
            first = base + 2 * inner
            even = site_product(op[2 * inner], first, pos, dup, terms, dof)
            odd = site_product(op[2 * inner + 1], first + 1, pos, dup, terms, dof)
            put(base // 2 + inner, jnp.where(mask, even, odd))
            return carry

        lax.fori_loop(0, op.shape[0] // 2, body, 0, unroll=True)
        base += op.shape[0]


def put_copies(out):
    def put(pair, values):
        for block in range(out.shape[0]):
            out[block, pair] = values

    return put


def start_copies(sources, targets, sems):
    copies = [
        pltpu.make_async_copy(source, target, sems.at[index])
        for index, (source, target) in enumerate(zip(sources, targets))
    ]
    for copy in copies:
        copy.start()
    return copies


def over_pairs(fields, step, init):
    n_pair = fields[0].shape[0]
    for half in range(2):
        init = lax.fori_loop(
            0, n_pair, lambda pair, carry, half=half: step(half, pair, carry), init, unroll=8
        )
    return init


def first_kernel(count, base, dof, terms, pos, own, par, *rest):
    ops, rest = rest[:count], rest[count:]
    before = None
    if base:
        before, rest = rest[0], rest[1:]
    out, held, sems, dup = rest[0], rest[1 : count + 1], rest[count + 1], rest[count + 2]
    copies = start_copies(ops, held, sems)
    n_pair = own.shape[0]
    fields = (own, par)

    def build(half, pair, carry):
        spread(dup, half * n_pair + pair, fields[half][pair], dof)
        return carry

    over_pairs(fields, build, 0)
    put = put_copies(out)
    if base:
        for pair in range(base // 2):
            put(pair, before[0, pair])
    for copy in copies:
        copy.wait()
    apply_rows(held, pos, dup, terms, dof, put, base)


def second_kernel(count, sends, dof, terms, ids, pos, b_own, b_par, z_own, z_par, *rest):
    ops, (out, basis, mine, coeffs) = rest[:count], rest[count : count + 4]
    shares, rest = rest[count + 4 : count + 4 + sends], rest[count + 4 + sends :]
    held, sems, dup = rest[:count], rest[count], rest[count + 1]
    copies = start_copies(ops, held, sems)
    n_pair = b_own.shape[0]
    b_ref, z_ref = (b_own, b_par), (z_own, z_par)
    shape = b_own.shape[1:]
    zero = jnp.zeros(shape, F32)

    def dots(half, pair, carry):
        b, z = b_ref[half][pair], z_ref[half][pair]
        return carry[0] + b * b, carry[1] + b * z

    norm, cross = over_pairs(b_ref, dots, (zero, zero))
    beta_sq = lane_sum(norm)
    beta = jnp.sqrt(beta_sq)
    scale = 1.0 / beta
    h00 = lane_sum(cross) * scale * scale

    def remove(half, pair, carry):
        w = z_ref[half][pair] * scale - (h00 * scale) * b_ref[half][pair]
        basis[half * n_pair + pair] = w
        return carry + w * w

    h10 = jnp.sqrt(lane_sum(over_pairs(b_ref, remove, zero)))
    unit = 1.0 / h10

    def build(half, pair, carry):
        v = basis[half * n_pair + pair] * unit
        basis[half * n_pair + pair] = v
        spread(dup, half * n_pair + pair, v, dof)
        return carry

    over_pairs(b_ref, build, 0)
    coeffs[...] = place([beta, h00, h10], shape)
    n_mine = mine.shape[0]
    mine[...] = basis[pl.ds(ids[0] * n_mine, n_mine)]
    for copy in copies:
        copy.wait()

    apply_rows(held, pos, dup, terms, dof, put_copies(out))
    for index, share in enumerate(shares):
        start = index * share.shape[1]
        for inner in range(share.shape[1]):
            share[0, inner] = z_own[ids[0] * n_mine + start + inner]
            share[1, inner] = out[0, start + inner]


def third_kernel(
    count, dof, terms, ids, pos, b_own, b_par, basis, z_own, z_par, b_mine, v1_mine, coeffs, *rest
):
    ops, (sums, mine) = rest[:count], rest[count : count + 2]
    rest = rest[count + 2 :]
    held, sems, dup, work, image = (
        rest[:count],
        rest[count],
        rest[count + 1],
        rest[count + 2],
        rest[count + 3],
    )
    copies = start_copies(ops, held, sems)
    n_pair = b_own.shape[0]
    b_ref, z_ref = (b_own, b_par), (z_own, z_par)
    shape = b_own.shape[1:]
    zero = jnp.zeros(shape, F32)
    known = coeffs[...]
    scale = 1.0 / known[:, 0:1]

    def dots(half, pair, carry):
        z = z_ref[half][pair]
        return carry[0] + b_ref[half][pair] * z, carry[1] + basis[half * n_pair + pair] * z

    first, second = over_pairs(b_ref, dots, (zero, zero))
    h01 = lane_sum(first) * scale
    h11 = lane_sum(second)

    def remove(half, pair, carry):
        w = (
            z_ref[half][pair]
            - (h01 * scale) * b_ref[half][pair]
            - h11 * basis[half * n_pair + pair]
        )
        work[half * n_pair + pair] = w
        return carry + w * w

    h21 = jnp.sqrt(lane_sum(over_pairs(b_ref, remove, zero)))
    unit = 1.0 / h21

    def build(half, pair, carry):
        v = work[half * n_pair + pair] * unit
        work[half * n_pair + pair] = v
        spread(dup, half * n_pair + pair, v, dof)
        return carry

    over_pairs(b_ref, build, 0)
    n_mine = mine.shape[0]
    mine[...] = work[pl.ds(ids[0] * n_mine, n_mine)]
    for copy in copies:
        copy.wait()

    def put(pair, values):
        image[pair] = values

    apply_rows(held, pos, dup, terms, dof, put)

    def last(pair, carry):
        u = image[pair]
        return (
            carry[0] + b_mine[pair] * u,
            carry[1] + v1_mine[pair] * u,
            carry[2] + mine[pair] * u,
            carry[3] + u * u,
        )

    parts = lax.fori_loop(0, n_mine, last, (zero, zero, zero, zero), unroll=True)
    solved = [known[:, 0:1], known[:, 1:2], known[:, 2:3], h01, h11, h21]
    columns = [lane_sum(part) for part in parts] + solved
    if len(sums.shape) == 3 and sums.shape[1:] == shape:
        packed = place(columns, shape)
    else:
        packed = dense_rows(columns, shape, sums.shape[1])
    for block in range(sums.shape[0]):
        sums[block] = packed


def weigh(values):
    d02, h12, h22, g22, beta, h00, h10, h01, h11, h21 = values
    scale = 1.0 / beta
    h02 = d02 * scale
    g00 = h00 * h00 + h10 * h10
    g01 = h00 * h01 + h10 * h11
    g02 = h00 * h02 + h10 * h12
    g11 = h01 * h01 + h11 * h11 + h21 * h21
    g12 = h01 * h02 + h11 * h12 + h21 * h22
    inv0 = 1.0 / g00
    l10 = g01 * inv0
    l20 = g02 * inv0
    d1 = g11 - l10 * g01
    e21 = g12 - l20 * g01
    inv1 = 1.0 / d1
    l21 = e21 * inv1
    d2 = g22 - l20 * g02 - l21 * e21
    r0 = beta * h00
    r1 = beta * h01 - l10 * r0
    r2 = beta * h02 - l20 * r0 - l21 * r1
    y2 = r2 / d2
    y1 = r1 * inv1 - l21 * y2
    y0 = r0 * inv0 - l10 * y1 - l20 * y2
    return scale, y0, y1, y2


def combine_kernel(sums, b_mine, v1_mine, v2_mine, out):
    total = sums[0]
    for block in range(1, sums.shape[0]):
        total = total + sums[block]
    known = sums[0]
    values = [(total if i < 4 else known)[:, i : i + 1] for i in range(10)]
    scale, y0, y1, y2 = weigh(values)
    for pair in range(b_mine.shape[0]):
        out[pair] = (y0 * scale) * b_mine[pair] + y1 * v1_mine[pair] + y2 * v2_mine[pair]


def finish_kernel(dof, ids, info, turned, *rest):
    shares, out, stack, factor = rest[:-3], rest[-3], rest[-2], rest[-1]
    n_sub, per_part, rhs, lanes = turned.shape
    per_row = lanes // rhs
    n_rows = info.shape[1]
    first = [info[quarter] for quarter in range(n_sub)]
    total = list(first)
    for block in range(1, info.shape[0] // n_sub):
        for quarter in range(n_sub):
            total[quarter] = total[quarter] + info[block * n_sub + quarter]
    known = [jnp.concatenate([f[r : r + 1] for f in first], axis=0) for r in range(n_rows)]
    added = [jnp.concatenate([t[r : r + 1] for t in total], axis=0) for r in range(n_rows)]
    values = []
    for index in range(10):
        source = (added if index < 4 else known)[index // per_row]
        shift = rhs * (index % per_row)
        values.append(pltpu.roll(source, lanes - shift, 1) if shift else source)
    scale, y0, y1, y2 = weigh(values)
    h00, h10, h01, h11, h21 = values[5:]
    gamma = y2 / h21
    both = (y1 - gamma * h11) / h10
    coeffs = [(y0 - both * h00 - gamma * h01) * scale, both * scale, gamma]
    flipped = jnp.concatenate(coeffs, axis=0)
    spare = -flipped.shape[0] % 8
    if spare:
        flipped = jnp.concatenate([flipped, jnp.zeros((spare, lanes), F32)], axis=0)
    flipped = flipped.T
    for index in range(3 * n_sub):
        factor[index] = jnp.broadcast_to(flipped[:rhs, index : index + 1], (rhs, lanes))
    for k in range(n_sub):
        quarter = ids[2] ^ k
        alpha, beta, gamma = (factor[part * n_sub + quarter] for part in range(3))
        start = pl.multiple_of(quarter * rhs, 8)
        for pair in range(per_part):
            mixed = alpha * turned[quarter, pair] + beta * shares[k][0, pair]
            stack[pair, pl.ds(start, rhs), :] = mixed + gamma * shares[k][1, pair]
    for pair in range(per_part):
        both = stack[pair].T
        out[2 * pair] = both[:dof]
        out[2 * pair + 1] = both[dof:]


def per_device(coarse_op, right_side, owner_map, neighbor_table):
    nz = lax.axis_size("z")
    n_sub = lax.axis_size("sub")
    per_dev, dof, width = coarse_op.shape
    terms = width // dof
    hops = terms - 1
    rhs = right_side.shape[2] // n_sub
    n_loc = n_sub * per_dev
    n_own = n_loc // 2
    me_z, me_c, me_s = lax.axis_index("z"), lax.axis_index("core"), lax.axis_index("sub")
    ids = jnp.stack([me_z, me_c, me_s]).astype(jnp.int32)
    even = per_dev % 2 == 0
    lanes = 2 * dof
    field = (n_own, rhs, lanes)

    relay = n_sub == 4 and even
    order = jnp.arange(n_sub, dtype=jnp.int32) ^ me_s
    hops_to = [[(s, s ^ k) for s in range(n_sub)] for k in range(n_sub)]
    half = per_dev // 2
    if relay:
        op_low, op_high = coarse_op[:half], coarse_op[half:]
        x_high = lax.ppermute(op_high, "sub", hops_to[1])
        y_low = lax.ppermute(op_low, "sub", hops_to[2])
        x_low = lax.ppermute(op_low, "sub", hops_to[1])
        y_high = lax.ppermute(op_high, "sub", hops_to[2])

    positions = pl.pallas_call(
        functools.partial(position_kernel, (per_dev, n_sub, nz, hops)),
        out_shape=jax.ShapeDtypeStruct((n_loc * terms,), jnp.int32),
        in_specs=[SMEM, SMEM, SMEM],
        out_specs=SMEM,
        scratch_shapes=[pltpu.SMEM((owner_map.shape[0],), jnp.int32)],
        compiler_params=SMALL,
        name="positions",
    )(ids, owner_map, neighbor_table.reshape(-1))

    turned = right_side.reshape(per_dev, dof, n_sub, rhs).transpose(2, 0, 3, 1)
    if even:
        turned = turned.reshape(n_sub, per_dev // 2, 2, rhs, dof).transpose(0, 1, 3, 2, 4)
        turned = turned.reshape(n_sub, per_dev // 2, rhs, lanes)
    mine = lax.all_to_all(turned, "sub", split_axis=0, concat_axis=0, tiled=True)
    mine = mine[order]
    if not even:
        mine = mine.reshape(n_own, 2, rhs, dof).transpose(0, 2, 1, 3)
    b_mine = mine.reshape(field)

    swap = [(c, c ^ 1) for c in range(CORES)]

    def over_z(copies):
        return lax.all_to_all(copies, "z", split_axis=0, concat_axis=0, tiled=True)

    def partner(own):
        par = lax.ppermute(own, "core", swap)
        return own.reshape((nz * n_own,) + field[1:]), par.reshape((nz * n_own,) + field[1:])

    if relay:
        d_low = lax.ppermute(y_low, "sub", hops_to[1])
        d_high = lax.ppermute(x_high, "sub", hops_to[2])
        stages = [[coarse_op, x_low, x_high, y_low, y_high], [d_low, d_high]]
    b_own = over_z(jnp.broadcast_to(b_mine[None], (nz,) + field))
    if not relay:
        every = lax.all_gather(coarse_op, "sub", axis=0)[order]
        stages = [[every[k] for k in range(n_sub)]]
    b_own, b_par = partner(b_own)
    ops = [op for stage in stages for op in stage]
    count = len(ops)

    def held(parts):
        return [pltpu.VMEM(op.shape, F32) for op in parts] + [
            pltpu.SemaphoreType.DMA((len(parts),)),
            pltpu.VMEM((CORES * nz * n_loc, rhs, lanes), F32),
        ]

    full = (CORES * nz * n_own,) + field[1:]
    small = jax.ShapeDtypeStruct(field[1:], F32)
    own_shape = jax.ShapeDtypeStruct(field, F32)

    z1, base = [], 0
    for index, stage in enumerate(stages):
        rows = base + sum(op.shape[0] for op in stage)
        blocks = nz if index + 1 == len(stages) else 1
        z1 = [
            pl.pallas_call(
                functools.partial(first_kernel, len(stage), base, dof, terms),
                out_shape=jax.ShapeDtypeStruct((blocks, rows // 2) + field[1:], F32),
                in_specs=[SMEM, VMEM, VMEM] + [ANY] * len(stage) + [VMEM] * len(z1),
                out_specs=VMEM,
                scratch_shapes=held(stage),
                compiler_params=PARAMS,
                name="first",
            )(positions, b_own, b_par, *stage, *z1)
        ]
        base = rows
    z1 = z1[0]
    z1_own, z1_par = partner(over_z(z1))

    sends = n_sub if even else 0
    share = jax.ShapeDtypeStruct((2, per_dev // 2, rhs, lanes), F32)
    z2, basis, v1_mine, coeffs, *shares = pl.pallas_call(
        functools.partial(second_kernel, count, sends, dof, terms),
        out_shape=[
            jax.ShapeDtypeStruct((nz,) + field, F32),
            jax.ShapeDtypeStruct(full, F32),
            own_shape,
            small,
        ]
        + [share] * sends,
        in_specs=[SMEM, SMEM] + [VMEM] * 4 + [ANY] * count,
        out_specs=[VMEM] * (4 + sends),
        scratch_shapes=held(ops),
        compiler_params=PARAMS,
        name="second",
    )(ids, positions, b_own, b_par, z1_own, z1_par, *ops)
    z2_own = over_z(z2)
    shares[1:] = [lax.ppermute(shares[k], "sub", hops_to[k]) for k in range(1, sends)]
    z2_own, z2_par = partner(z2_own)

    axes = ("z", "core", "sub") if even else ("z", "core")
    copies = nz * CORES * (n_sub if even else 1)
    note = (pl.cdiv(10 * rhs, lanes), lanes) if even else field[1:]
    sums, v2_mine = pl.pallas_call(
        functools.partial(third_kernel, count, dof, terms),
        out_shape=[jax.ShapeDtypeStruct((copies,) + note, F32), own_shape],
        in_specs=[SMEM, SMEM] + [VMEM] * 8 + [ANY] * count,
        out_specs=[VMEM] * 2,
        scratch_shapes=held(ops) + [pltpu.VMEM(full, F32), pltpu.VMEM(field, F32)],
        compiler_params=PARAMS,
        name="third",
    )(ids, positions, b_own, b_par, basis, z2_own, z2_par, b_mine, v1_mine, coeffs, *ops)
    sums = lax.all_to_all(sums, axes, split_axis=0, concat_axis=0, tiled=True)

    if even:
        return pl.pallas_call(
            functools.partial(finish_kernel, dof),
            out_shape=jax.ShapeDtypeStruct(right_side.shape, F32),
            in_specs=[SMEM] + [VMEM] * (2 + sends),
            out_specs=VMEM,
            scratch_shapes=[
                pltpu.VMEM((per_dev // 2, n_sub * rhs, lanes), F32),
                pltpu.VMEM((3 * n_sub, rhs, lanes), F32),
            ],
            compiler_params=SMALL,
            name="finish",
        )(ids, sums, turned, *shares)
    result = pl.pallas_call(
        combine_kernel,
        out_shape=own_shape,
        in_specs=[VMEM] * 4,
        out_specs=VMEM,
        compiler_params=SMALL,
            name="combine",
    )(sums, b_mine, v1_mine, v2_mine)
    result = result.reshape(n_own, rhs, 2, dof).transpose(0, 2, 1, 3)
    result = result.reshape(n_sub, per_dev, rhs, dof)[order]
    result = lax.all_to_all(result, "sub", split_axis=0, concat_axis=0, tiled=True)
    return result.transpose(1, 3, 0, 2).reshape(right_side.shape)


def solution(mesh):
    n_grp, n_sub = mesh.shape["grp"], mesh.shape["sub"]
    inner = Mesh(mesh.devices.reshape(n_grp // CORES, CORES, n_sub), ("z", "core", "sub"))
    split = P(("z", "core", "sub"), None, None)

    return jax.shard_map(
        per_device,
        mesh=inner,
        in_specs=(split, split, P(), P()),
        out_specs=split,
        check_vma=False,
    )
```

```python
import functools

import jax
import jax.numpy as jnp
from jax import lax
from jax.experimental import pallas as pl
from jax.experimental.pallas import tpu as pltpu
from jax.sharding import Mesh
from jax.sharding import PartitionSpec as P


F32 = jnp.float32
BF16 = jnp.bfloat16
CORES = 2
VMEM = pl.BlockSpec(memory_space=pltpu.VMEM)
SMEM = pl.BlockSpec(memory_space=pltpu.SMEM)
HBM = pl.BlockSpec(memory_space=pltpu.HBM)
ANY = pl.BlockSpec(memory_space=pl.ANY)
PARAMS = pltpu.CompilerParams(vmem_limit_bytes=20 * 1024 * 1024)
SMALL = pltpu.CompilerParams(vmem_limit_bytes=4 * 1024 * 1024)


def divide(value, size):
    if size & (size - 1):
        return lax.div(value, jnp.int32(size))
    return lax.shift_right_logical(value, jnp.int32(size.bit_length() - 1))


def remain(value, size):
    if size & (size - 1):
        return lax.rem(value, jnp.int32(size))
    return value & (size - 1)


def low_half(shape, dof):
    return lax.broadcasted_iota(jnp.int32, shape, 1) < dof


def lane_sum(values):
    return jnp.sum(values, axis=1, keepdims=True)


def split_bf16(values):
    high = values.astype(BF16)
    return high, (values - high.astype(F32)).astype(BF16)


def place(columns, shape):
    lane = lax.broadcasted_iota(jnp.int32, shape, 1)
    packed = jnp.zeros(shape, F32)
    for index, column in enumerate(columns):
        packed = jnp.where(lane == index, column, packed)
    return packed


def dense_rows(columns, shape, rows):
    size, lanes = shape
    per_row = lanes // size
    flipped = place(columns, shape).T
    lane = lax.broadcasted_iota(jnp.int32, (1, lanes), 1)
    wide = jnp.concatenate([flipped] * per_row, axis=1)
    packed = []
    for row in range(rows):
        line = jnp.zeros((1, lanes), F32)
        for inner in range(per_row):
            index = row * per_row + inner
            if index < len(columns):
                line = jnp.where(divide(lane, size) == inner, wide[index : index + 1], line)
        packed.append(line)
    return jnp.concatenate(packed, axis=0)


def position_kernel(geometry, ids, owner, table, out, where):
    per_dev, n_sub, nz, hops = geometry
    me_z, me_c, me_s = ids[0], ids[1], ids[2]
    sites = owner.shape[0]

    def locate(slot):
        dev = divide(slot, per_dev)
        grp = divide(dev, n_sub)
        block = (remain(grp, CORES) ^ me_c) * nz + (divide(grp, CORES) ^ me_z)
        return (block * n_sub + (remain(dev, n_sub) ^ me_s)) * per_dev + remain(slot, per_dev)

    def fill(slot, carry):
        where[owner[slot]] = locate(slot)
        return carry

    lax.fori_loop(0, sites, fill, 0, unroll=8)

    def look(local, carry):
        dev = (me_z * CORES + me_c) * n_sub + (divide(local, per_dev) ^ me_s)
        slot = dev * per_dev + remain(local, per_dev)
        base = owner[slot] * hops
        out[local * (hops + 1)] = locate(slot)
        for hop in range(hops):
            out[local * (hops + 1) + 1 + hop] = where[table[base + hop]]
        return carry

    lax.fori_loop(0, n_sub * per_dev, look, 0, unroll=2)


def pack_kernel(dof, op, right, low, high, turned, held, op_held, sems):
    half = op.shape[0] // 2
    sources = [right, op.at[pl.ds(0, half)], op.at[pl.ds(half, half)]]
    copies = start_copies(sources, [held, op_held.at[0], op_held.at[1]], sems)
    n_sub, per_part, rhs = turned.shape[0], turned.shape[1], turned.shape[2]
    copies[0].wait()
    for pair in range(per_part):
        both = jnp.concatenate([held[2 * pair], held[2 * pair + 1]], axis=0).T
        for quarter in range(n_sub):
            turned[quarter, pair] = both[quarter * rhs : (quarter + 1) * rhs]
    main = op.shape[2] - dof
    for index, target in enumerate((low, high)):
        copies[index + 1].wait()
        for pair in range(half // 2):
            even, odd = op_held[index, 2 * pair], op_held[index, 2 * pair + 1]
            target[pair, :, :main] = even[:, :main]
            target[pair, :, main : 2 * main] = odd[:, :main]
            target[pair, :, 2 * main :] = jnp.concatenate([even[:, main:], odd[:, main:]], axis=1)


def spread(dup, pair, values, dof):
    mask = low_half(values.shape, dof)
    rolled = pltpu.roll(values, dof, 1)
    dup[2 * pair] = jnp.where(mask, values, rolled)
    dup[2 * pair + 1] = jnp.where(mask, rolled, values)


def site_product(stacked, local, pos, dup, terms, dof):
    rows = dup.shape[1]
    mask = low_half((rows, 2 * dof), dof)
    tiles = []
    for first in range(0, terms - 1, 2):
        left = dup[pos[local * terms + first]]
        right = dup[pos[local * terms + first + 1]]
        tiles.append(jnp.where(mask, left, right))
    if terms % 2:
        tiles.append(dup[pos[local * terms + terms - 1]][:, :dof])
    high, low = split_bf16(jnp.concatenate(tiles, axis=1))
    product = lax.dot_general(
        jnp.concatenate([high, low], axis=0),
        stacked,
        (((1,), (1,)), ((), ())),
        preferred_element_type=F32,
    )
    total = product[:rows] + product[rows:]
    return total + pltpu.roll(total, dof, 1)


def stack_split(op):
    high, low = split_bf16(op)
    return jnp.concatenate([high, low], axis=0)


def pair_product(stacks, local, pos, dup, terms, dof):
    even, odd = (
        site_product(stack, local + i, pos, dup, terms, dof) for i, stack in enumerate(stacks)
    )
    return jnp.where(low_half(even.shape, dof), even, odd)


def apply_rows(stages, pos, dup, terms, dof, put):
    base = 0
    for stage in stages:

        def body(pair, carry, base=base, stage=stage):
            stacks = [stage[2 * pair], stage[2 * pair + 1]]
            put(base // 2 + pair, pair_product(stacks, base + 2 * pair, pos, dup, terms, dof))
            return carry

        lax.fori_loop(0, stage.shape[0] // 2, body, 0, unroll=4)
        base += stage.shape[0]


def split_rows(ops, split, base, pos, dup, terms, dof, put):
    offset = 0
    if ops[0].shape[2] == terms * dof:
        flat = [(op, i) for op in ops for i in range(op.shape[0])]
        for pair in range(len(flat) // 2):
            stacks = [stack_split(op[i]) for op, i in flat[2 * pair : 2 * pair + 2]]
            split[2 * pair], split[2 * pair + 1] = stacks
            put((base + 2 * pair) // 2, pair_product(stacks, base + 2 * pair, pos, dup, terms, dof))
        return
    for op in ops:
        main = op.shape[2] // 2 - dof

        def body(pair, carry, offset=offset, op=op, main=main):
            rows = op[pair]
            tail = rows[:, 2 * main :]
            even = jnp.concatenate([rows[:, :main], tail[:, :dof]], axis=1)
            odd = jnp.concatenate([rows[:, main : 2 * main], tail[:, dof:]], axis=1)
            stacks = [stack_split(even), stack_split(odd)]
            split[offset + 2 * pair], split[offset + 2 * pair + 1] = stacks
            local = base + offset + 2 * pair
            put(divide(local, 2), pair_product(stacks, local, pos, dup, terms, dof))
            return carry

        lax.fori_loop(0, op.shape[0], body, 0, unroll=True)
        offset += 2 * op.shape[0]


def start_copies(sources, targets, sems):
    copies = [
        pltpu.make_async_copy(source, target, sems.at[index])
        for index, (source, target) in enumerate(zip(sources, targets))
    ]
    for copy in copies:
        copy.start()
    return copies


def over_pairs(fields, step, init):
    n_pair = fields[0].shape[0]
    for block in range(len(fields)):
        init = lax.fori_loop(
            0, n_pair, lambda pair, carry, block=block: step(block, pair, carry), init, unroll=8
        )
    return init


def share_out(values, shares):
    for index, share in enumerate(shares):
        for inner in range(share.shape[0]):
            share[inner] = values[index * share.shape[0] + inner]


def first_kernel(n_field, count, dof, terms, pos, *rest):
    fields, ops, rest = rest[:n_field], rest[n_field : n_field + count], rest[n_field + count :]
    out, split, dup = rest[:3]
    held, sems = rest[3 : count + 3], rest[count + 3]
    copies = start_copies(ops, held, sems)
    n_pair = fields[0].shape[0]

    def build(block, pair, carry):
        spread(dup, block * n_pair + pair, fields[block][pair], dof)
        return carry

    over_pairs(fields, build, 0)
    for copy in copies:
        copy.wait()

    def put(pair, values):
        out[pair] = values

    split_rows(held, split, 0, pos, dup, terms, dof, put)


def more_kernel(count, dof, terms, pos, dup, before, *rest):
    ops, out, split, shares = rest[:count], rest[count], rest[count + 1], rest[count + 2 :]
    base = 2 * before.shape[0]
    for pair in range(before.shape[0]):
        out[pair] = before[pair]

    def put(pair, values):
        out[pair] = values

    split_rows(ops, split, base, pos, dup, terms, dof, put)
    share_out(out, shares)


def second_kernel(n_field, count, sends, dof, terms, pos, *rest):
    b_ref, z_ref, rest = rest[:n_field], rest[n_field : 2 * n_field], rest[2 * n_field :]
    stages, (out, basis, mine, coeffs) = rest[:count], rest[count : count + 4]
    shares, dup = rest[count + 4 : count + 4 + sends], rest[count + 4 + sends]
    n_pair = b_ref[0].shape[0]
    shape = b_ref[0].shape[1:]
    zero = jnp.zeros(shape, F32)

    def dots(block, pair, carry):
        b, z = b_ref[block][pair], z_ref[block][pair]
        return carry[0] + b * b, carry[1] + b * z

    norm, cross = over_pairs(b_ref, dots, (zero, zero))
    beta = jnp.sqrt(lane_sum(norm))
    scale = 1.0 / beta
    h00 = lane_sum(cross) * scale * scale

    def remove(block, pair, carry):
        w = z_ref[block][pair] * scale - (h00 * scale) * b_ref[block][pair]
        basis[block * n_pair + pair] = w
        return carry + w * w

    h10 = jnp.sqrt(lane_sum(over_pairs(b_ref, remove, zero)))
    unit = 1.0 / h10

    def build(block, pair, carry):
        v = basis[block * n_pair + pair] * unit
        basis[block * n_pair + pair] = v
        spread(dup, block * n_pair + pair, v, dof)
        return carry

    over_pairs(b_ref, build, 0)
    coeffs[...] = place([beta, h00, h10], shape)
    mine[...] = basis[:n_pair]

    def put(pair, values):
        out[pair] = values

    apply_rows(stages, pos, dup, terms, dof, put)
    share_out(out, shares)


def third_kernel(n_field, count, dof, terms, pos, basis, v1_mine, coeffs, *rest):
    b_ref, z_ref, rest = rest[:n_field], rest[n_field : 2 * n_field], rest[2 * n_field :]
    stages, (sums, mine, dup, work, image) = rest[:count], rest[count:]
    b_mine = b_ref[0]
    n_pair = b_mine.shape[0]
    shape = b_mine.shape[1:]
    zero = jnp.zeros(shape, F32)
    known = coeffs[...]
    scale = 1.0 / known[:, 0:1]

    def dots(block, pair, carry):
        z = z_ref[block][pair]
        return carry[0] + b_ref[block][pair] * z, carry[1] + basis[block * n_pair + pair] * z

    first, second = over_pairs(b_ref, dots, (zero, zero))
    h01 = lane_sum(first) * scale
    h11 = lane_sum(second)

    def remove(block, pair, carry):
        w = (
            z_ref[block][pair]
            - (h01 * scale) * b_ref[block][pair]
            - h11 * basis[block * n_pair + pair]
        )
        work[block * n_pair + pair] = w
        return carry + w * w

    h21 = jnp.sqrt(lane_sum(over_pairs(b_ref, remove, zero)))
    unit = 1.0 / h21

    def build(block, pair, carry):
        v = work[block * n_pair + pair] * unit
        work[block * n_pair + pair] = v
        spread(dup, block * n_pair + pair, v, dof)
        return carry

    over_pairs(b_ref, build, 0)
    mine[...] = work[:n_pair]

    def put(pair, values):
        image[pair] = values

    apply_rows(stages, pos, dup, terms, dof, put)

    def last(pair, carry):
        u = image[pair]
        return (
            carry[0] + b_mine[pair] * u,
            carry[1] + v1_mine[pair] * u,
            carry[2] + mine[pair] * u,
            carry[3] + u * u,
        )

    parts = lax.fori_loop(0, n_pair, last, (zero, zero, zero, zero), unroll=True)
    solved = [known[:, 0:1], known[:, 1:2], known[:, 2:3], h01, h11, h21]
    columns = [lane_sum(part) for part in parts] + solved
    if len(sums.shape) == 3 and sums.shape[1:] == shape:
        packed = place(columns, shape)
    else:
        packed = dense_rows(columns, shape, sums.shape[1])
    for block in range(sums.shape[0]):
        sums[block] = packed


def weigh(values):
    d02, h12, h22, g22, beta, h00, h10, h01, h11, h21 = values
    scale = 1.0 / beta
    h02 = d02 * scale
    g00 = h00 * h00 + h10 * h10
    g01 = h00 * h01 + h10 * h11
    g02 = h00 * h02 + h10 * h12
    g11 = h01 * h01 + h11 * h11 + h21 * h21
    g12 = h01 * h02 + h11 * h12 + h21 * h22
    inv0 = 1.0 / g00
    l10 = g01 * inv0
    l20 = g02 * inv0
    d1 = g11 - l10 * g01
    e21 = g12 - l20 * g01
    inv1 = 1.0 / d1
    l21 = e21 * inv1
    d2 = g22 - l20 * g02 - l21 * e21
    r0 = beta * h00
    r1 = beta * h01 - l10 * r0
    r2 = beta * h02 - l20 * r0 - l21 * r1
    y2 = r2 / d2
    y1 = r1 * inv1 - l21 * y2
    y0 = r0 * inv0 - l10 * y1 - l20 * y2
    return scale, y0, y1, y2


def combine_kernel(sums, b_mine, v1_mine, v2_mine, out):
    total = sums[0]
    for block in range(1, sums.shape[0]):
        total = total + sums[block]
    known = sums[0]
    values = [(total if i < 4 else known)[:, i : i + 1] for i in range(10)]
    scale, y0, y1, y2 = weigh(values)
    for pair in range(b_mine.shape[0]):
        out[pair] = (y0 * scale) * b_mine[pair] + y1 * v1_mine[pair] + y2 * v2_mine[pair]


def finish_kernel(dof, ids, info, turned, *rest):
    out, stack, factor = rest[-3:]
    n_sub, per_part, rhs, lanes = turned.shape
    z1, z2 = rest[:n_sub], rest[n_sub : 2 * n_sub]
    per_row = lanes // rhs
    n_rows = info.shape[1]
    first = [info[quarter] for quarter in range(n_sub)]
    total = list(first)
    for block in range(1, info.shape[0] // n_sub):
        for quarter in range(n_sub):
            total[quarter] = total[quarter] + info[block * n_sub + quarter]
    known = [jnp.concatenate([f[r : r + 1] for f in first], axis=0) for r in range(n_rows)]
    added = [jnp.concatenate([t[r : r + 1] for t in total], axis=0) for r in range(n_rows)]
    values = []
    for index in range(10):
        source = (added if index < 4 else known)[index // per_row]
        shift = rhs * (index % per_row)
        values.append(pltpu.roll(source, lanes - shift, 1) if shift else source)
    scale, y0, y1, y2 = weigh(values)
    h00, h10, h01, h11, h21 = values[5:]
    gamma = y2 / h21
    both = (y1 - gamma * h11) / h10
    coeffs = [(y0 - both * h00 - gamma * h01) * scale, both * scale, gamma]
    flipped = jnp.concatenate(coeffs, axis=0)
    spare = -flipped.shape[0] % 8
    if spare:
        flipped = jnp.concatenate([flipped, jnp.zeros((spare, lanes), F32)], axis=0)
    flipped = flipped.T
    for index in range(3 * n_sub):
        factor[index] = jnp.broadcast_to(flipped[:rhs, index : index + 1], (rhs, lanes))
    for k in range(n_sub):
        quarter = ids[2] ^ k
        alpha, beta, gamma = (factor[part * n_sub + quarter] for part in range(3))
        start = pl.multiple_of(quarter * rhs, 8)
        for pair in range(per_part):
            mixed = alpha * turned[quarter, pair] + beta * z1[k][pair]
            stack[pair, pl.ds(start, rhs), :] = mixed + gamma * z2[k][pair]
    for pair in range(per_part):
        both = stack[pair].T
        out[2 * pair] = both[:dof]
        out[2 * pair + 1] = both[dof:]


def per_device(coarse_op, right_side, owner_map, neighbor_table):
    nz = lax.axis_size("z")
    n_sub = lax.axis_size("sub")
    per_dev, dof, width = coarse_op.shape
    terms = width // dof
    hops = terms - 1
    rhs = right_side.shape[2] // n_sub
    n_loc = n_sub * per_dev
    n_own = n_loc // 2
    me_z, me_c, me_s = lax.axis_index("z"), lax.axis_index("core"), lax.axis_index("sub")
    ids = jnp.stack([me_z, me_c, me_s]).astype(jnp.int32)
    even = per_dev % 2 == 0
    lanes = 2 * dof
    field = (n_own, rhs, lanes)

    relay = n_sub == 4 and per_dev % 4 == 0 and terms % 2 == 1
    order = jnp.arange(n_sub, dtype=jnp.int32) ^ me_s
    hops_to = [[(s, s ^ k) for s in range(n_sub)] for k in range(n_sub)]
    half = per_dev // 2
    if relay:
        halves = [jax.ShapeDtypeStruct((half // 2, dof, 2 * width), F32)] * 2
        op_low, op_high, turned = pl.pallas_call(
            functools.partial(pack_kernel, dof),
            out_shape=halves + [jax.ShapeDtypeStruct((n_sub, half, rhs, lanes), F32)],
            in_specs=[HBM, HBM],
            out_specs=[VMEM] * 3,
            scratch_shapes=[
                pltpu.VMEM(right_side.shape, F32),
                pltpu.VMEM((2, half, dof, width), F32),
                pltpu.SemaphoreType.DMA((3,)),
            ],
            compiler_params=SMALL,
            name="pack",
        )(coarse_op, right_side)
        x_high = lax.ppermute(op_high, "sub", hops_to[1])
        y_low = lax.ppermute(op_low, "sub", hops_to[2])
        x_low = lax.ppermute(op_low, "sub", hops_to[1])
        y_high = lax.ppermute(op_high, "sub", hops_to[2])

    positions = pl.pallas_call(
        functools.partial(position_kernel, (per_dev, n_sub, nz, hops)),
        out_shape=jax.ShapeDtypeStruct((n_loc * terms,), jnp.int32),
        in_specs=[SMEM, SMEM, SMEM],
        out_specs=SMEM,
        scratch_shapes=[pltpu.SMEM((owner_map.shape[0],), jnp.int32)],
        compiler_params=SMALL,
        name="positions",
    )(ids, owner_map, neighbor_table.reshape(-1))

    if not relay:
        turned = right_side.reshape(per_dev, dof, n_sub, rhs).transpose(2, 0, 3, 1)
    if even and not relay:
        turned = turned.reshape(n_sub, per_dev // 2, 2, rhs, dof).transpose(0, 1, 3, 2, 4)
        turned = turned.reshape(n_sub, per_dev // 2, rhs, lanes)
    mine = lax.all_to_all(turned, "sub", split_axis=0, concat_axis=0, tiled=True)
    mine = mine[order]
    if not even:
        mine = mine.reshape(n_own, 2, rhs, dof).transpose(0, 2, 1, 3)
    b_mine = mine.reshape(field)

    swap = [(c, c ^ 1) for c in range(CORES)]

    def step_z(own, offset):
        return lax.ppermute(own, "z", [(z, z ^ offset) for z in range(nz)])

    def gather(own):
        direct = (2, 1) if nz == 4 else range(1, nz)
        found = {offset: step_z(own, offset) for offset in direct}
        if nz == 4:
            found[3] = step_z(found[2], 1)
        parts = [own] + [found[offset] for offset in range(1, nz)]
        return parts + [lax.ppermute(part, "core", swap) for part in parts]

    if relay:
        d_low = lax.ppermute(y_low, "sub", hops_to[1])
        d_high = lax.ppermute(x_high, "sub", hops_to[2])
        stages = [[op_low, op_high, x_low, x_high, y_low, y_high], [d_low, d_high]]
    if not relay:
        every = lax.all_gather(coarse_op, "sub", axis=0)[order]
        stages = [[every[k] for k in range(n_sub)]]
    b_parts = gather(b_mine)
    n_field = len(b_parts)
    dup = (CORES * nz * n_loc, rhs, lanes)
    full = (CORES * nz * n_own,) + field[1:]
    small = jax.ShapeDtypeStruct(field[1:], F32)
    own_shape = jax.ShapeDtypeStruct(field, F32)
    sends = n_sub if even else 0
    share = [jax.ShapeDtypeStruct((per_dev // 2, rhs, lanes), F32)] * sends

    def split_shape(sites):
        return jax.ShapeDtypeStruct((sites, 2 * dof, width), BF16)

    ops = stages[0]
    rows = sum(op.shape[0] * op.shape[2] // width for op in ops)
    z1, split, spread_b = pl.pallas_call(
        functools.partial(first_kernel, n_field, len(ops), dof, terms),
        out_shape=[
            jax.ShapeDtypeStruct((rows // 2,) + field[1:], F32),
            split_shape(rows),
            jax.ShapeDtypeStruct(dup, F32),
        ],
        in_specs=[SMEM] + [VMEM] * n_field + [ANY] * len(ops),
        out_specs=[VMEM] * 3,
        scratch_shapes=[pltpu.VMEM(op.shape, F32) for op in ops]
        + [pltpu.SemaphoreType.DMA((len(ops),))],
        compiler_params=PARAMS,
        name="first",
    )(positions, *b_parts, *ops)
    splits, shares1 = [split], []
    if relay:
        ops = stages[1]
        z1, split, *shares1 = pl.pallas_call(
            functools.partial(more_kernel, len(ops), dof, terms),
            out_shape=[own_shape, split_shape(n_loc - rows)] + share,
            in_specs=[SMEM, VMEM, VMEM] + [VMEM] * len(ops),
            out_specs=[VMEM] * (2 + sends),
            compiler_params=PARAMS,
            name="more",
        )(positions, spread_b, z1, *ops)
        splits.append(split)
    elif even:
        shares1 = [z1[k * per_dev // 2 : (k + 1) * per_dev // 2] for k in range(n_sub)]
    count = len(splits)

    def send(shares):
        return shares[:1] + [lax.ppermute(shares[k], "sub", hops_to[k]) for k in range(1, sends)]

    z1_parts = gather(z1)
    shares1 = send(shares1)

    z2, basis, v1_mine, coeffs, *shares2 = pl.pallas_call(
        functools.partial(second_kernel, n_field, count, sends, dof, terms),
        out_shape=[own_shape, jax.ShapeDtypeStruct(full, F32), own_shape, small] + share,
        in_specs=[SMEM] + [VMEM] * (2 * n_field + count),
        out_specs=[VMEM] * (4 + sends),
        scratch_shapes=[pltpu.VMEM(dup, F32)],
        compiler_params=PARAMS,
        name="second",
    )(positions, *b_parts, *z1_parts, *splits)
    z2_parts = gather(z2)
    shares2 = send(shares2)
    z2_parts, shares1, shares2 = lax.optimization_barrier((z2_parts, shares1, shares2))

    axes = ("z", "core", "sub") if even else ("z", "core")
    copies = nz * CORES * (n_sub if even else 1)
    note = (pl.cdiv(10 * rhs, lanes), lanes) if even else field[1:]
    sums, v2_mine = pl.pallas_call(
        functools.partial(third_kernel, n_field, count, dof, terms),
        out_shape=[jax.ShapeDtypeStruct((copies,) + note, F32), own_shape],
        in_specs=[SMEM] + [VMEM] * (3 + 2 * n_field + count),
        out_specs=[VMEM] * 2,
        scratch_shapes=[pltpu.VMEM(dup, F32), pltpu.VMEM(full, F32), pltpu.VMEM(field, F32)],
        compiler_params=PARAMS,
        name="third",
    )(positions, basis, v1_mine, coeffs, *b_parts, *z2_parts, *splits)
    sums = lax.all_to_all(sums, axes, split_axis=0, concat_axis=0, tiled=True)

    if even:
        return pl.pallas_call(
            functools.partial(finish_kernel, dof),
            out_shape=jax.ShapeDtypeStruct(right_side.shape, F32),
            in_specs=[SMEM] + [VMEM] * (2 + 2 * sends),
            out_specs=VMEM,
            scratch_shapes=[
                pltpu.VMEM((per_dev // 2, n_sub * rhs, lanes), F32),
                pltpu.VMEM((3 * n_sub, rhs, lanes), F32),
            ],
            compiler_params=SMALL,
            name="finish",
        )(ids, sums, turned, *shares1, *shares2)
    result = pl.pallas_call(
        combine_kernel,
        out_shape=own_shape,
        in_specs=[VMEM] * 4,
        out_specs=VMEM,
        compiler_params=SMALL,
            name="combine",
    )(sums, b_mine, v1_mine, v2_mine)
    result = result.reshape(n_own, rhs, 2, dof).transpose(0, 2, 1, 3)
    result = result.reshape(n_sub, per_dev, rhs, dof)[order]
    result = lax.all_to_all(result, "sub", split_axis=0, concat_axis=0, tiled=True)
    return result.transpose(1, 3, 0, 2).reshape(right_side.shape)


def solution(mesh):
    n_grp, n_sub = mesh.shape["grp"], mesh.shape["sub"]
    inner = Mesh(mesh.devices.reshape(n_grp // CORES, CORES, n_sub), ("z", "core", "sub"))
    split = P(("z", "core", "sub"), None, None)

    return jax.shard_map(
        per_device,
        mesh=inner,
        in_specs=(split, split, P(), P()),
        out_specs=split,
        check_vma=False,
    )
```

```python
import functools

import jax
import jax.numpy as jnp
from jax import lax
from jax.experimental import pallas as pl
from jax.experimental.pallas import tpu as pltpu
from jax.sharding import Mesh
from jax.sharding import PartitionSpec as P


F32 = jnp.float32
BF16 = jnp.bfloat16
CORES = 2
VMEM = pl.BlockSpec(memory_space=pltpu.VMEM)
SMEM = pl.BlockSpec(memory_space=pltpu.SMEM)
HBM = pl.BlockSpec(memory_space=pltpu.HBM)
ANY = pl.BlockSpec(memory_space=pl.ANY)
PARAMS = pltpu.CompilerParams(vmem_limit_bytes=20 * 1024 * 1024)
SMALL = pltpu.CompilerParams(vmem_limit_bytes=4 * 1024 * 1024)


def divide(value, size):
    if size & (size - 1):
        return lax.div(value, jnp.int32(size))
    return lax.shift_right_logical(value, jnp.int32(size.bit_length() - 1))


def remain(value, size):
    if size & (size - 1):
        return lax.rem(value, jnp.int32(size))
    return value & (size - 1)


def low_half(shape, dof):
    return lax.broadcasted_iota(jnp.int32, shape, 1) < dof


def lane_sum(values):
    return jnp.sum(values, axis=1, keepdims=True)


def split_bf16(values):
    high = values.astype(BF16)
    return high, (values - high.astype(F32)).astype(BF16)


def place(columns, shape):
    lane = lax.broadcasted_iota(jnp.int32, shape, 1)
    packed = jnp.zeros(shape, F32)
    for index, column in enumerate(columns):
        packed = jnp.where(lane == index, column, packed)
    return packed


def dense_rows(columns, shape, rows):
    size, lanes = shape
    per_row = lanes // size
    flipped = place(columns, shape).T
    lane = lax.broadcasted_iota(jnp.int32, (1, lanes), 1)
    wide = jnp.concatenate([flipped] * per_row, axis=1)
    packed = []
    for row in range(rows):
        line = jnp.zeros((1, lanes), F32)
        for inner in range(per_row):
            index = row * per_row + inner
            if index < len(columns):
                line = jnp.where(divide(lane, size) == inner, wide[index : index + 1], line)
        packed.append(line)
    return jnp.concatenate(packed, axis=0)


def position_kernel(geometry, ids, owner, table, out, where):
    per_dev, n_sub, nz, hops = geometry
    me_z, me_c, me_s = ids[0], ids[1], ids[2]
    sites = owner.shape[0]

    def locate(slot):
        dev = divide(slot, per_dev)
        grp = divide(dev, n_sub)
        block = (remain(grp, CORES) ^ me_c) * nz + (divide(grp, CORES) ^ me_z)
        return (block * n_sub + (remain(dev, n_sub) ^ me_s)) * per_dev + remain(slot, per_dev)

    def fill(slot, carry):
        where[owner[slot]] = locate(slot)
        return carry

    lax.fori_loop(0, sites, fill, 0, unroll=8)

    def look(local, carry):
        dev = (me_z * CORES + me_c) * n_sub + (divide(local, per_dev) ^ me_s)
        slot = dev * per_dev + remain(local, per_dev)
        base = owner[slot] * hops
        out[local * (hops + 1)] = locate(slot)
        for hop in range(hops):
            out[local * (hops + 1) + 1 + hop] = where[table[base + hop]]
        return carry

    lax.fori_loop(0, n_sub * per_dev, look, 0, unroll=2)


def pack_kernel(dof, op, right, low, high, turned, kept, held, op_held, sems):
    half = op.shape[0] // 2
    sources = [right, op.at[pl.ds(0, half)], op.at[pl.ds(half, half)]]
    copies = start_copies(sources, [held, op_held.at[0], op_held.at[1]], sems)
    n_sub, per_part, rhs = turned.shape[0], turned.shape[1], turned.shape[2]
    copies[0].wait()
    for pair in range(per_part):
        both = jnp.concatenate([held[2 * pair], held[2 * pair + 1]], axis=0).T
        for quarter in range(n_sub):
            turned[quarter, pair] = both[quarter * rhs : (quarter + 1) * rhs]
            kept[quarter, pair] = both[quarter * rhs : (quarter + 1) * rhs]
    main = op.shape[2] - dof
    for index, target in enumerate((low, high)):
        copies[index + 1].wait()
        for pair in range(half // 2):
            even, odd = op_held[index, 2 * pair], op_held[index, 2 * pair + 1]
            target[pair, :, :main] = even[:, :main]
            target[pair, :, main : 2 * main] = odd[:, :main]
            target[pair, :, 2 * main :] = jnp.concatenate([even[:, main:], odd[:, main:]], axis=1)


def spread(dup, pair, values, dof):
    mask = low_half(values.shape, dof)
    rolled = pltpu.roll(values, dof, 1)
    dup[2 * pair] = jnp.where(mask, values, rolled)
    dup[2 * pair + 1] = jnp.where(mask, rolled, values)


def site_vector(local, pos, dup, terms, dof):
    mask = low_half((dup.shape[1], 2 * dof), dof)
    tiles = []
    for first in range(0, terms - 1, 2):
        left = dup[pos[local * terms + first]]
        right = dup[pos[local * terms + first + 1]]
        tiles.append(jnp.where(mask, left, right))
    if terms % 2:
        tiles.append(dup[pos[local * terms + terms - 1]][:, :dof])
    return list(split_bf16(jnp.concatenate(tiles, axis=1)))


def row_pairs(op, pair, dof):
    if op.shape[1] == 2 * dof:
        return op[pair, :dof], op[pair, dof:]
    main = op.shape[2] // 2 - dof
    rows = op[pair]
    tail = rows[:, 2 * main :]
    even = jnp.concatenate([rows[:, :main], tail[:, :dof]], axis=1)
    odd = jnp.concatenate([rows[:, main : 2 * main], tail[:, dof:]], axis=1)
    return even, odd


def to_columns(even, odd):
    width, lanes = even.shape[1], 2 * even.shape[0]
    pieces = []
    for start in range(0, width, lanes):
        stop = min(start + lanes, width)
        pieces.append(jnp.concatenate([even[:, start:stop], odd[:, start:stop]], axis=0).T)
    return jnp.concatenate(split_bf16(jnp.concatenate(pieces, axis=0)), axis=1)


def pair_product(columns, local, pos, dup, terms, dof):
    rows, lanes = dup.shape[1], 2 * dof
    vectors = [v for i in range(2) for v in site_vector(local + i, pos, dup, terms, dof)]
    product = lax.dot_general(
        jnp.concatenate(vectors, axis=0),
        columns,
        (((1,), (0,)), ((), ())),
        preferred_element_type=F32,
    )
    product = product[:, :lanes] + product[:, lanes:]
    even = product[:rows] + product[rows : 2 * rows]
    odd = product[2 * rows : 3 * rows] + product[3 * rows :]
    return jnp.where(low_half(even.shape, dof), even, odd)


def rows_product(pair_rows, local, pos, dup, terms, dof):
    rows = dup.shape[1]
    halves = []
    for i, op in enumerate(pair_rows):
        product = lax.dot_general(
            jnp.concatenate(site_vector(local + i, pos, dup, terms, dof), axis=0),
            jnp.concatenate(split_bf16(op), axis=0),
            (((1,), (1,)), ((), ())),
            preferred_element_type=F32,
        )
        total = product[:rows] + product[rows:]
        halves.append(total + pltpu.roll(total, dof, 1))
    return jnp.where(low_half(halves[0].shape, dof), halves[0], halves[1])


def apply_rows(stages, pos, dup, terms, dof, put):
    base = 0
    for stage in stages:
        for pair in range(stage.shape[0]):
            columns = stage[pair]
            put(base + pair, pair_product(columns, 2 * (base + pair), pos, dup, terms, dof))
        base += stage.shape[0]


def start_copies(sources, targets, sems):
    copies = [
        pltpu.make_async_copy(source, target, sems.at[index])
        for index, (source, target) in enumerate(zip(sources, targets))
    ]
    for copy in copies:
        copy.start()
    return copies


def over_pairs(fields, step, init):
    n_pair = fields[0].shape[0]
    for block in range(len(fields)):
        init = lax.fori_loop(
            0, n_pair, lambda pair, carry, block=block: step(block, pair, carry), init, unroll=16
        )
    return init


def share_out(values, shares):
    for index, share in enumerate(shares):
        for inner in range(share.shape[0]):
            share[inner] = values[index * share.shape[0] + inner]


def first_kernel(n_field, count, dof, terms, pos, *rest):
    fields, ops, rest = rest[:n_field], rest[n_field : n_field + count], rest[n_field + count :]
    out, split, dup = rest[:3]
    held, sems = rest[3 : count + 3], rest[count + 3]
    copies = start_copies(ops, held, sems)
    n_pair = fields[0].shape[0]

    def build(block, pair, carry):
        spread(dup, block * n_pair + pair, fields[block][pair], dof)
        return carry

    over_pairs(fields, build, 0)
    for copy in copies:
        copy.wait()

    def put(pair, values):
        out[pair] = values

    base = 0
    for op in held:
        for inner in range(op.shape[0]):
            columns = to_columns(*row_pairs(op, inner, dof))
            split[base] = columns
            put(base, pair_product(columns, 2 * base, pos, dup, terms, dof))
            base += 1


def more_kernel(count, dof, terms, pos, dup, before, *rest):
    ops, out, shares = rest[:count], rest[count], rest[count + 1 :]
    base = before.shape[0]
    for pair in range(base):
        out[pair] = before[pair]
    for op in ops:
        for inner in range(op.shape[0]):
            out[base] = rows_product(row_pairs(op, inner, dof), 2 * base, pos, dup, terms, dof)
            base += 1
    share_out(out, shares)


def turn_kernel(count, dof, *rest):
    ops, split = rest[:count], rest[count]
    base = 0
    for op in ops:
        for inner in range(op.shape[0]):
            split[base] = to_columns(*row_pairs(op, inner, dof))
            base += 1


def second_kernel(n_field, count, sends, dof, terms, pos, *rest):
    b_ref, z_ref, rest = rest[:n_field], rest[n_field : 2 * n_field], rest[2 * n_field :]
    stages, (out, basis, coeffs) = rest[:count], rest[count : count + 3]
    shares, dup = rest[count + 3 : count + 3 + sends], rest[count + 3 + sends]
    n_pair = b_ref[0].shape[0]
    shape = b_ref[0].shape[1:]
    zero = jnp.zeros(shape, F32)

    def dots(block, pair, carry):
        b, z = b_ref[block][pair], z_ref[block][pair]
        return carry[0] + b * b, carry[1] + b * z

    norm, cross = over_pairs(b_ref, dots, (zero, zero))
    beta = jnp.sqrt(lane_sum(norm))
    scale = 1.0 / beta
    h00 = lane_sum(cross) * scale * scale

    def remove(block, pair, carry):
        w = z_ref[block][pair] * scale - (h00 * scale) * b_ref[block][pair]
        basis[block * n_pair + pair] = w
        return carry + w * w

    h10 = jnp.sqrt(lane_sum(over_pairs(b_ref, remove, zero)))
    unit = 1.0 / h10

    def build(block, pair, carry):
        v = basis[block * n_pair + pair] * unit
        basis[block * n_pair + pair] = v
        spread(dup, block * n_pair + pair, v, dof)
        return carry

    over_pairs(b_ref, build, 0)
    coeffs[...] = place([beta, h00, h10], shape)

    def put(pair, values):
        out[pair] = values

    apply_rows(stages, pos, dup, terms, dof, put)
    share_out(out, shares)


def third_kernel(n_field, count, dof, terms, pos, basis, coeffs, *rest):
    b_ref, z_ref, rest = rest[:n_field], rest[n_field : 2 * n_field], rest[2 * n_field :]
    stages, (sums, work, dup, image) = rest[:count], rest[count:]
    b_mine = b_ref[0]
    n_pair = b_mine.shape[0]
    shape = b_mine.shape[1:]
    zero = jnp.zeros(shape, F32)
    known = coeffs[...]
    scale = 1.0 / known[:, 0:1]

    def dots(block, pair, carry):
        z = z_ref[block][pair]
        return carry[0] + b_ref[block][pair] * z, carry[1] + basis[block * n_pair + pair] * z

    first, second = over_pairs(b_ref, dots, (zero, zero))
    h01 = lane_sum(first) * scale
    h11 = lane_sum(second)

    def remove(block, pair, carry):
        w = (
            z_ref[block][pair]
            - (h01 * scale) * b_ref[block][pair]
            - h11 * basis[block * n_pair + pair]
        )
        work[block * n_pair + pair] = w
        return carry + w * w

    h21 = jnp.sqrt(lane_sum(over_pairs(b_ref, remove, zero)))
    unit = 1.0 / h21

    def build(block, pair, carry):
        v = work[block * n_pair + pair] * unit
        work[block * n_pair + pair] = v
        spread(dup, block * n_pair + pair, v, dof)
        return carry

    over_pairs(b_ref, build, 0)

    def put(pair, values):
        image[pair] = values

    apply_rows(stages, pos, dup, terms, dof, put)

    def last(pair, carry):
        u = image[pair]
        return (
            carry[0] + b_mine[pair] * u,
            carry[1] + basis[pair] * u,
            carry[2] + work[pair] * u,
            carry[3] + u * u,
        )

    parts = lax.fori_loop(0, n_pair, last, (zero, zero, zero, zero), unroll=True)
    solved = [known[:, 0:1], known[:, 1:2], known[:, 2:3], h01, h11, h21]
    columns = [lane_sum(part) for part in parts] + solved
    if len(sums.shape) == 3 and sums.shape[1:] == shape:
        packed = place(columns, shape)
    else:
        packed = dense_rows(columns, shape, sums.shape[1])
    for block in range(sums.shape[0]):
        sums[block] = packed


def weigh(values):
    d02, h12, h22, g22, beta, h00, h10, h01, h11, h21 = values
    scale = 1.0 / beta
    h02 = d02 * scale
    g00 = h00 * h00 + h10 * h10
    g01 = h00 * h01 + h10 * h11
    g02 = h00 * h02 + h10 * h12
    g11 = h01 * h01 + h11 * h11 + h21 * h21
    g12 = h01 * h02 + h11 * h12 + h21 * h22
    inv0 = 1.0 / g00
    l10 = g01 * inv0
    l20 = g02 * inv0
    d1 = g11 - l10 * g01
    e21 = g12 - l20 * g01
    inv1 = 1.0 / d1
    l21 = e21 * inv1
    d2 = g22 - l20 * g02 - l21 * e21
    r0 = beta * h00
    r1 = beta * h01 - l10 * r0
    r2 = beta * h02 - l20 * r0 - l21 * r1
    y2 = r2 / d2
    y1 = r1 * inv1 - l21 * y2
    y0 = r0 * inv0 - l10 * y1 - l20 * y2
    return scale, y0, y1, y2


def combine_kernel(sums, b_mine, v1_mine, v2_mine, out):
    total = sums[0]
    for block in range(1, sums.shape[0]):
        total = total + sums[block]
    known = sums[0]
    values = [(total if i < 4 else known)[:, i : i + 1] for i in range(10)]
    scale, y0, y1, y2 = weigh(values)
    for pair in range(b_mine.shape[0]):
        out[pair] = (y0 * scale) * b_mine[pair] + y1 * v1_mine[pair] + y2 * v2_mine[pair]


def finish_kernel(dof, ids, info, turned, *rest):
    out, stack, factor = rest[-3:]
    n_sub, per_part, rhs, lanes = turned.shape
    z1, z2 = rest[:n_sub], rest[n_sub : 2 * n_sub]
    per_row = lanes // rhs
    n_rows = info.shape[1]
    first = [info[quarter] for quarter in range(n_sub)]
    total = list(first)
    for block in range(1, info.shape[0] // n_sub):
        for quarter in range(n_sub):
            total[quarter] = total[quarter] + info[block * n_sub + quarter]
    known = [jnp.concatenate([f[r : r + 1] for f in first], axis=0) for r in range(n_rows)]
    added = [jnp.concatenate([t[r : r + 1] for t in total], axis=0) for r in range(n_rows)]
    values = []
    for index in range(10):
        source = (added if index < 4 else known)[index // per_row]
        shift = rhs * (index % per_row)
        values.append(pltpu.roll(source, lanes - shift, 1) if shift else source)
    scale, y0, y1, y2 = weigh(values)
    h00, h10, h01, h11, h21 = values[5:]
    gamma = y2 / h21
    both = (y1 - gamma * h11) / h10
    coeffs = [(y0 - both * h00 - gamma * h01) * scale, both * scale, gamma]
    flipped = jnp.concatenate(coeffs, axis=0)
    spare = -flipped.shape[0] % 8
    if spare:
        flipped = jnp.concatenate([flipped, jnp.zeros((spare, lanes), F32)], axis=0)
    flipped = flipped.T
    for index in range(3 * n_sub):
        factor[index] = jnp.broadcast_to(flipped[:rhs, index : index + 1], (rhs, lanes))
    for k in range(n_sub):
        quarter = ids[2] ^ k
        alpha, beta, gamma = (factor[part * n_sub + quarter] for part in range(3))
        start = pl.multiple_of(quarter * rhs, 8)
        for pair in range(per_part):
            mixed = alpha * turned[quarter, pair] + beta * z1[k][pair]
            stack[pair, pl.ds(start, rhs), :] = mixed + gamma * z2[k][pair]
    for pair in range(per_part):
        both = stack[pair].T
        out[2 * pair] = both[:dof]
        out[2 * pair + 1] = both[dof:]


def per_device(coarse_op, right_side, owner_map, neighbor_table):
    nz = lax.axis_size("z")
    n_sub = lax.axis_size("sub")
    per_dev, dof, width = coarse_op.shape
    terms = width // dof
    hops = terms - 1
    rhs = right_side.shape[2] // n_sub
    n_loc = n_sub * per_dev
    n_own = n_loc // 2
    me_z, me_c, me_s = lax.axis_index("z"), lax.axis_index("core"), lax.axis_index("sub")
    ids = jnp.stack([me_z, me_c, me_s]).astype(jnp.int32)
    even = per_dev % 2 == 0
    lanes = 2 * dof
    field = (n_own, rhs, lanes)

    relay = n_sub == 4 and per_dev % 4 == 0 and terms % 2 == 1
    order = jnp.arange(n_sub, dtype=jnp.int32) ^ me_s
    hops_to = [[(s, s ^ k) for s in range(n_sub)] for k in range(n_sub)]
    half = per_dev // 2
    if relay:
        halves = [jax.ShapeDtypeStruct((half // 2, dof, 2 * width), F32)] * 2
        op_low, op_high, turned, kept = pl.pallas_call(
            functools.partial(pack_kernel, dof),
            out_shape=halves + [jax.ShapeDtypeStruct((n_sub, half, rhs, lanes), F32)] * 2,
            in_specs=[HBM, HBM],
            out_specs=[VMEM] * 4,
            scratch_shapes=[
                pltpu.VMEM(right_side.shape, F32),
                pltpu.VMEM((2, half, dof, width), F32),
                pltpu.SemaphoreType.DMA((3,)),
            ],
            compiler_params=SMALL,
            name="pack",
        )(coarse_op, right_side)
        x_high = lax.ppermute(op_high, "sub", hops_to[1])
        y_low = lax.ppermute(op_low, "sub", hops_to[2])
        x_low = lax.ppermute(op_low, "sub", hops_to[1])
        y_high = lax.ppermute(op_high, "sub", hops_to[2])

    positions = pl.pallas_call(
        functools.partial(position_kernel, (per_dev, n_sub, nz, hops)),
        out_shape=jax.ShapeDtypeStruct((n_loc * terms,), jnp.int32),
        in_specs=[SMEM, SMEM, SMEM],
        out_specs=SMEM,
        scratch_shapes=[pltpu.SMEM((owner_map.shape[0],), jnp.int32)],
        compiler_params=SMALL,
        name="positions",
    )(ids, owner_map, neighbor_table.reshape(-1))

    if not relay:
        turned = right_side.reshape(per_dev, dof, n_sub, rhs).transpose(2, 0, 3, 1)
    if even and not relay:
        turned = turned.reshape(n_sub, per_dev // 2, 2, rhs, dof).transpose(0, 1, 3, 2, 4)
        turned = turned.reshape(n_sub, per_dev // 2, rhs, lanes)
    if not relay:
        kept = turned
    mine = lax.all_to_all(turned, "sub", split_axis=0, concat_axis=0, tiled=True)
    mine = mine[order]
    if not even:
        mine = mine.reshape(n_own, 2, rhs, dof).transpose(0, 2, 1, 3)
    b_mine = mine.reshape(field)

    swap = [(c, c ^ 1) for c in range(CORES)]

    def step_z(own, offset):
        return lax.ppermute(own, "z", [(z, z ^ offset) for z in range(nz)])

    def gather(own):
        direct = (2, 1) if nz == 4 else range(1, nz)
        found = {offset: step_z(own, offset) for offset in direct}
        if nz == 4:
            found[3] = step_z(found[2], 1)
        parts = [own] + [found[offset] for offset in range(1, nz)]
        return parts + [lax.ppermute(part, "core", swap) for part in parts]

    if relay:
        d_low = lax.ppermute(y_low, "sub", hops_to[1])
        d_high = lax.ppermute(x_high, "sub", hops_to[2])
        stages = [[op_low, op_high, x_low, x_high, y_low, y_high], [d_low, d_high]]
    if not relay:
        every = lax.all_gather(coarse_op, "sub", axis=0)[order]
        stages = [[every.reshape(n_own, 2 * dof, width)]]
    b_parts = gather(b_mine)
    n_field = len(b_parts)
    dup = (CORES * nz * n_loc, rhs, lanes)
    full = (CORES * nz * n_own,) + field[1:]
    small = jax.ShapeDtypeStruct(field[1:], F32)
    own_shape = jax.ShapeDtypeStruct(field, F32)
    sends = n_sub if even else 0
    share = [jax.ShapeDtypeStruct((per_dev // 2, rhs, lanes), F32)] * sends

    def split_shape(pairs):
        return jax.ShapeDtypeStruct((pairs, width, 4 * dof), BF16)

    ops = stages[0]
    done = sum(op.shape[0] for op in ops)
    z1, split, spread_b = pl.pallas_call(
        functools.partial(first_kernel, n_field, len(ops), dof, terms),
        out_shape=[
            jax.ShapeDtypeStruct((done,) + field[1:], F32),
            split_shape(done),
            jax.ShapeDtypeStruct(dup, F32),
        ],
        in_specs=[SMEM] + [VMEM] * n_field + [ANY] * len(ops),
        out_specs=[VMEM] * 3,
        scratch_shapes=[pltpu.VMEM(op.shape, F32) for op in ops]
        + [pltpu.SemaphoreType.DMA((len(ops),))],
        compiler_params=PARAMS,
        name="first",
    )(positions, *b_parts, *ops)
    splits, shares1 = [split], []
    if relay:
        ops = stages[1]
        z1, *shares1 = pl.pallas_call(
            functools.partial(more_kernel, len(ops), dof, terms),
            out_shape=[own_shape] + share,
            in_specs=[SMEM, VMEM, VMEM] + [VMEM] * len(ops),
            out_specs=[VMEM] * (1 + sends),
            compiler_params=PARAMS,
            name="more",
        )(positions, spread_b, z1, *ops)
        split = pl.pallas_call(
            functools.partial(turn_kernel, len(ops), dof),
            out_shape=split_shape(n_own - done),
            in_specs=[VMEM] * len(ops),
            out_specs=VMEM,
            compiler_params=PARAMS,
            name="turn",
        )(*ops)
        splits.append(split)
    elif even:
        shares1 = [z1[k * per_dev // 2 : (k + 1) * per_dev // 2] for k in range(n_sub)]
    count = len(splits)

    def send(shares):
        return shares[:1] + [lax.ppermute(shares[k], "sub", hops_to[k]) for k in range(1, sends)]

    z1_parts = gather(z1)
    shares1 = send(shares1)

    z2, basis, coeffs, *shares2 = pl.pallas_call(
        functools.partial(second_kernel, n_field, count, sends, dof, terms),
        out_shape=[own_shape, jax.ShapeDtypeStruct(full, F32), small] + share,
        in_specs=[SMEM] + [VMEM] * (2 * n_field + count),
        out_specs=[VMEM] * (3 + sends),
        scratch_shapes=[pltpu.VMEM(dup, F32)],
        compiler_params=PARAMS,
        name="second",
    )(positions, *b_parts, *z1_parts, *splits)
    z2_parts = gather(z2)
    shares2 = send(shares2)
    z2_parts, shares1, shares2 = lax.optimization_barrier((z2_parts, shares1, shares2))

    axes = ("z", "core", "sub") if even else ("z", "core")
    copies = nz * CORES * (n_sub if even else 1)
    note = (pl.cdiv(10 * rhs, lanes), lanes) if even else field[1:]
    keep = [] if even else [jax.ShapeDtypeStruct(full, F32)]
    sums, *work = pl.pallas_call(
        functools.partial(third_kernel, n_field, count, dof, terms),
        out_shape=[jax.ShapeDtypeStruct((copies,) + note, F32)] + keep,
        in_specs=[SMEM] + [VMEM] * (2 + 2 * n_field + count),
        out_specs=[VMEM] * (1 + len(keep)),
        scratch_shapes=[pltpu.VMEM(full, F32)] * (1 - len(keep))
        + [pltpu.VMEM(dup, F32), pltpu.VMEM(field, F32)],
        compiler_params=PARAMS,
        name="third",
    )(positions, basis, coeffs, *b_parts, *z2_parts, *splits)
    sums = lax.all_to_all(sums, axes, split_axis=0, concat_axis=0, tiled=True)

    if even:
        return pl.pallas_call(
            functools.partial(finish_kernel, dof),
            out_shape=jax.ShapeDtypeStruct(right_side.shape, F32),
            in_specs=[SMEM] + [VMEM] * (2 + 2 * sends),
            out_specs=VMEM,
            scratch_shapes=[
                pltpu.VMEM((per_dev // 2, n_sub * rhs, lanes), F32),
                pltpu.VMEM((3 * n_sub, rhs, lanes), F32),
            ],
            compiler_params=SMALL,
            name="finish",
        )(ids, sums, kept, *shares1, *shares2)
    result = pl.pallas_call(
        combine_kernel,
        out_shape=own_shape,
        in_specs=[VMEM] * 4,
        out_specs=VMEM,
        compiler_params=SMALL,
            name="combine",
    )(sums, b_mine, basis[:n_own], work[0][:n_own])
    result = result.reshape(n_own, rhs, 2, dof).transpose(0, 2, 1, 3)
    result = result.reshape(n_sub, per_dev, rhs, dof)[order]
    result = lax.all_to_all(result, "sub", split_axis=0, concat_axis=0, tiled=True)
    return result.transpose(1, 3, 0, 2).reshape(right_side.shape)


def solution(mesh):
    n_grp, n_sub = mesh.shape["grp"], mesh.shape["sub"]
    inner = Mesh(mesh.devices.reshape(n_grp // CORES, CORES, n_sub), ("z", "core", "sub"))
    split = P(("z", "core", "sub"), None, None)

    return jax.shard_map(
        per_device,
        mesh=inner,
        in_specs=(split, split, P(), P()),
        out_specs=split,
        check_vma=False,
    )
```

```python
import functools

import jax
import jax.numpy as jnp
from jax import lax
from jax.experimental import pallas as pl
from jax.experimental.pallas import tpu as pltpu
from jax.sharding import Mesh
from jax.sharding import PartitionSpec as P


F32 = jnp.float32
BF16 = jnp.bfloat16
CORES = 2
VMEM = pl.BlockSpec(memory_space=pltpu.VMEM)
SMEM = pl.BlockSpec(memory_space=pltpu.SMEM)
HBM = pl.BlockSpec(memory_space=pltpu.HBM)
ANY = pl.BlockSpec(memory_space=pl.ANY)
PARAMS = pltpu.CompilerParams(vmem_limit_bytes=20 * 1024 * 1024)
SMALL = pltpu.CompilerParams(vmem_limit_bytes=4 * 1024 * 1024)


def divide(value, size):
    if size & (size - 1):
        return lax.div(value, jnp.int32(size))
    return lax.shift_right_logical(value, jnp.int32(size.bit_length() - 1))


def remain(value, size):
    if size & (size - 1):
        return lax.rem(value, jnp.int32(size))
    return value & (size - 1)


def low_half(shape, dof):
    return lax.broadcasted_iota(jnp.int32, shape, 1) < dof


def lane_sum(values):
    return jnp.sum(values, axis=1, keepdims=True)


def split_bf16(values):
    high = values.astype(BF16)
    return high, (values - high.astype(F32)).astype(BF16)


def place(columns, shape):
    lane = lax.broadcasted_iota(jnp.int32, shape, 1)
    packed = jnp.zeros(shape, F32)
    for index, column in enumerate(columns):
        packed = jnp.where(lane == index, column, packed)
    return packed


def dense_rows(columns, shape, rows):
    size, lanes = shape
    per_row = lanes // size
    flipped = place(columns, shape).T
    lane = lax.broadcasted_iota(jnp.int32, (1, lanes), 1)
    wide = jnp.concatenate([flipped] * per_row, axis=1)
    packed = []
    for row in range(rows):
        line = jnp.zeros((1, lanes), F32)
        for inner in range(per_row):
            index = row * per_row + inner
            if index < len(columns):
                line = jnp.where(divide(lane, size) == inner, wide[index : index + 1], line)
        packed.append(line)
    return jnp.concatenate(packed, axis=0)


def position_kernel(geometry, ids, owner, table, out, where):
    per_dev, n_sub, nz, hops = geometry
    me_z, me_c, me_s = ids[0], ids[1], ids[2]
    sites = owner.shape[0]

    def locate(slot):
        dev = divide(slot, per_dev)
        grp = divide(dev, n_sub)
        block = (remain(grp, CORES) ^ me_c) * nz + (divide(grp, CORES) ^ me_z)
        return (block * n_sub + (remain(dev, n_sub) ^ me_s)) * per_dev + remain(slot, per_dev)

    def fill(slot, carry):
        where[owner[slot]] = locate(slot)
        return carry

    lax.fori_loop(0, sites, fill, 0, unroll=8)

    def look(local, carry):
        dev = (me_z * CORES + me_c) * n_sub + (divide(local, per_dev) ^ me_s)
        slot = dev * per_dev + remain(local, per_dev)
        base = owner[slot] * hops
        out[local * (hops + 1)] = locate(slot)
        for hop in range(hops):
            out[local * (hops + 1) + 1 + hop] = where[table[base + hop]]
        return carry

    lax.fori_loop(0, n_sub * per_dev, look, 0, unroll=2)


def pack_kernel(dof, op, right, low, high, turned, kept, held, op_held, sems):
    half = op.shape[0] // 2
    sources = [right, op.at[pl.ds(0, half)], op.at[pl.ds(half, half)]]
    copies = start_copies(sources, [held, op_held.at[0], op_held.at[1]], sems)
    n_sub, per_part, rhs = turned.shape[0], turned.shape[1], turned.shape[2]
    copies[0].wait()
    for pair in range(per_part):
        both = jnp.concatenate([held[2 * pair], held[2 * pair + 1]], axis=0).T
        for quarter in range(n_sub):
            turned[quarter, pair] = both[quarter * rhs : (quarter + 1) * rhs]
            kept[quarter, pair] = both[quarter * rhs : (quarter + 1) * rhs]
    main = op.shape[2] - dof
    for index, target in enumerate((low, high)):
        copies[index + 1].wait()
        for pair in range(half // 2):
            even, odd = op_held[index, 2 * pair], op_held[index, 2 * pair + 1]
            target[pair, :, :main] = even[:, :main]
            target[pair, :, main : 2 * main] = odd[:, :main]
            target[pair, :, 2 * main :] = jnp.concatenate([even[:, main:], odd[:, main:]], axis=1)


def spread(dup, pair, values, dof):
    mask = low_half(values.shape, dof)
    rolled = pltpu.roll(values, dof, 1)
    dup[2 * pair] = jnp.where(mask, values, rolled)
    dup[2 * pair + 1] = jnp.where(mask, rolled, values)


def site_vector(local, pos, dup, terms, dof):
    mask = low_half((dup.shape[1], 2 * dof), dof)
    tiles = []
    for first in range(0, terms - 1, 2):
        left = dup[pos[local * terms + first]]
        right = dup[pos[local * terms + first + 1]]
        tiles.append(jnp.where(mask, left, right))
    if terms % 2:
        tiles.append(dup[pos[local * terms + terms - 1]][:, :dof])
    return list(split_bf16(jnp.concatenate(tiles, axis=1)))


def row_pairs(op, pair, dof):
    if op.shape[1] == 2 * dof:
        return op[pair, :dof], op[pair, dof:]
    main = op.shape[2] // 2 - dof
    rows = op[pair]
    tail = rows[:, 2 * main :]
    even = jnp.concatenate([rows[:, :main], tail[:, :dof]], axis=1)
    odd = jnp.concatenate([rows[:, main : 2 * main], tail[:, dof:]], axis=1)
    return even, odd


def to_columns(even, odd):
    width, lanes = even.shape[1], 2 * even.shape[0]
    pieces = []
    for start in range(0, width, lanes):
        stop = min(start + lanes, width)
        pieces.append(jnp.concatenate([even[:, start:stop], odd[:, start:stop]], axis=0).T)
    return jnp.concatenate(split_bf16(jnp.concatenate(pieces, axis=0)), axis=1)


def pair_product(columns, local, pos, dup, terms, dof):
    rows, lanes = dup.shape[1], 2 * dof
    vectors = [v for i in range(2) for v in site_vector(local + i, pos, dup, terms, dof)]
    product = lax.dot_general(
        jnp.concatenate(vectors, axis=0),
        columns,
        (((1,), (0,)), ((), ())),
        preferred_element_type=F32,
    )
    product = product[:, :lanes] + product[:, lanes:]
    even = product[:rows] + product[rows : 2 * rows]
    odd = product[2 * rows : 3 * rows] + product[3 * rows :]
    return jnp.where(low_half(even.shape, dof), even, odd)


def rows_product(pair_rows, local, pos, dup, terms, dof):
    rows = dup.shape[1]
    halves = []
    for i, op in enumerate(pair_rows):
        product = lax.dot_general(
            jnp.concatenate(site_vector(local + i, pos, dup, terms, dof), axis=0),
            jnp.concatenate(split_bf16(op), axis=0),
            (((1,), (1,)), ((), ())),
            preferred_element_type=F32,
        )
        total = product[:rows] + product[rows:]
        halves.append(total + pltpu.roll(total, dof, 1))
    return jnp.where(low_half(halves[0].shape, dof), halves[0], halves[1])


def apply_rows(stages, pos, dup, terms, dof, put):
    base = 0
    for stage in stages:
        for pair in range(stage.shape[0]):
            columns = stage[pair]
            put(base + pair, pair_product(columns, 2 * (base + pair), pos, dup, terms, dof))
        base += stage.shape[0]


def start_copies(sources, targets, sems):
    copies = [
        pltpu.make_async_copy(source, target, sems.at[index])
        for index, (source, target) in enumerate(zip(sources, targets))
    ]
    for copy in copies:
        copy.start()
    return copies


def over_pairs(blocks, step, init):
    spot = 0
    for block, chunks in enumerate(blocks):
        start = 0
        for chunk in chunks:

            def body(pair, carry, block=block, chunk=chunk, start=start, spot=spot):
                return step(block, chunk[pair], start + pair, spot + pair, carry)

            init = lax.fori_loop(0, chunk.shape[0], body, init, unroll=True)
            start += chunk.shape[0]
            spot += chunk.shape[0]
    return init


def in_blocks(refs, chunks):
    size = len(refs) // chunks
    return [[refs[chunk * size + block] for chunk in range(chunks)] for block in range(size)]


def share_out(chunks, values, shares):
    first = [(chunk, pair) for chunk in chunks for pair in range(chunk.shape[0])]
    for index, share in enumerate(shares):
        for inner in range(share.shape[1]):
            spot = index * share.shape[1] + inner
            chunk, pair = first[spot]
            share[0, inner] = chunk[pair]
            share[1, inner] = values[spot]


def first_kernel(n_field, count, dof, terms, pos, *rest):
    fields, ops, rest = rest[:n_field], rest[n_field : n_field + count], rest[n_field + count :]
    out, split, dup = rest[:3]
    held, sems = rest[3 : 3 + count], rest[3 + count]
    copies = start_copies(ops, held, sems)

    def build(block, value, pair, spot, carry):
        spread(dup, spot, value, dof)
        return carry

    over_pairs(in_blocks(fields, 1), build, 0)
    for copy in copies:
        copy.wait()

    def put(pair, values):
        out[pair] = values

    base = 0
    for op in held:
        for inner in range(op.shape[0]):
            columns = to_columns(*row_pairs(op, inner, dof))
            split[base] = columns
            put(base, pair_product(columns, 2 * base, pos, dup, terms, dof))
            base += 1


def more_kernel(base, dof, terms, pos, dup, *rest):
    ops, out = rest[:-1], rest[-1]
    done = 0
    for op in ops:
        for inner in range(op.shape[0]):
            local = 2 * (base + done)
            out[done] = rows_product(row_pairs(op, inner, dof), local, pos, dup, terms, dof)
            done += 1


def turn_kernel(count, dof, *rest):
    ops, split = rest[:count], rest[count]
    base = 0
    for op in ops:
        for inner in range(op.shape[0]):
            split[base] = to_columns(*row_pairs(op, inner, dof))
            base += 1


def second_kernel(n_field, chunks, count, sends, dof, terms, pos, *rest):
    b_ref, rest = rest[:n_field], rest[n_field:]
    z_blocks, rest = in_blocks(rest[: chunks * n_field], chunks), rest[chunks * n_field :]
    stages, (out, basis, coeffs) = rest[:count], rest[count : count + 3]
    shares, dup = rest[count + 3 : count + 3 + sends], rest[count + 3 + sends]
    shape = b_ref[0].shape[1:]
    zero = jnp.zeros(shape, F32)

    def dots(block, z, pair, spot, carry):
        b = b_ref[block][pair]
        return carry[0] + b * b, carry[1] + b * z

    norm, cross = over_pairs(z_blocks, dots, (zero, zero))
    beta = jnp.sqrt(lane_sum(norm))
    scale = 1.0 / beta
    h00 = lane_sum(cross) * scale * scale

    def remove(block, z, pair, spot, carry):
        w = z * scale - (h00 * scale) * b_ref[block][pair]
        basis[spot] = w
        return carry + w * w

    h10 = jnp.sqrt(lane_sum(over_pairs(z_blocks, remove, zero)))
    unit = 1.0 / h10

    def build(block, w, pair, spot, carry):
        v = w * unit
        basis[spot] = v
        spread(dup, spot, v, dof)
        return carry

    over_pairs([[basis]], build, 0)
    coeffs[...] = place([beta, h00, h10], shape)

    def put(pair, values):
        out[pair] = values

    apply_rows(stages, pos, dup, terms, dof, put)
    share_out(z_blocks[0], out, shares)


def third_kernel(n_field, count, dof, terms, pos, basis, coeffs, *rest):
    b_ref, rest = rest[:n_field], rest[n_field:]
    z_blocks, rest = in_blocks(rest[:n_field], 1), rest[n_field:]
    stages, (sums, work, dup, image) = rest[:count], rest[count:]
    b_mine = b_ref[0]
    n_pair = b_mine.shape[0]
    shape = b_mine.shape[1:]
    zero = jnp.zeros(shape, F32)
    known = coeffs[...]
    scale = 1.0 / known[:, 0:1]

    def dots(block, z, pair, spot, carry):
        return carry[0] + b_ref[block][pair] * z, carry[1] + basis[spot] * z

    first, second = over_pairs(z_blocks, dots, (zero, zero))
    h01 = lane_sum(first) * scale
    h11 = lane_sum(second)

    def remove(block, z, pair, spot, carry):
        w = z - (h01 * scale) * b_ref[block][pair] - h11 * basis[spot]
        work[spot] = w
        return carry + w * w

    h21 = jnp.sqrt(lane_sum(over_pairs(z_blocks, remove, zero)))
    unit = 1.0 / h21

    def build(block, w, pair, spot, carry):
        v = w * unit
        work[spot] = v
        spread(dup, spot, v, dof)
        return carry

    over_pairs([[work]], build, 0)

    def put(pair, values):
        image[pair] = values

    apply_rows(stages, pos, dup, terms, dof, put)

    def last(pair, carry):
        u = image[pair]
        return (
            carry[0] + b_mine[pair] * u,
            carry[1] + basis[pair] * u,
            carry[2] + work[pair] * u,
            carry[3] + u * u,
        )

    parts = lax.fori_loop(0, n_pair, last, (zero, zero, zero, zero), unroll=True)
    solved = [known[:, 0:1], known[:, 1:2], known[:, 2:3], h01, h11, h21]
    columns = [lane_sum(part) for part in parts] + solved
    if len(sums.shape) == 3 and sums.shape[1:] == shape:
        packed = place(columns, shape)
    else:
        packed = dense_rows(columns, shape, sums.shape[1])
    for block in range(sums.shape[0]):
        sums[block] = packed


def weigh(values):
    d02, h12, h22, g22, beta, h00, h10, h01, h11, h21 = values
    scale = 1.0 / beta
    h02 = d02 * scale
    g00 = h00 * h00 + h10 * h10
    g01 = h00 * h01 + h10 * h11
    g02 = h00 * h02 + h10 * h12
    g11 = h01 * h01 + h11 * h11 + h21 * h21
    g12 = h01 * h02 + h11 * h12 + h21 * h22
    inv0 = 1.0 / g00
    l10 = g01 * inv0
    l20 = g02 * inv0
    d1 = g11 - l10 * g01
    e21 = g12 - l20 * g01
    inv1 = 1.0 / d1
    l21 = e21 * inv1
    d2 = g22 - l20 * g02 - l21 * e21
    r0 = beta * h00
    r1 = beta * h01 - l10 * r0
    r2 = beta * h02 - l20 * r0 - l21 * r1
    y2 = r2 / d2
    y1 = r1 * inv1 - l21 * y2
    y0 = r0 * inv0 - l10 * y1 - l20 * y2
    return scale, y0, y1, y2


def combine_kernel(sums, b_mine, v1_mine, v2_mine, out):
    total = sums[0]
    for block in range(1, sums.shape[0]):
        total = total + sums[block]
    known = sums[0]
    values = [(total if i < 4 else known)[:, i : i + 1] for i in range(10)]
    scale, y0, y1, y2 = weigh(values)
    for pair in range(b_mine.shape[0]):
        out[pair] = (y0 * scale) * b_mine[pair] + y1 * v1_mine[pair] + y2 * v2_mine[pair]


def finish_kernel(dof, ids, info, turned, *rest):
    out, stack, factor = rest[-3:]
    n_sub, per_part, rhs, lanes = turned.shape
    shares = rest[:n_sub]
    per_row = lanes // rhs
    n_rows = info.shape[1]
    first = [info[quarter] for quarter in range(n_sub)]
    total = list(first)
    for block in range(1, info.shape[0] // n_sub):
        for quarter in range(n_sub):
            total[quarter] = total[quarter] + info[block * n_sub + quarter]
    known = [jnp.concatenate([f[r : r + 1] for f in first], axis=0) for r in range(n_rows)]
    added = [jnp.concatenate([t[r : r + 1] for t in total], axis=0) for r in range(n_rows)]
    values = []
    for index in range(10):
        source = (added if index < 4 else known)[index // per_row]
        shift = rhs * (index % per_row)
        values.append(pltpu.roll(source, lanes - shift, 1) if shift else source)
    scale, y0, y1, y2 = weigh(values)
    h00, h10, h01, h11, h21 = values[5:]
    gamma = y2 / h21
    both = (y1 - gamma * h11) / h10
    coeffs = [(y0 - both * h00 - gamma * h01) * scale, both * scale, gamma]
    flipped = jnp.concatenate(coeffs, axis=0)
    spare = -flipped.shape[0] % 8
    if spare:
        flipped = jnp.concatenate([flipped, jnp.zeros((spare, lanes), F32)], axis=0)
    flipped = flipped.T
    for index in range(3 * n_sub):
        factor[index] = jnp.broadcast_to(flipped[:rhs, index : index + 1], (rhs, lanes))
    for k in range(n_sub):
        quarter = ids[2] ^ k
        alpha, beta, gamma = (factor[part * n_sub + quarter] for part in range(3))
        start = pl.multiple_of(quarter * rhs, 8)
        for pair in range(per_part):
            mixed = alpha * turned[quarter, pair] + beta * shares[k][0, pair]
            stack[pair, pl.ds(start, rhs), :] = mixed + gamma * shares[k][1, pair]
    for pair in range(per_part):
        both = stack[pair].T
        out[2 * pair] = both[:dof]
        out[2 * pair + 1] = both[dof:]


def per_device(coarse_op, right_side, owner_map, neighbor_table):
    nz = lax.axis_size("z")
    n_sub = lax.axis_size("sub")
    per_dev, dof, width = coarse_op.shape
    terms = width // dof
    hops = terms - 1
    rhs = right_side.shape[2] // n_sub
    n_loc = n_sub * per_dev
    n_own = n_loc // 2
    me_z, me_c, me_s = lax.axis_index("z"), lax.axis_index("core"), lax.axis_index("sub")
    ids = jnp.stack([me_z, me_c, me_s]).astype(jnp.int32)
    even = per_dev % 2 == 0
    lanes = 2 * dof
    field = (n_own, rhs, lanes)

    relay = n_sub == 4 and per_dev % 4 == 0 and terms % 2 == 1
    order = jnp.arange(n_sub, dtype=jnp.int32) ^ me_s
    hops_to = [[(s, s ^ k) for s in range(n_sub)] for k in range(n_sub)]
    half = per_dev // 2
    if relay:
        halves = [jax.ShapeDtypeStruct((half // 2, dof, 2 * width), F32)] * 2
        op_low, op_high, turned, kept = pl.pallas_call(
            functools.partial(pack_kernel, dof),
            out_shape=halves + [jax.ShapeDtypeStruct((n_sub, half, rhs, lanes), F32)] * 2,
            in_specs=[HBM, HBM],
            out_specs=[VMEM] * 4,
            scratch_shapes=[
                pltpu.VMEM(right_side.shape, F32),
                pltpu.VMEM((2, half, dof, width), F32),
                pltpu.SemaphoreType.DMA((3,)),
            ],
            compiler_params=SMALL,
            name="pack",
        )(coarse_op, right_side)
        x_high = lax.ppermute(op_high, "sub", hops_to[1])
        y_low = lax.ppermute(op_low, "sub", hops_to[2])
        x_low = lax.ppermute(op_low, "sub", hops_to[1])
        y_high = lax.ppermute(op_high, "sub", hops_to[2])

    positions = pl.pallas_call(
        functools.partial(position_kernel, (per_dev, n_sub, nz, hops)),
        out_shape=jax.ShapeDtypeStruct((n_loc * terms,), jnp.int32),
        in_specs=[SMEM, SMEM, SMEM],
        out_specs=SMEM,
        scratch_shapes=[pltpu.SMEM((owner_map.shape[0],), jnp.int32)],
        compiler_params=SMALL,
        name="positions",
    )(ids, owner_map, neighbor_table.reshape(-1))

    if not relay:
        turned = right_side.reshape(per_dev, dof, n_sub, rhs).transpose(2, 0, 3, 1)
    if even and not relay:
        turned = turned.reshape(n_sub, per_dev // 2, 2, rhs, dof).transpose(0, 1, 3, 2, 4)
        turned = turned.reshape(n_sub, per_dev // 2, rhs, lanes)
    if not relay:
        kept = turned
    mine = lax.all_to_all(turned, "sub", split_axis=0, concat_axis=0, tiled=True)
    mine = mine[order]
    if not even:
        mine = mine.reshape(n_own, 2, rhs, dof).transpose(0, 2, 1, 3)
    b_mine = mine.reshape(field)

    swap = [(c, c ^ 1) for c in range(CORES)]

    def step_z(own, offset):
        return lax.ppermute(own, "z", [(z, z ^ offset) for z in range(nz)])

    def gather(own):
        if nz == 4:
            cross, near = step_z(own, 2), step_z(own, 1)
            parts = [own, near, cross, step_z(cross, 1)]
        else:
            parts = [own] + [step_z(own, offset) for offset in range(1, nz)]
        for index in range(nz):
            parts.append(lax.ppermute(parts[index], "core", swap))
        return parts

    if relay:
        d_low = lax.ppermute(y_low, "sub", hops_to[1])
        d_high = lax.ppermute(x_high, "sub", hops_to[2])
        stages = [[op_low, op_high, x_low, x_high, y_low, y_high], [d_low, d_high]]
    if not relay:
        every = lax.all_gather(coarse_op, "sub", axis=0)[order]
        stages = [[every.reshape(n_own, 2 * dof, width)]]
    b_parts = gather(b_mine)
    n_field = len(b_parts)
    dup = (CORES * nz * n_loc, rhs, lanes)
    full = (CORES * nz * n_own,) + field[1:]
    small = jax.ShapeDtypeStruct(field[1:], F32)
    own_shape = jax.ShapeDtypeStruct(field, F32)
    sends = n_sub if even else 0
    share = [jax.ShapeDtypeStruct((2, per_dev // 2, rhs, lanes), F32)] * sends

    def split_shape(pairs):
        return jax.ShapeDtypeStruct((pairs, width, 4 * dof), BF16)

    ops = stages[0]
    done = sum(op.shape[0] for op in ops)
    z1, split, spread_b = pl.pallas_call(
        functools.partial(first_kernel, n_field, len(ops), dof, terms),
        out_shape=[
            jax.ShapeDtypeStruct((done,) + field[1:], F32),
            split_shape(done),
            jax.ShapeDtypeStruct(dup, F32),
        ],
        in_specs=[SMEM] + [VMEM] * n_field + [ANY] * len(ops),
        out_specs=[VMEM] * 3,
        scratch_shapes=[pltpu.VMEM(op.shape, F32) for op in ops]
        + [pltpu.SemaphoreType.DMA((len(ops),))],
        compiler_params=PARAMS,
        name="first",
    )(positions, *b_parts, *ops)
    splits, chunks = [split], 1
    z1_parts = gather(z1)
    if relay:
        ops, chunks = stages[1], 2
        late = pl.pallas_call(
            functools.partial(more_kernel, done, dof, terms),
            out_shape=jax.ShapeDtypeStruct((n_own - done,) + field[1:], F32),
            in_specs=[SMEM, VMEM] + [VMEM] * len(ops),
            out_specs=VMEM,
            compiler_params=PARAMS,
            name="more",
        )(positions, spread_b, *ops)
        z1_parts = z1_parts + gather(late)
        split = pl.pallas_call(
            functools.partial(turn_kernel, len(ops), dof),
            out_shape=split_shape(n_own - done),
            in_specs=[VMEM] * len(ops),
            out_specs=VMEM,
            compiler_params=PARAMS,
            name="turn",
        )(*ops)
        splits.append(split)
    count = len(splits)

    z2, basis, coeffs, *shares = pl.pallas_call(
        functools.partial(second_kernel, n_field, chunks, count, sends, dof, terms),
        out_shape=[own_shape, jax.ShapeDtypeStruct(full, F32), small] + share,
        in_specs=[SMEM] + [VMEM] * ((1 + chunks) * n_field + count),
        out_specs=[VMEM] * (3 + sends),
        scratch_shapes=[pltpu.VMEM(dup, F32)],
        compiler_params=PARAMS,
        name="second",
    )(positions, *b_parts, *z1_parts, *splits)
    z2_parts = gather(z2)
    shares[1:] = [lax.ppermute(shares[k], "sub", hops_to[k]) for k in range(1, sends)]
    z2_parts, shares = lax.optimization_barrier((z2_parts, shares))

    axes = ("z", "core", "sub") if even else ("z", "core")
    copies = nz * CORES * (n_sub if even else 1)
    note = (pl.cdiv(10 * rhs, lanes), lanes) if even else field[1:]
    keep = [] if even else [jax.ShapeDtypeStruct(full, F32)]
    sums, *work = pl.pallas_call(
        functools.partial(third_kernel, n_field, count, dof, terms),
        out_shape=[jax.ShapeDtypeStruct((copies,) + note, F32)] + keep,
        in_specs=[SMEM] + [VMEM] * (2 + 2 * n_field + count),
        out_specs=[VMEM] * (1 + len(keep)),
        scratch_shapes=[pltpu.VMEM(full, F32)] * (1 - len(keep))
        + [pltpu.VMEM(dup, F32), pltpu.VMEM(field, F32)],
        compiler_params=PARAMS,
        name="third",
    )(positions, basis, coeffs, *b_parts, *z2_parts, *splits)
    sums = lax.all_to_all(sums, axes, split_axis=0, concat_axis=0, tiled=True)

    if even:
        return pl.pallas_call(
            functools.partial(finish_kernel, dof),
            out_shape=jax.ShapeDtypeStruct(right_side.shape, F32),
            in_specs=[SMEM] + [VMEM] * (2 + sends),
            out_specs=VMEM,
            scratch_shapes=[
                pltpu.VMEM((per_dev // 2, n_sub * rhs, lanes), F32),
                pltpu.VMEM((3 * n_sub, rhs, lanes), F32),
            ],
            compiler_params=SMALL,
            name="finish",
        )(ids, sums, kept, *shares)
    result = pl.pallas_call(
        combine_kernel,
        out_shape=own_shape,
        in_specs=[VMEM] * 4,
        out_specs=VMEM,
        compiler_params=SMALL,
            name="combine",
    )(sums, b_mine, basis[:n_own], work[0][:n_own])
    result = result.reshape(n_own, rhs, 2, dof).transpose(0, 2, 1, 3)
    result = result.reshape(n_sub, per_dev, rhs, dof)[order]
    result = lax.all_to_all(result, "sub", split_axis=0, concat_axis=0, tiled=True)
    return result.transpose(1, 3, 0, 2).reshape(right_side.shape)


def solution(mesh):
    n_grp, n_sub = mesh.shape["grp"], mesh.shape["sub"]
    inner = Mesh(mesh.devices.reshape(n_grp // CORES, CORES, n_sub), ("z", "core", "sub"))
    split = P(("z", "core", "sub"), None, None)

    return jax.shard_map(
        per_device,
        mesh=inner,
        in_specs=(split, split, P(), P()),
        out_specs=split,
        check_vma=False,
    )
```

```python
import functools

import jax
import jax.numpy as jnp
from jax import lax
from jax.experimental import pallas as pl
from jax.experimental.pallas import tpu as pltpu
from jax.sharding import Mesh
from jax.sharding import PartitionSpec as P


F32 = jnp.float32
BF16 = jnp.bfloat16
CORES = 2
VMEM = pl.BlockSpec(memory_space=pltpu.VMEM)
SMEM = pl.BlockSpec(memory_space=pltpu.SMEM)
HBM = pl.BlockSpec(memory_space=pltpu.HBM)
ANY = pl.BlockSpec(memory_space=pl.ANY)
PARAMS = pltpu.CompilerParams(vmem_limit_bytes=20 * 1024 * 1024)
SMALL = pltpu.CompilerParams(vmem_limit_bytes=4 * 1024 * 1024)


def divide(value, size):
    if size & (size - 1):
        return lax.div(value, jnp.int32(size))
    return lax.shift_right_logical(value, jnp.int32(size.bit_length() - 1))


def remain(value, size):
    if size & (size - 1):
        return lax.rem(value, jnp.int32(size))
    return value & (size - 1)


def low_half(shape, dof):
    return lax.broadcasted_iota(jnp.int32, shape, 1) < dof


def lane_sum(values):
    return jnp.sum(values, axis=1, keepdims=True)


def split_bf16(values):
    high = values.astype(BF16)
    return high, (values - high.astype(F32)).astype(BF16)


def place(columns, shape):
    lane = lax.broadcasted_iota(jnp.int32, shape, 1)
    packed = jnp.zeros(shape, F32)
    for index, column in enumerate(columns):
        packed = jnp.where(lane == index, column, packed)
    return packed


def dense_rows(columns, shape, rows):
    size, lanes = shape
    per_row = lanes // size
    flipped = place(columns, shape).T
    lane = lax.broadcasted_iota(jnp.int32, (1, lanes), 1)
    wide = jnp.concatenate([flipped] * per_row, axis=1)
    packed = []
    for row in range(rows):
        line = jnp.zeros((1, lanes), F32)
        for inner in range(per_row):
            index = row * per_row + inner
            if index < len(columns):
                line = jnp.where(divide(lane, size) == inner, wide[index : index + 1], line)
        packed.append(line)
    return jnp.concatenate(packed, axis=0)


def position_kernel(geometry, ids, owner, table, out, where):
    per_dev, n_sub, nz, hops = geometry
    me_z, me_c, me_s = ids[0], ids[1], ids[2]
    sites = owner.shape[0]

    def locate(slot):
        dev = divide(slot, per_dev)
        grp = divide(dev, n_sub)
        block = (remain(grp, CORES) ^ me_c) * nz + (divide(grp, CORES) ^ me_z)
        return (block * n_sub + (remain(dev, n_sub) ^ me_s)) * per_dev + remain(slot, per_dev)

    def fill(slot, carry):
        where[owner[slot]] = locate(slot)
        return carry

    lax.fori_loop(0, sites, fill, 0, unroll=8)

    def look(local, carry):
        dev = (me_z * CORES + me_c) * n_sub + (divide(local, per_dev) ^ me_s)
        slot = dev * per_dev + remain(local, per_dev)
        base = owner[slot] * hops
        out[local * (hops + 1)] = locate(slot)
        for hop in range(hops):
            out[local * (hops + 1) + 1 + hop] = where[table[base + hop]]
        return carry

    lax.fori_loop(0, n_sub * per_dev, look, 0, unroll=2)


def pack_kernel(dof, op, low, high, held, sems):
    half = op.shape[0] // 2
    count = sems.shape[0]
    size = op.shape[0] // count
    sources = [op.at[pl.ds(size * index, size)] for index in range(count)]
    copies = start_copies(sources, [held.at[index] for index in range(count)], sems)
    main = op.shape[2] - dof
    for index in range(count):
        copies[index].wait()
        for inner in range(size // 2):
            even, odd = held[index, 2 * inner], held[index, 2 * inner + 1]
            pair = (size * index) // 2 + inner
            target, pair = (low, pair) if pair < half // 2 else (high, pair - half // 2)
            target[pair, :, :main] = even[:, :main]
            target[pair, :, main : 2 * main] = odd[:, :main]
            target[pair, :, 2 * main :] = jnp.concatenate([even[:, main:], odd[:, main:]], axis=1)


def turn_right_kernel(right, turned, kept):
    n_sub, per_part, rhs = turned.shape[0], turned.shape[1], turned.shape[2]
    for pair in range(per_part):
        both = jnp.concatenate([right[2 * pair], right[2 * pair + 1]], axis=0).T
        for quarter in range(n_sub):
            turned[quarter, pair] = both[quarter * rhs : (quarter + 1) * rhs]
            kept[quarter, pair] = both[quarter * rhs : (quarter + 1) * rhs]


def spread(dup, pair, values, dof):
    mask = low_half(values.shape, dof)
    rolled = pltpu.roll(values, dof, 1)
    dup[2 * pair] = jnp.where(mask, values, rolled)
    dup[2 * pair + 1] = jnp.where(mask, rolled, values)


def site_vector(local, pos, dup, terms, dof):
    mask = low_half((dup.shape[1], 2 * dof), dof)
    tiles = []
    for first in range(0, terms - 1, 2):
        left = dup[pos[local * terms + first]]
        right = dup[pos[local * terms + first + 1]]
        tiles.append(jnp.where(mask, left, right))
    if terms % 2:
        tiles.append(dup[pos[local * terms + terms - 1]][:, :dof])
    return list(split_bf16(jnp.concatenate(tiles, axis=1)))


def row_pairs(op, pair, dof):
    if op.shape[1] == 2 * dof:
        return op[pair, :dof], op[pair, dof:]
    main = op.shape[2] // 2 - dof
    rows = op[pair]
    tail = rows[:, 2 * main :]
    even = jnp.concatenate([rows[:, :main], tail[:, :dof]], axis=1)
    odd = jnp.concatenate([rows[:, main : 2 * main], tail[:, dof:]], axis=1)
    return even, odd


def to_columns(even, odd):
    width, lanes = even.shape[1], 2 * even.shape[0]
    pieces = []
    for start in range(0, width, lanes):
        stop = min(start + lanes, width)
        pieces.append(jnp.concatenate([even[:, start:stop], odd[:, start:stop]], axis=0).T)
    return jnp.concatenate(split_bf16(jnp.concatenate(pieces, axis=0)), axis=1)


def pair_product(columns, local, pos, dup, terms, dof):
    rows, lanes = dup.shape[1], 2 * dof
    vectors = [v for i in range(2) for v in site_vector(local + i, pos, dup, terms, dof)]
    product = lax.dot_general(
        jnp.concatenate(vectors, axis=0),
        columns,
        (((1,), (0,)), ((), ())),
        preferred_element_type=F32,
    )
    product = product[:, :lanes] + product[:, lanes:]
    even = product[:rows] + product[rows : 2 * rows]
    odd = product[2 * rows : 3 * rows] + product[3 * rows :]
    return jnp.where(low_half(even.shape, dof), even, odd)


def rows_product(pair_rows, local, pos, dup, terms, dof):
    rows = dup.shape[1]
    halves = []
    for i, op in enumerate(pair_rows):
        product = lax.dot_general(
            jnp.concatenate(site_vector(local + i, pos, dup, terms, dof), axis=0),
            jnp.concatenate(split_bf16(op), axis=0),
            (((1,), (1,)), ((), ())),
            preferred_element_type=F32,
        )
        total = product[:rows] + product[rows:]
        halves.append(total + pltpu.roll(total, dof, 1))
    return jnp.where(low_half(halves[0].shape, dof), halves[0], halves[1])


def apply_rows(stages, pos, dup, terms, dof, put):
    base = 0
    for stage in stages:
        for pair in range(stage.shape[0]):
            columns = stage[pair]
            put(base + pair, pair_product(columns, 2 * (base + pair), pos, dup, terms, dof))
        base += stage.shape[0]


def start_copies(sources, targets, sems):
    copies = [
        pltpu.make_async_copy(source, target, sems.at[index])
        for index, (source, target) in enumerate(zip(sources, targets))
    ]
    for copy in copies:
        copy.start()
    return copies


def over_pairs(blocks, step, init):
    spot = 0
    for block, chunks in enumerate(blocks):
        start = 0
        for chunk in chunks:

            def body(pair, carry, block=block, chunk=chunk, start=start, spot=spot):
                return step(block, chunk[pair], start + pair, spot + pair, carry)

            init = lax.fori_loop(0, chunk.shape[0], body, init, unroll=True)
            start += chunk.shape[0]
            spot += chunk.shape[0]
    return init


def in_blocks(refs, chunks):
    size = len(refs) // chunks
    return [[refs[chunk * size + block] for chunk in range(chunks)] for block in range(size)]


def share_out(chunks, values, shares):
    first = [(chunk, pair) for chunk in chunks for pair in range(chunk.shape[0])]
    for index, share in enumerate(shares):
        for inner in range(share.shape[1]):
            spot = index * share.shape[1] + inner
            chunk, pair = first[spot]
            share[0, inner] = chunk[pair]
            share[1, inner] = values[spot]


def first_kernel(n_field, count, dof, terms, pos, *rest):
    fields, ops, rest = rest[:n_field], rest[n_field : n_field + count], rest[n_field + count :]
    out, split, dup = rest[:3]
    held, sems = rest[3 : 3 + count], rest[3 + count]
    copies = start_copies(ops, held, sems)

    def build(block, value, pair, spot, carry):
        spread(dup, spot, value, dof)
        return carry

    over_pairs(in_blocks(fields, 1), build, 0)
    for copy in copies:
        copy.wait()

    def put(pair, values):
        out[pair] = values

    base = 0
    for op in held:
        for inner in range(op.shape[0]):
            columns = to_columns(*row_pairs(op, inner, dof))
            split[base] = columns
            put(base, pair_product(columns, 2 * base, pos, dup, terms, dof))
            base += 1


def more_kernel(base, dof, terms, pos, dup, *rest):
    ops, out = rest[:-1], rest[-1]
    done = 0
    for op in ops:
        for inner in range(op.shape[0]):
            local = 2 * (base + done)
            out[done] = rows_product(row_pairs(op, inner, dof), local, pos, dup, terms, dof)
            done += 1


def turn_kernel(count, dof, *rest):
    ops, split = rest[:count], rest[count]
    base = 0
    for op in ops:
        for inner in range(op.shape[0]):
            split[base] = to_columns(*row_pairs(op, inner, dof))
            base += 1


def second_kernel(n_field, chunks, count, sends, dof, terms, pos, *rest):
    b_ref, rest = rest[:n_field], rest[n_field:]
    z_blocks, rest = in_blocks(rest[: chunks * n_field], chunks), rest[chunks * n_field :]
    stages, (out, basis, coeffs) = rest[:count], rest[count : count + 3]
    shares, dup = rest[count + 3 : count + 3 + sends], rest[count + 3 + sends]
    shape = b_ref[0].shape[1:]
    zero = jnp.zeros(shape, F32)

    def dots(block, z, pair, spot, carry):
        b = b_ref[block][pair]
        return carry[0] + b * b, carry[1] + b * z

    norm, cross = over_pairs(z_blocks, dots, (zero, zero))
    beta = jnp.sqrt(lane_sum(norm))
    scale = 1.0 / beta
    h00 = lane_sum(cross) * scale * scale

    def remove(block, z, pair, spot, carry):
        w = z * scale - (h00 * scale) * b_ref[block][pair]
        basis[spot] = w
        return carry + w * w

    h10 = jnp.sqrt(lane_sum(over_pairs(z_blocks, remove, zero)))
    unit = 1.0 / h10

    def build(block, w, pair, spot, carry):
        v = w * unit
        basis[spot] = v
        spread(dup, spot, v, dof)
        return carry

    over_pairs([[basis]], build, 0)
    coeffs[...] = place([beta, h00, h10], shape)

    def put(pair, values):
        out[pair] = values

    apply_rows(stages, pos, dup, terms, dof, put)
    share_out(z_blocks[0], out, shares)


def third_kernel(n_field, count, dof, terms, pos, basis, coeffs, *rest):
    b_ref, rest = rest[:n_field], rest[n_field:]
    z_blocks, rest = in_blocks(rest[:n_field], 1), rest[n_field:]
    stages, (sums, work, dup, image) = rest[:count], rest[count:]
    b_mine = b_ref[0]
    n_pair = b_mine.shape[0]
    shape = b_mine.shape[1:]
    zero = jnp.zeros(shape, F32)
    known = coeffs[...]
    scale = 1.0 / known[:, 0:1]

    def dots(block, z, pair, spot, carry):
        return carry[0] + b_ref[block][pair] * z, carry[1] + basis[spot] * z

    first, second = over_pairs(z_blocks, dots, (zero, zero))
    h01 = lane_sum(first) * scale
    h11 = lane_sum(second)

    def remove(block, z, pair, spot, carry):
        w = z - (h01 * scale) * b_ref[block][pair] - h11 * basis[spot]
        work[spot] = w
        return carry + w * w

    h21 = jnp.sqrt(lane_sum(over_pairs(z_blocks, remove, zero)))
    unit = 1.0 / h21

    def build(block, w, pair, spot, carry):
        v = w * unit
        work[spot] = v
        spread(dup, spot, v, dof)
        return carry

    over_pairs([[work]], build, 0)

    def put(pair, values):
        image[pair] = values

    apply_rows(stages, pos, dup, terms, dof, put)

    def last(pair, carry):
        u = image[pair]
        return (
            carry[0] + b_mine[pair] * u,
            carry[1] + basis[pair] * u,
            carry[2] + work[pair] * u,
            carry[3] + u * u,
        )

    parts = lax.fori_loop(0, n_pair, last, (zero, zero, zero, zero), unroll=True)
    solved = [known[:, 0:1], known[:, 1:2], known[:, 2:3], h01, h11, h21]
    columns = [lane_sum(part) for part in parts] + solved
    if len(sums.shape) == 3 and sums.shape[1:] == shape:
        packed = place(columns, shape)
    else:
        packed = dense_rows(columns, shape, sums.shape[1])
    for block in range(sums.shape[0]):
        sums[block] = packed


def weigh(values):
    d02, h12, h22, g22, beta, h00, h10, h01, h11, h21 = values
    scale = 1.0 / beta
    h02 = d02 * scale
    g00 = h00 * h00 + h10 * h10
    g01 = h00 * h01 + h10 * h11
    g02 = h00 * h02 + h10 * h12
    g11 = h01 * h01 + h11 * h11 + h21 * h21
    g12 = h01 * h02 + h11 * h12 + h21 * h22
    inv0 = 1.0 / g00
    l10 = g01 * inv0
    l20 = g02 * inv0
    d1 = g11 - l10 * g01
    e21 = g12 - l20 * g01
    inv1 = 1.0 / d1
    l21 = e21 * inv1
    d2 = g22 - l20 * g02 - l21 * e21
    r0 = beta * h00
    r1 = beta * h01 - l10 * r0
    r2 = beta * h02 - l20 * r0 - l21 * r1
    y2 = r2 / d2
    y1 = r1 * inv1 - l21 * y2
    y0 = r0 * inv0 - l10 * y1 - l20 * y2
    return scale, y0, y1, y2


def combine_kernel(sums, b_mine, v1_mine, v2_mine, out):
    total = sums[0]
    for block in range(1, sums.shape[0]):
        total = total + sums[block]
    known = sums[0]
    values = [(total if i < 4 else known)[:, i : i + 1] for i in range(10)]
    scale, y0, y1, y2 = weigh(values)
    for pair in range(b_mine.shape[0]):
        out[pair] = (y0 * scale) * b_mine[pair] + y1 * v1_mine[pair] + y2 * v2_mine[pair]


def finish_kernel(dof, ids, info, turned, *rest):
    out, stack, factor = rest[-3:]
    n_sub, per_part, rhs, lanes = turned.shape
    shares = rest[:n_sub]
    per_row = lanes // rhs
    n_rows = info.shape[1]
    first = [info[quarter] for quarter in range(n_sub)]
    total = list(first)
    for block in range(1, info.shape[0] // n_sub):
        for quarter in range(n_sub):
            total[quarter] = total[quarter] + info[block * n_sub + quarter]
    known = [jnp.concatenate([f[r : r + 1] for f in first], axis=0) for r in range(n_rows)]
    added = [jnp.concatenate([t[r : r + 1] for t in total], axis=0) for r in range(n_rows)]
    values = []
    for index in range(10):
        source = (added if index < 4 else known)[index // per_row]
        shift = rhs * (index % per_row)
        values.append(pltpu.roll(source, lanes - shift, 1) if shift else source)
    scale, y0, y1, y2 = weigh(values)
    h00, h10, h01, h11, h21 = values[5:]
    gamma = y2 / h21
    both = (y1 - gamma * h11) / h10
    coeffs = [(y0 - both * h00 - gamma * h01) * scale, both * scale, gamma]
    flipped = jnp.concatenate(coeffs, axis=0)
    spare = -flipped.shape[0] % 8
    if spare:
        flipped = jnp.concatenate([flipped, jnp.zeros((spare, lanes), F32)], axis=0)
    flipped = flipped.T
    for index in range(3 * n_sub):
        factor[index] = jnp.broadcast_to(flipped[:rhs, index : index + 1], (rhs, lanes))
    for k in range(n_sub):
        quarter = ids[2] ^ k
        alpha, beta, gamma = (factor[part * n_sub + quarter] for part in range(3))
        start = pl.multiple_of(quarter * rhs, 8)
        for pair in range(per_part):
            mixed = alpha * turned[quarter, pair] + beta * shares[k][0, pair]
            stack[pair, pl.ds(start, rhs), :] = mixed + gamma * shares[k][1, pair]
    for pair in range(per_part):
        both = stack[pair].T
        out[2 * pair] = both[:dof]
        out[2 * pair + 1] = both[dof:]


def per_device(coarse_op, right_side, owner_map, neighbor_table):
    nz = lax.axis_size("z")
    n_sub = lax.axis_size("sub")
    per_dev, dof, width = coarse_op.shape
    terms = width // dof
    hops = terms - 1
    rhs = right_side.shape[2] // n_sub
    n_loc = n_sub * per_dev
    n_own = n_loc // 2
    me_z, me_c, me_s = lax.axis_index("z"), lax.axis_index("core"), lax.axis_index("sub")
    ids = jnp.stack([me_z, me_c, me_s]).astype(jnp.int32)
    even = per_dev % 2 == 0
    lanes = 2 * dof
    field = (n_own, rhs, lanes)

    relay = n_sub == 4 and per_dev % 4 == 0 and terms % 2 == 1
    order = jnp.arange(n_sub, dtype=jnp.int32) ^ me_s
    hops_to = [[(s, s ^ k) for s in range(n_sub)] for k in range(n_sub)]
    half = per_dev // 2
    if relay:
        halves = [jax.ShapeDtypeStruct((half // 2, dof, 2 * width), F32)] * 2
        parts = per_dev // 2
        op_low, op_high = pl.pallas_call(
            functools.partial(pack_kernel, dof),
            out_shape=halves,
            in_specs=[HBM],
            out_specs=[VMEM] * 2,
            scratch_shapes=[
                pltpu.VMEM((parts, 2, dof, width), F32),
                pltpu.SemaphoreType.DMA((parts,)),
            ],
            compiler_params=SMALL,
            name="pack",
        )(pltpu.with_memory_space_constraint(coarse_op, pltpu.HBM))
        turned, kept = pl.pallas_call(
            turn_right_kernel,
            out_shape=[jax.ShapeDtypeStruct((n_sub, half, rhs, lanes), F32)] * 2,
            in_specs=[VMEM],
            out_specs=[VMEM] * 2,
            compiler_params=SMALL,
            name="pack_right",
        )(right_side)
        x_high = lax.ppermute(op_high, "sub", hops_to[1])
        y_low = lax.ppermute(op_low, "sub", hops_to[2])
        x_low = lax.ppermute(op_low, "sub", hops_to[1])
        y_high = lax.ppermute(op_high, "sub", hops_to[2])

    positions = pl.pallas_call(
        functools.partial(position_kernel, (per_dev, n_sub, nz, hops)),
        out_shape=jax.ShapeDtypeStruct((n_loc * terms,), jnp.int32),
        in_specs=[SMEM, SMEM, SMEM],
        out_specs=SMEM,
        scratch_shapes=[pltpu.SMEM((owner_map.shape[0],), jnp.int32)],
        compiler_params=SMALL,
        name="positions",
    )(ids, owner_map, neighbor_table.reshape(-1))

    if not relay:
        turned = right_side.reshape(per_dev, dof, n_sub, rhs).transpose(2, 0, 3, 1)
    if even and not relay:
        turned = turned.reshape(n_sub, per_dev // 2, 2, rhs, dof).transpose(0, 1, 3, 2, 4)
        turned = turned.reshape(n_sub, per_dev // 2, rhs, lanes)
    if not relay:
        kept = turned
    mine = lax.all_to_all(turned, "sub", split_axis=0, concat_axis=0, tiled=True)
    mine = mine[order]
    if not even:
        mine = mine.reshape(n_own, 2, rhs, dof).transpose(0, 2, 1, 3)
    b_mine = mine.reshape(field)

    swap = [(c, c ^ 1) for c in range(CORES)]

    def step_z(own, offset):
        return lax.ppermute(own, "z", [(z, z ^ offset) for z in range(nz)])

    def gather(own):
        if nz == 4:
            cross = step_z(own, 2)
            near = step_z(own, 1)
            parts = [own, near, cross, step_z(cross, 1)]
        else:
            parts = [own] + [step_z(own, offset) for offset in range(1, nz)]
        for index in range(nz):
            parts.append(lax.ppermute(parts[index], "core", swap))
        return parts

    if relay:
        d_low = lax.ppermute(y_low, "sub", hops_to[1])
        d_high = lax.ppermute(x_high, "sub", hops_to[2])
        stages = [[op_low, op_high, x_low, x_high, y_low, y_high], [d_low, d_high]]
    if not relay:
        every = lax.all_gather(coarse_op, "sub", axis=0)[order]
        stages = [[every.reshape(n_own, 2 * dof, width)]]
    b_parts = gather(b_mine)
    n_field = len(b_parts)
    dup = (CORES * nz * n_loc, rhs, lanes)
    full = (CORES * nz * n_own,) + field[1:]
    small = jax.ShapeDtypeStruct(field[1:], F32)
    own_shape = jax.ShapeDtypeStruct(field, F32)
    sends = n_sub if even else 0
    share = [jax.ShapeDtypeStruct((2, per_dev // 2, rhs, lanes), F32)] * sends

    def split_shape(pairs):
        return jax.ShapeDtypeStruct((pairs, width, 4 * dof), BF16)

    ops = stages[0]
    done = sum(op.shape[0] for op in ops)
    z1, split, spread_b = pl.pallas_call(
        functools.partial(first_kernel, n_field, len(ops), dof, terms),
        out_shape=[
            jax.ShapeDtypeStruct((done,) + field[1:], F32),
            split_shape(done),
            jax.ShapeDtypeStruct(dup, F32),
        ],
        in_specs=[SMEM] + [VMEM] * n_field + [ANY] * len(ops),
        out_specs=[VMEM] * 3,
        scratch_shapes=[pltpu.VMEM(op.shape, F32) for op in ops]
        + [pltpu.SemaphoreType.DMA((len(ops),))],
        compiler_params=PARAMS,
        name="first",
    )(positions, *b_parts, *ops)
    splits, chunks = [split], 1
    z1_parts = gather(z1)
    if relay:
        ops, chunks = stages[1], 2
        late = pl.pallas_call(
            functools.partial(more_kernel, done, dof, terms),
            out_shape=jax.ShapeDtypeStruct((n_own - done,) + field[1:], F32),
            in_specs=[SMEM, VMEM] + [VMEM] * len(ops),
            out_specs=VMEM,
            compiler_params=PARAMS,
            name="more",
        )(positions, spread_b, *ops)
        z1_parts = z1_parts + gather(late)
        split = pl.pallas_call(
            functools.partial(turn_kernel, len(ops), dof),
            out_shape=split_shape(n_own - done),
            in_specs=[VMEM] * len(ops),
            out_specs=VMEM,
            compiler_params=PARAMS,
            name="turn",
        )(*ops)
        splits.append(split)
    count = len(splits)

    z2, basis, coeffs, *shares = pl.pallas_call(
        functools.partial(second_kernel, n_field, chunks, count, sends, dof, terms),
        out_shape=[own_shape, jax.ShapeDtypeStruct(full, F32), small] + share,
        in_specs=[SMEM] + [VMEM] * ((1 + chunks) * n_field + count),
        out_specs=[VMEM] * (3 + sends),
        scratch_shapes=[pltpu.VMEM(dup, F32)],
        compiler_params=PARAMS,
        name="second",
    )(positions, *b_parts, *z1_parts, *splits)
    z2_parts = gather(z2)
    shares[1:] = [lax.ppermute(shares[k], "sub", hops_to[k]) for k in range(1, sends)]
    z2_parts, shares = lax.optimization_barrier((z2_parts, shares))

    axes = ("z", "core", "sub") if even else ("z", "core")
    copies = nz * CORES * (n_sub if even else 1)
    note = (pl.cdiv(10 * rhs, lanes), lanes) if even else field[1:]
    keep = [] if even else [jax.ShapeDtypeStruct(full, F32)]
    sums, *work = pl.pallas_call(
        functools.partial(third_kernel, n_field, count, dof, terms),
        out_shape=[jax.ShapeDtypeStruct((copies,) + note, F32)] + keep,
        in_specs=[SMEM] + [VMEM] * (2 + 2 * n_field + count),
        out_specs=[VMEM] * (1 + len(keep)),
        scratch_shapes=[pltpu.VMEM(full, F32)] * (1 - len(keep))
        + [pltpu.VMEM(dup, F32), pltpu.VMEM(field, F32)],
        compiler_params=PARAMS,
        name="third",
    )(positions, basis, coeffs, *b_parts, *z2_parts, *splits)
    sums = lax.all_to_all(sums, axes, split_axis=0, concat_axis=0, tiled=True)

    if even:
        return pl.pallas_call(
            functools.partial(finish_kernel, dof),
            out_shape=jax.ShapeDtypeStruct(right_side.shape, F32),
            in_specs=[SMEM] + [VMEM] * (2 + sends),
            out_specs=VMEM,
            scratch_shapes=[
                pltpu.VMEM((per_dev // 2, n_sub * rhs, lanes), F32),
                pltpu.VMEM((3 * n_sub, rhs, lanes), F32),
            ],
            compiler_params=SMALL,
            name="finish",
        )(ids, sums, kept, *shares)
    result = pl.pallas_call(
        combine_kernel,
        out_shape=own_shape,
        in_specs=[VMEM] * 4,
        out_specs=VMEM,
        compiler_params=SMALL,
            name="combine",
    )(sums, b_mine, basis[:n_own], work[0][:n_own])
    result = result.reshape(n_own, rhs, 2, dof).transpose(0, 2, 1, 3)
    result = result.reshape(n_sub, per_dev, rhs, dof)[order]
    result = lax.all_to_all(result, "sub", split_axis=0, concat_axis=0, tiled=True)
    return result.transpose(1, 3, 0, 2).reshape(right_side.shape)


def solution(mesh):
    n_grp, n_sub = mesh.shape["grp"], mesh.shape["sub"]
    inner = Mesh(mesh.devices.reshape(n_grp // CORES, CORES, n_sub), ("z", "core", "sub"))
    split = P(("z", "core", "sub"), None, None)

    return jax.shard_map(
        per_device,
        mesh=inner,
        in_specs=(split, split, P(), P()),
        out_specs=split,
        check_vma=False,
    )
```

```python
import functools

import jax
import jax.numpy as jnp
from jax import lax
from jax.experimental import pallas as pl
from jax.experimental.pallas import tpu as pltpu
from jax.sharding import Mesh
from jax.sharding import PartitionSpec as P


F32 = jnp.float32
BF16 = jnp.bfloat16
CORES = 2
VMEM = pl.BlockSpec(memory_space=pltpu.VMEM)
SMEM = pl.BlockSpec(memory_space=pltpu.SMEM)
HBM = pl.BlockSpec(memory_space=pltpu.HBM)
ANY = pl.BlockSpec(memory_space=pl.ANY)
PARAMS = pltpu.CompilerParams(vmem_limit_bytes=20 * 1024 * 1024)
SMALL = pltpu.CompilerParams(vmem_limit_bytes=4 * 1024 * 1024)


def divide(value, size):
    if size & (size - 1):
        return lax.div(value, jnp.int32(size))
    return lax.shift_right_logical(value, jnp.int32(size.bit_length() - 1))


def remain(value, size):
    if size & (size - 1):
        return lax.rem(value, jnp.int32(size))
    return value & (size - 1)


def low_half(shape, dof):
    return lax.broadcasted_iota(jnp.int32, shape, 1) < dof


def lane_sum(values):
    return jnp.sum(values, axis=1, keepdims=True)


def split_bf16(values):
    high = values.astype(BF16)
    return high, (values - high.astype(F32)).astype(BF16)


def place(columns, shape):
    lane = lax.broadcasted_iota(jnp.int32, shape, 1)
    packed = jnp.zeros(shape, F32)
    for index, column in enumerate(columns):
        packed = jnp.where(lane == index, column, packed)
    return packed


def dense_rows(columns, shape, rows):
    size, lanes = shape
    per_row = lanes // size
    flipped = place(columns, shape).T
    lane = lax.broadcasted_iota(jnp.int32, (1, lanes), 1)
    wide = jnp.concatenate([flipped] * per_row, axis=1)
    packed = []
    for row in range(rows):
        line = jnp.zeros((1, lanes), F32)
        for inner in range(per_row):
            index = row * per_row + inner
            if index < len(columns):
                line = jnp.where(divide(lane, size) == inner, wide[index : index + 1], line)
        packed.append(line)
    return jnp.concatenate(packed, axis=0)


def position_kernel(geometry, ids, owner, table, out, where):
    per_dev, n_sub, nz, hops = geometry
    me_z, me_c, me_s = ids[0], ids[1], ids[2]
    sites = owner.shape[0]

    def locate(slot):
        dev = divide(slot, per_dev)
        grp = divide(dev, n_sub)
        block = (remain(grp, CORES) ^ me_c) * nz + (divide(grp, CORES) ^ me_z)
        return (block * n_sub + (remain(dev, n_sub) ^ me_s)) * per_dev + remain(slot, per_dev)

    def fill(slot, carry):
        where[owner[slot]] = locate(slot)
        return carry

    lax.fori_loop(0, sites, fill, 0, unroll=8)

    def look(local, carry):
        dev = (me_z * CORES + me_c) * n_sub + (divide(local, per_dev) ^ me_s)
        slot = dev * per_dev + remain(local, per_dev)
        base = owner[slot] * hops
        out[local * (hops + 1)] = locate(slot)
        for hop in range(hops):
            out[local * (hops + 1) + 1 + hop] = where[table[base + hop]]
        return carry

    lax.fori_loop(0, n_sub * per_dev, look, 0, unroll=2)


def pack_kernel(dof, op, low, high, held, sems):
    half = op.shape[0] // 2
    count = sems.shape[0]
    size = op.shape[0] // count
    sources = [op.at[pl.ds(size * index, size)] for index in range(count)]
    copies = start_copies(sources, [held.at[index] for index in range(count)], sems)
    main = op.shape[2] - dof
    for index in range(count):
        copies[index].wait()
        for inner in range(size // 2):
            even, odd = held[index, 2 * inner], held[index, 2 * inner + 1]
            pair = (size * index) // 2 + inner
            target, pair = (low, pair) if pair < half // 2 else (high, pair - half // 2)
            target[pair, :, :main] = even[:, :main]
            target[pair, :, main : 2 * main] = odd[:, :main]
            target[pair, :, 2 * main :] = jnp.concatenate([even[:, main:], odd[:, main:]], axis=1)


def turn_right_kernel(right, turned, kept):
    n_sub, per_part, rhs = turned.shape[0], turned.shape[1], turned.shape[2]
    for pair in range(per_part):
        both = jnp.concatenate([right[2 * pair], right[2 * pair + 1]], axis=0).T
        for quarter in range(n_sub):
            turned[quarter, pair] = both[quarter * rhs : (quarter + 1) * rhs]
            kept[quarter, pair] = both[quarter * rhs : (quarter + 1) * rhs]


def spread(dup, pair, values, dof):
    mask = low_half(values.shape, dof)
    rolled = pltpu.roll(values, dof, 1)
    dup[2 * pair] = jnp.where(mask, values, rolled)
    dup[2 * pair + 1] = jnp.where(mask, rolled, values)


def site_vector(local, pos, dup, terms, dof):
    mask = low_half((dup.shape[1], 2 * dof), dof)
    tiles = []
    for first in range(0, terms - 1, 2):
        left = dup[pos[local * terms + first]]
        right = dup[pos[local * terms + first + 1]]
        tiles.append(jnp.where(mask, left, right))
    if terms % 2:
        tiles.append(dup[pos[local * terms + terms - 1]][:, :dof])
    return list(split_bf16(jnp.concatenate(tiles, axis=1)))


def row_pairs(op, pair, dof):
    if op.shape[1] == 2 * dof:
        return op[pair, :dof], op[pair, dof:]
    main = op.shape[2] // 2 - dof
    rows = op[pair]
    tail = rows[:, 2 * main :]
    even = jnp.concatenate([rows[:, :main], tail[:, :dof]], axis=1)
    odd = jnp.concatenate([rows[:, main : 2 * main], tail[:, dof:]], axis=1)
    return even, odd


def to_columns(even, odd):
    width, lanes = even.shape[1], 2 * even.shape[0]
    pieces = []
    for start in range(0, width, lanes):
        stop = min(start + lanes, width)
        pieces.append(jnp.concatenate([even[:, start:stop], odd[:, start:stop]], axis=0).T)
    return jnp.concatenate(split_bf16(jnp.concatenate(pieces, axis=0)), axis=1)


def pair_product(columns, local, pos, dup, terms, dof):
    rows, lanes = dup.shape[1], 2 * dof
    vectors = [v for i in range(2) for v in site_vector(local + i, pos, dup, terms, dof)]
    product = lax.dot_general(
        jnp.concatenate(vectors, axis=0),
        columns,
        (((1,), (0,)), ((), ())),
        preferred_element_type=F32,
    )
    product = product[:, :lanes] + product[:, lanes:]
    even = product[:rows] + product[rows : 2 * rows]
    odd = product[2 * rows : 3 * rows] + product[3 * rows :]
    return jnp.where(low_half(even.shape, dof), even, odd)


def rows_product(pair_rows, local, pos, dup, terms, dof):
    rows = dup.shape[1]
    halves = []
    for i, op in enumerate(pair_rows):
        product = lax.dot_general(
            jnp.concatenate(site_vector(local + i, pos, dup, terms, dof), axis=0),
            jnp.concatenate(split_bf16(op), axis=0),
            (((1,), (1,)), ((), ())),
            preferred_element_type=F32,
        )
        total = product[:rows] + product[rows:]
        halves.append(total + pltpu.roll(total, dof, 1))
    return jnp.where(low_half(halves[0].shape, dof), halves[0], halves[1])


def apply_rows(stages, pos, dup, terms, dof, put):
    base = 0
    for stage in stages:
        for pair in range(stage.shape[0]):
            columns = stage[pair]
            put(base + pair, pair_product(columns, 2 * (base + pair), pos, dup, terms, dof))
        base += stage.shape[0]


def start_copies(sources, targets, sems):
    copies = [
        pltpu.make_async_copy(source, target, sems.at[index])
        for index, (source, target) in enumerate(zip(sources, targets))
    ]
    for copy in copies:
        copy.start()
    return copies


def over_pairs(blocks, step, init):
    spot = 0
    for block, chunks in enumerate(blocks):
        start = 0
        for chunk in chunks:

            def body(pair, carry, block=block, chunk=chunk, start=start, spot=spot):
                return step(block, chunk[pair], start + pair, spot + pair, carry)

            init = lax.fori_loop(0, chunk.shape[0], body, init, unroll=True)
            start += chunk.shape[0]
            spot += chunk.shape[0]
    return init


def in_blocks(refs, chunks):
    size = len(refs) // chunks
    return [[refs[chunk * size + block] for chunk in range(chunks)] for block in range(size)]


def share_out(chunks, values, shares):
    first = [(chunk, pair) for chunk in chunks for pair in range(chunk.shape[0])]
    for index, share in enumerate(shares):
        for inner in range(share.shape[1]):
            spot = index * share.shape[1] + inner
            chunk, pair = first[spot]
            share[0, inner] = chunk[pair]
            share[1, inner] = values[spot]


def first_kernel(n_field, count, dof, terms, pos, *rest):
    fields, ops, rest = rest[:n_field], rest[n_field : n_field + count], rest[n_field + count :]
    out, split, dup = rest[:3]
    held, sems = rest[3 : 3 + count], rest[3 + count]
    copies = start_copies(ops, held, sems)

    def build(block, value, pair, spot, carry):
        spread(dup, spot, value, dof)
        return carry

    over_pairs(in_blocks(fields, 1), build, 0)
    for copy in copies:
        copy.wait()

    def put(pair, values):
        out[pair] = values

    base = 0
    for op in held:
        for inner in range(op.shape[0]):
            columns = to_columns(*row_pairs(op, inner, dof))
            split[base] = columns
            put(base, pair_product(columns, 2 * base, pos, dup, terms, dof))
            base += 1


def more_kernel(base, dof, terms, pos, dup, *rest):
    ops, out = rest[:-1], rest[-1]
    done = 0
    for op in ops:
        for inner in range(op.shape[0]):
            local = 2 * (base + done)
            out[done] = rows_product(row_pairs(op, inner, dof), local, pos, dup, terms, dof)
            done += 1


def turn_kernel(count, dof, *rest):
    ops, split = rest[:count], rest[count]
    base = 0
    for op in ops:
        for inner in range(op.shape[0]):
            split[base] = to_columns(*row_pairs(op, inner, dof))
            base += 1


def second_kernel(n_field, chunks, count, sends, dof, terms, links, *rest):
    rest, (pos, sem) = rest[:-2], rest[-2:]
    copy = pltpu.make_async_copy(links, pos, sem)
    copy.start()
    b_ref, rest = rest[:n_field], rest[n_field:]
    z_blocks, rest = in_blocks(rest[: chunks * n_field], chunks), rest[chunks * n_field :]
    stages, (out, basis, coeffs) = rest[:count], rest[count : count + 3]
    shares, dup = rest[count + 3 : count + 3 + sends], rest[count + 3 + sends]
    shape = b_ref[0].shape[1:]
    zero = jnp.zeros(shape, F32)

    def dots(block, z, pair, spot, carry):
        b = b_ref[block][pair]
        return carry[0] + b * b, carry[1] + b * z

    norm, cross = over_pairs(z_blocks, dots, (zero, zero))
    beta = jnp.sqrt(lane_sum(norm))
    scale = 1.0 / beta
    h00 = lane_sum(cross) * scale * scale

    def remove(block, z, pair, spot, carry):
        w = z * scale - (h00 * scale) * b_ref[block][pair]
        basis[spot] = w
        return carry + w * w

    h10 = jnp.sqrt(lane_sum(over_pairs(z_blocks, remove, zero)))
    unit = 1.0 / h10

    def build(block, w, pair, spot, carry):
        v = w * unit
        basis[spot] = v
        spread(dup, spot, v, dof)
        return carry

    over_pairs([[basis]], build, 0)
    coeffs[...] = place([beta, h00, h10], shape)

    def put(pair, values):
        out[pair] = values

    copy.wait()
    apply_rows(stages, pos, dup, terms, dof, put)
    share_out(z_blocks[0], out, shares)


def third_kernel(n_field, count, dof, terms, links, basis, coeffs, *rest):
    rest, (pos, sem) = rest[:-2], rest[-2:]
    copy = pltpu.make_async_copy(links, pos, sem)
    copy.start()
    b_ref, rest = rest[:n_field], rest[n_field:]
    z_blocks, rest = in_blocks(rest[:n_field], 1), rest[n_field:]
    stages, (sums, work, dup, image) = rest[:count], rest[count:]
    b_mine = b_ref[0]
    n_pair = b_mine.shape[0]
    shape = b_mine.shape[1:]
    zero = jnp.zeros(shape, F32)
    known = coeffs[...]
    scale = 1.0 / known[:, 0:1]

    def dots(block, z, pair, spot, carry):
        return carry[0] + b_ref[block][pair] * z, carry[1] + basis[spot] * z

    first, second = over_pairs(z_blocks, dots, (zero, zero))
    h01 = lane_sum(first) * scale
    h11 = lane_sum(second)

    def remove(block, z, pair, spot, carry):
        w = z - (h01 * scale) * b_ref[block][pair] - h11 * basis[spot]
        work[spot] = w
        return carry + w * w

    h21 = jnp.sqrt(lane_sum(over_pairs(z_blocks, remove, zero)))
    unit = 1.0 / h21

    def build(block, w, pair, spot, carry):
        v = w * unit
        work[spot] = v
        spread(dup, spot, v, dof)
        return carry

    over_pairs([[work]], build, 0)

    def put(pair, values):
        image[pair] = values

    copy.wait()
    apply_rows(stages, pos, dup, terms, dof, put)

    def last(pair, carry):
        u = image[pair]
        return (
            carry[0] + b_mine[pair] * u,
            carry[1] + basis[pair] * u,
            carry[2] + work[pair] * u,
            carry[3] + u * u,
        )

    parts = lax.fori_loop(0, n_pair, last, (zero, zero, zero, zero), unroll=True)
    solved = [known[:, 0:1], known[:, 1:2], known[:, 2:3], h01, h11, h21]
    columns = [lane_sum(part) for part in parts] + solved
    if len(sums.shape) == 3 and sums.shape[1:] == shape:
        packed = place(columns, shape)
    else:
        packed = dense_rows(columns, shape, sums.shape[1])
    for block in range(sums.shape[0]):
        sums[block] = packed


def weigh(values):
    d02, h12, h22, g22, beta, h00, h10, h01, h11, h21 = values
    scale = 1.0 / beta
    h02 = d02 * scale
    g00 = h00 * h00 + h10 * h10
    g01 = h00 * h01 + h10 * h11
    g02 = h00 * h02 + h10 * h12
    g11 = h01 * h01 + h11 * h11 + h21 * h21
    g12 = h01 * h02 + h11 * h12 + h21 * h22
    inv0 = 1.0 / g00
    l10 = g01 * inv0
    l20 = g02 * inv0
    d1 = g11 - l10 * g01
    e21 = g12 - l20 * g01
    inv1 = 1.0 / d1
    l21 = e21 * inv1
    d2 = g22 - l20 * g02 - l21 * e21
    r0 = beta * h00
    r1 = beta * h01 - l10 * r0
    r2 = beta * h02 - l20 * r0 - l21 * r1
    y2 = r2 / d2
    y1 = r1 * inv1 - l21 * y2
    y0 = r0 * inv0 - l10 * y1 - l20 * y2
    return scale, y0, y1, y2


def combine_kernel(sums, b_mine, v1_mine, v2_mine, out):
    total = sums[0]
    for block in range(1, sums.shape[0]):
        total = total + sums[block]
    known = sums[0]
    values = [(total if i < 4 else known)[:, i : i + 1] for i in range(10)]
    scale, y0, y1, y2 = weigh(values)
    for pair in range(b_mine.shape[0]):
        out[pair] = (y0 * scale) * b_mine[pair] + y1 * v1_mine[pair] + y2 * v2_mine[pair]


def finish_kernel(dof, info, turned, *rest):
    out, stack, factor = rest[-3:]
    n_sub, per_part, rhs, lanes = turned.shape
    shares = rest[:n_sub]
    per_row = lanes // rhs
    n_rows = info.shape[1]
    first = [info[quarter] for quarter in range(n_sub)]
    total = list(first)
    for block in range(1, info.shape[0] // n_sub):
        for quarter in range(n_sub):
            total[quarter] = total[quarter] + info[block * n_sub + quarter]
    known = [jnp.concatenate([f[r : r + 1] for f in first], axis=0) for r in range(n_rows)]
    added = [jnp.concatenate([t[r : r + 1] for t in total], axis=0) for r in range(n_rows)]
    values = []
    for index in range(10):
        source = (added if index < 4 else known)[index // per_row]
        shift = rhs * (index % per_row)
        values.append(pltpu.roll(source, lanes - shift, 1) if shift else source)
    scale, y0, y1, y2 = weigh(values)
    h00, h10, h01, h11, h21 = values[5:]
    gamma = y2 / h21
    both = (y1 - gamma * h11) / h10
    coeffs = [(y0 - both * h00 - gamma * h01) * scale, both * scale, gamma]
    flipped = jnp.concatenate(coeffs, axis=0)
    spare = -flipped.shape[0] % 8
    if spare:
        flipped = jnp.concatenate([flipped, jnp.zeros((spare, lanes), F32)], axis=0)
    flipped = flipped.T
    for index in range(3 * n_sub):
        factor[index] = jnp.broadcast_to(flipped[:rhs, index : index + 1], (rhs, lanes))
    for k in range(n_sub):
        quarter = lax.axis_index("sub") ^ k
        alpha, beta, gamma = (factor[part * n_sub + quarter] for part in range(3))
        start = pl.multiple_of(quarter * rhs, 8)
        for pair in range(per_part):
            mixed = alpha * turned[quarter, pair] + beta * shares[k][0, pair]
            stack[pair, pl.ds(start, rhs), :] = mixed + gamma * shares[k][1, pair]
    for pair in range(per_part):
        both = stack[pair].T
        out[2 * pair] = both[:dof]
        out[2 * pair + 1] = both[dof:]


def per_device(coarse_op, right_side, owner_map, neighbor_table):
    nz = lax.axis_size("z")
    n_sub = lax.axis_size("sub")
    per_dev, dof, width = coarse_op.shape
    terms = width // dof
    hops = terms - 1
    rhs = right_side.shape[2] // n_sub
    n_loc = n_sub * per_dev
    n_own = n_loc // 2
    me_z, me_c, me_s = lax.axis_index("z"), lax.axis_index("core"), lax.axis_index("sub")
    ids = jnp.stack([me_z, me_c, me_s]).astype(jnp.int32)
    even = per_dev % 2 == 0
    lanes = 2 * dof
    field = (n_own, rhs, lanes)

    relay = n_sub == 4 and per_dev % 4 == 0 and terms % 2 == 1
    order = jnp.arange(n_sub, dtype=jnp.int32) ^ me_s
    hops_to = [[(s, s ^ k) for s in range(n_sub)] for k in range(n_sub)]
    half = per_dev // 2
    if relay:
        halves = [jax.ShapeDtypeStruct((half // 2, dof, 2 * width), F32)] * 2
        parts = per_dev // 2
        op_low, op_high = pl.pallas_call(
            functools.partial(pack_kernel, dof),
            out_shape=halves,
            in_specs=[HBM],
            out_specs=[VMEM] * 2,
            scratch_shapes=[
                pltpu.VMEM((parts, 2, dof, width), F32),
                pltpu.SemaphoreType.DMA((parts,)),
            ],
            compiler_params=SMALL,
            name="pack",
        )(pltpu.with_memory_space_constraint(coarse_op, pltpu.HBM))
        turned, kept = pl.pallas_call(
            turn_right_kernel,
            out_shape=[jax.ShapeDtypeStruct((n_sub, half, rhs, lanes), F32)] * 2,
            in_specs=[VMEM],
            out_specs=[VMEM] * 2,
            compiler_params=SMALL,
            name="pack_right",
        )(right_side)
        x_high = lax.ppermute(op_high, "sub", hops_to[1])
        y_low = lax.ppermute(op_low, "sub", hops_to[2])
        x_low = lax.ppermute(op_low, "sub", hops_to[1])
        y_high = lax.ppermute(op_high, "sub", hops_to[2])

    positions = pl.pallas_call(
        functools.partial(position_kernel, (per_dev, n_sub, nz, hops)),
        out_shape=jax.ShapeDtypeStruct((n_loc * terms,), jnp.int32),
        in_specs=[SMEM, SMEM, SMEM],
        out_specs=SMEM,
        scratch_shapes=[pltpu.SMEM((owner_map.shape[0],), jnp.int32)],
        compiler_params=SMALL,
        name="positions",
    )(ids, owner_map, neighbor_table.reshape(-1))

    if not relay:
        turned = right_side.reshape(per_dev, dof, n_sub, rhs).transpose(2, 0, 3, 1)
    if even and not relay:
        turned = turned.reshape(n_sub, per_dev // 2, 2, rhs, dof).transpose(0, 1, 3, 2, 4)
        turned = turned.reshape(n_sub, per_dev // 2, rhs, lanes)
    if not relay:
        kept = turned
    mine = lax.all_to_all(turned, "sub", split_axis=0, concat_axis=0, tiled=True)
    mine = mine[order]
    if not even:
        mine = mine.reshape(n_own, 2, rhs, dof).transpose(0, 2, 1, 3)
    b_mine = mine.reshape(field)

    swap = [(c, c ^ 1) for c in range(CORES)]

    def step_z(own, offset):
        return lax.ppermute(own, "z", [(z, z ^ offset) for z in range(nz)])

    def gather(own):
        if nz == 4:
            cross = step_z(own, 2)
            near = step_z(own, 1)
            parts = [own, near, cross, step_z(cross, 1)]
        else:
            parts = [own] + [step_z(own, offset) for offset in range(1, nz)]
        for index in range(nz):
            parts.append(lax.ppermute(parts[index], "core", swap))
        return parts

    if relay:
        d_low = lax.ppermute(y_low, "sub", hops_to[1])
        d_high = lax.ppermute(x_high, "sub", hops_to[2])
        stages = [[op_low, op_high, x_low, x_high, y_low, y_high], [d_low, d_high]]
    if not relay:
        every = lax.all_gather(coarse_op, "sub", axis=0)[order]
        stages = [[every.reshape(n_own, 2 * dof, width)]]
    b_parts = gather(b_mine)
    n_field = len(b_parts)
    dup = (CORES * nz * n_loc, rhs, lanes)
    full = (CORES * nz * n_own,) + field[1:]
    small = jax.ShapeDtypeStruct(field[1:], F32)
    own_shape = jax.ShapeDtypeStruct(field, F32)
    sends = n_sub if even else 0
    share = [jax.ShapeDtypeStruct((2, per_dev // 2, rhs, lanes), F32)] * sends

    def split_shape(pairs):
        return jax.ShapeDtypeStruct((pairs, width, 4 * dof), BF16)

    ops = stages[0]
    done = sum(op.shape[0] for op in ops)
    z1, split, spread_b = pl.pallas_call(
        functools.partial(first_kernel, n_field, len(ops), dof, terms),
        out_shape=[
            jax.ShapeDtypeStruct((done,) + field[1:], F32),
            split_shape(done),
            jax.ShapeDtypeStruct(dup, F32),
        ],
        in_specs=[SMEM] + [VMEM] * n_field + [ANY] * len(ops),
        out_specs=[VMEM] * 3,
        scratch_shapes=[pltpu.VMEM(op.shape, F32) for op in ops]
        + [pltpu.SemaphoreType.DMA((len(ops),))],
        compiler_params=PARAMS,
        name="first",
    )(positions, *b_parts, *ops)
    splits, chunks = [split], 1
    z1_parts = gather(z1)
    if relay:
        ops, chunks = stages[1], 2
        late = pl.pallas_call(
            functools.partial(more_kernel, done, dof, terms),
            out_shape=jax.ShapeDtypeStruct((n_own - done,) + field[1:], F32),
            in_specs=[SMEM, VMEM] + [VMEM] * len(ops),
            out_specs=VMEM,
            compiler_params=PARAMS,
            name="more",
        )(positions, spread_b, *ops)
        z1_parts = z1_parts + gather(late)
        split = pl.pallas_call(
            functools.partial(turn_kernel, len(ops), dof),
            out_shape=split_shape(n_own - done),
            in_specs=[VMEM] * len(ops),
            out_specs=VMEM,
            compiler_params=PARAMS,
            name="turn",
        )(*ops)
        splits.append(split)
    count = len(splits)
    links = [pltpu.SMEM(positions.shape, jnp.int32), pltpu.SemaphoreType.DMA]

    z2, basis, coeffs, *shares = pl.pallas_call(
        functools.partial(second_kernel, n_field, chunks, count, sends, dof, terms),
        out_shape=[own_shape, jax.ShapeDtypeStruct(full, F32), small] + share,
        in_specs=[ANY] + [VMEM] * ((1 + chunks) * n_field + count),
        out_specs=[VMEM] * (3 + sends),
        scratch_shapes=[pltpu.VMEM(dup, F32)] + links,
        compiler_params=PARAMS,
        name="second",
    )(positions, *b_parts, *z1_parts, *splits)
    z2_parts = gather(z2)
    shares[1:] = [lax.ppermute(shares[k], "sub", hops_to[k]) for k in range(1, sends)]
    z2_parts, shares = lax.optimization_barrier((z2_parts, shares))

    axes = ("z", "core", "sub") if even else ("z", "core")
    copies = nz * CORES * (n_sub if even else 1)
    note = (pl.cdiv(10 * rhs, lanes), lanes) if even else field[1:]
    keep = [] if even else [jax.ShapeDtypeStruct(full, F32)]
    sums, *work = pl.pallas_call(
        functools.partial(third_kernel, n_field, count, dof, terms),
        out_shape=[jax.ShapeDtypeStruct((copies,) + note, F32)] + keep,
        in_specs=[ANY] + [VMEM] * (2 + 2 * n_field + count),
        out_specs=[VMEM] * (1 + len(keep)),
        scratch_shapes=[pltpu.VMEM(full, F32)] * (1 - len(keep))
        + [pltpu.VMEM(dup, F32), pltpu.VMEM(field, F32)]
        + links,
        compiler_params=PARAMS,
        name="third",
    )(positions, basis, coeffs, *b_parts, *z2_parts, *splits)
    sums = lax.all_to_all(sums, axes, split_axis=0, concat_axis=0, tiled=True)

    if even:
        return pl.pallas_call(
            functools.partial(finish_kernel, dof),
            out_shape=jax.ShapeDtypeStruct(right_side.shape, F32),
            in_specs=[VMEM] * (2 + sends),
            out_specs=VMEM,
            scratch_shapes=[
                pltpu.VMEM((per_dev // 2, n_sub * rhs, lanes), F32),
                pltpu.VMEM((3 * n_sub, rhs, lanes), F32),
            ],
            compiler_params=SMALL,
            name="finish",
        )(sums, kept, *shares)
    result = pl.pallas_call(
        combine_kernel,
        out_shape=own_shape,
        in_specs=[VMEM] * 4,
        out_specs=VMEM,
        compiler_params=SMALL,
            name="combine",
    )(sums, b_mine, basis[:n_own], work[0][:n_own])
    result = result.reshape(n_own, rhs, 2, dof).transpose(0, 2, 1, 3)
    result = result.reshape(n_sub, per_dev, rhs, dof)[order]
    result = lax.all_to_all(result, "sub", split_axis=0, concat_axis=0, tiled=True)
    return result.transpose(1, 3, 0, 2).reshape(right_side.shape)


def solution(mesh):
    n_grp, n_sub = mesh.shape["grp"], mesh.shape["sub"]
    inner = Mesh(mesh.devices.reshape(n_grp // CORES, CORES, n_sub), ("z", "core", "sub"))
    split = P(("z", "core", "sub"), None, None)

    return jax.shard_map(
        per_device,
        mesh=inner,
        in_specs=(split, split, P(), P()),
        out_specs=split,
        check_vma=False,
    )
```

```python
import functools

import jax
import jax.numpy as jnp
from jax import lax
from jax.experimental import pallas as pl
from jax.experimental.pallas import tpu as pltpu
from jax.sharding import Mesh
from jax.sharding import PartitionSpec as P


F32 = jnp.float32
BF16 = jnp.bfloat16
CORES = 2
VMEM = pl.BlockSpec(memory_space=pltpu.VMEM)
SMEM = pl.BlockSpec(memory_space=pltpu.SMEM)
HBM = pl.BlockSpec(memory_space=pltpu.HBM)
ANY = pl.BlockSpec(memory_space=pl.ANY)
PARAMS = pltpu.CompilerParams(vmem_limit_bytes=20 * 1024 * 1024)
SMALL = pltpu.CompilerParams(vmem_limit_bytes=4 * 1024 * 1024)


def divide(value, size):
    if size & (size - 1):
        return lax.div(value, jnp.int32(size))
    return lax.shift_right_logical(value, jnp.int32(size.bit_length() - 1))


def remain(value, size):
    if size & (size - 1):
        return lax.rem(value, jnp.int32(size))
    return value & (size - 1)


def low_half(shape, dof):
    return lax.broadcasted_iota(jnp.int32, shape, 1) < dof


def lane_sum(values):
    return jnp.sum(values, axis=1, keepdims=True)


def split_bf16(values):
    high = values.astype(BF16)
    return high, (values - high.astype(F32)).astype(BF16)


def place(columns, shape):
    lane = lax.broadcasted_iota(jnp.int32, shape, 1)
    packed = jnp.zeros(shape, F32)
    for index, column in enumerate(columns):
        packed = jnp.where(lane == index, column, packed)
    return packed


def dense_rows(columns, shape, rows):
    size, lanes = shape
    per_row = lanes // size
    flipped = place(columns, shape).T
    lane = lax.broadcasted_iota(jnp.int32, (1, lanes), 1)
    wide = jnp.concatenate([flipped] * per_row, axis=1)
    packed = []
    for row in range(rows):
        line = jnp.zeros((1, lanes), F32)
        for inner in range(per_row):
            index = row * per_row + inner
            if index < len(columns):
                line = jnp.where(divide(lane, size) == inner, wide[index : index + 1], line)
        packed.append(line)
    return jnp.concatenate(packed, axis=0)


def position_kernel(geometry, ids, owner, table, out, where):
    per_dev, n_sub, nz, hops = geometry
    me_z, me_c, me_s = ids[0], ids[1], ids[2]
    sites = owner.shape[0]

    def locate(slot):
        dev = divide(slot, per_dev)
        grp = divide(dev, n_sub)
        block = (remain(grp, CORES) ^ me_c) * nz + (divide(grp, CORES) ^ me_z)
        return (block * n_sub + (remain(dev, n_sub) ^ me_s)) * per_dev + remain(slot, per_dev)

    def fill(slot, carry):
        where[owner[slot]] = locate(slot)
        return carry

    lax.fori_loop(0, sites, fill, 0, unroll=8)

    def look(local, carry):
        dev = (me_z * CORES + me_c) * n_sub + (divide(local, per_dev) ^ me_s)
        slot = dev * per_dev + remain(local, per_dev)
        base = owner[slot] * hops
        out[local * (hops + 1)] = locate(slot)
        for hop in range(hops):
            out[local * (hops + 1) + 1 + hop] = where[table[base + hop]]
        return carry

    lax.fori_loop(0, n_sub * per_dev, look, 0, unroll=2)


def pack_kernel(dof, op, low, high, held, sems):
    half = op.shape[0] // 2
    count = sems.shape[0]
    size = op.shape[0] // count
    sources = [op.at[pl.ds(size * index, size)] for index in range(count)]
    copies = start_copies(sources, [held.at[index] for index in range(count)], sems)
    main = op.shape[2] - dof
    for index in range(count):
        copies[index].wait()
        for inner in range(size // 2):
            even, odd = held[index, 2 * inner], held[index, 2 * inner + 1]
            pair = (size * index) // 2 + inner
            target, pair = (low, pair) if pair < half // 2 else (high, pair - half // 2)
            target[pair, :, :main] = even[:, :main]
            target[pair, :, main : 2 * main] = odd[:, :main]
            target[pair, :, 2 * main :] = jnp.concatenate([even[:, main:], odd[:, main:]], axis=1)


def turn_right_kernel(right, turned, kept):
    n_sub, per_part, rhs = turned.shape[0], turned.shape[1], turned.shape[2]
    for pair in range(per_part):
        both = jnp.concatenate([right[2 * pair], right[2 * pair + 1]], axis=0).T
        for quarter in range(n_sub):
            turned[quarter, pair] = both[quarter * rhs : (quarter + 1) * rhs]
            kept[quarter, pair] = both[quarter * rhs : (quarter + 1) * rhs]


def spread(dup, pair, values, dof):
    mask = low_half(values.shape, dof)
    rolled = pltpu.roll(values, dof, 1)
    dup[2 * pair] = jnp.where(mask, values, rolled)
    dup[2 * pair + 1] = jnp.where(mask, rolled, values)


def site_vector(local, pos, dup, terms, dof):
    mask = low_half((dup.shape[1], 2 * dof), dof)
    tiles = []
    for first in range(0, terms - 1, 2):
        left = dup[pos[local * terms + first]]
        right = dup[pos[local * terms + first + 1]]
        tiles.append(jnp.where(mask, left, right))
    if terms % 2:
        tiles.append(dup[pos[local * terms + terms - 1]][:, :dof])
    return list(split_bf16(jnp.concatenate(tiles, axis=1)))


def row_pairs(op, pair, dof):
    if op.shape[1] == 2 * dof:
        return op[pair, :dof], op[pair, dof:]
    main = op.shape[2] // 2 - dof
    rows = op[pair]
    tail = rows[:, 2 * main :]
    even = jnp.concatenate([rows[:, :main], tail[:, :dof]], axis=1)
    odd = jnp.concatenate([rows[:, main : 2 * main], tail[:, dof:]], axis=1)
    return even, odd


def to_columns(even, odd):
    width, lanes = even.shape[1], 2 * even.shape[0]
    pieces = []
    for start in range(0, width, lanes):
        stop = min(start + lanes, width)
        pieces.append(jnp.concatenate([even[:, start:stop], odd[:, start:stop]], axis=0).T)
    return jnp.concatenate(split_bf16(jnp.concatenate(pieces, axis=0)), axis=1)


def pair_product(columns, local, pos, dup, terms, dof):
    rows, lanes = dup.shape[1], 2 * dof
    vectors = [v for i in range(2) for v in site_vector(local + i, pos, dup, terms, dof)]
    product = lax.dot_general(
        jnp.concatenate(vectors, axis=0),
        columns,
        (((1,), (0,)), ((), ())),
        preferred_element_type=F32,
    )
    product = product[:, :lanes] + product[:, lanes:]
    even = product[:rows] + product[rows : 2 * rows]
    odd = product[2 * rows : 3 * rows] + product[3 * rows :]
    return jnp.where(low_half(even.shape, dof), even, odd)


def apply_rows(stages, pos, dup, terms, dof, put):
    base = 0
    for stage in stages:
        for pair in range(stage.shape[0]):
            columns = stage[pair]
            put(base + pair, pair_product(columns, 2 * (base + pair), pos, dup, terms, dof))
        base += stage.shape[0]


def start_copies(sources, targets, sems):
    copies = [
        pltpu.make_async_copy(source, target, sems.at[index])
        for index, (source, target) in enumerate(zip(sources, targets))
    ]
    for copy in copies:
        copy.start()
    return copies


def over_pairs(blocks, step, init):
    spot = 0
    for block, chunks in enumerate(blocks):
        start = 0
        for chunk in chunks:

            def body(pair, carry, block=block, chunk=chunk, start=start, spot=spot):
                return step(block, chunk[pair], start + pair, spot + pair, carry)

            init = lax.fori_loop(0, chunk.shape[0], body, init, unroll=True)
            start += chunk.shape[0]
            spot += chunk.shape[0]
    return init


def in_blocks(refs, chunks):
    size = len(refs) // chunks
    return [[refs[chunk * size + block] for chunk in range(chunks)] for block in range(size)]


def share_out(chunks, values, shares):
    first = [(chunk, pair) for chunk in chunks for pair in range(chunk.shape[0])]
    for index, share in enumerate(shares):
        for inner in range(share.shape[1]):
            spot = index * share.shape[1] + inner
            chunk, pair = first[spot]
            share[0, inner] = chunk[pair]
            share[1, inner] = values[spot]


def first_kernel(n_field, count, dof, terms, pos, *rest):
    fields, ops, rest = rest[:n_field], rest[n_field : n_field + count], rest[n_field + count :]
    out, split, dup = rest[:3]
    held, sems = rest[3 : 3 + count], rest[3 + count]
    copies = start_copies(ops, held, sems)

    def build(block, value, pair, spot, carry):
        spread(dup, spot, value, dof)
        return carry

    over_pairs(in_blocks(fields, 1), build, 0)
    for copy in copies:
        copy.wait()

    def put(pair, values):
        out[pair] = values

    base = 0
    for op in held:
        for inner in range(op.shape[0]):
            columns = to_columns(*row_pairs(op, inner, dof))
            split[base] = columns
            put(base, pair_product(columns, 2 * base, pos, dup, terms, dof))
            base += 1


def more_kernel(base, dof, terms, links, dup, *rest):
    ops, (out, split, pos, sem) = rest[:-4], rest[-4:]
    copy = pltpu.make_async_copy(links, pos, sem)
    copy.start()
    done = 0
    for op in ops:
        for inner in range(op.shape[0]):
            split[done] = to_columns(*row_pairs(op, inner, dof))
            done += 1
    copy.wait()
    for pair in range(done):
        local = 2 * (base + pair)
        out[pair] = pair_product(split[pair], local, pos, dup, terms, dof)


def second_kernel(n_field, chunks, count, sends, dof, terms, links, *rest):
    rest, (pos, sem) = rest[:-2], rest[-2:]
    copy = pltpu.make_async_copy(links, pos, sem)
    copy.start()
    b_ref, rest = rest[:n_field], rest[n_field:]
    z_blocks, rest = in_blocks(rest[: chunks * n_field], chunks), rest[chunks * n_field :]
    stages, (out, basis, coeffs) = rest[:count], rest[count : count + 3]
    shares, dup = rest[count + 3 : count + 3 + sends], rest[count + 3 + sends]
    shape = b_ref[0].shape[1:]
    zero = jnp.zeros(shape, F32)

    def dots(block, z, pair, spot, carry):
        b = b_ref[block][pair]
        return carry[0] + b * b, carry[1] + b * z

    norm, cross = over_pairs(z_blocks, dots, (zero, zero))
    beta = jnp.sqrt(lane_sum(norm))
    scale = 1.0 / beta
    h00 = lane_sum(cross) * scale * scale

    def remove(block, z, pair, spot, carry):
        w = z * scale - (h00 * scale) * b_ref[block][pair]
        basis[spot] = w
        return carry + w * w

    h10 = jnp.sqrt(lane_sum(over_pairs(z_blocks, remove, zero)))
    unit = 1.0 / h10

    def build(block, w, pair, spot, carry):
        v = w * unit
        basis[spot] = v
        spread(dup, spot, v, dof)
        return carry

    over_pairs([[basis]], build, 0)
    coeffs[...] = place([beta, h00, h10], shape)

    def put(pair, values):
        out[pair] = values

    copy.wait()
    apply_rows(stages, pos, dup, terms, dof, put)
    share_out(z_blocks[0], out, shares)


def third_kernel(n_field, count, dof, terms, links, basis, coeffs, *rest):
    rest, (pos, sem) = rest[:-2], rest[-2:]
    copy = pltpu.make_async_copy(links, pos, sem)
    copy.start()
    b_ref, rest = rest[:n_field], rest[n_field:]
    z_blocks, rest = in_blocks(rest[:n_field], 1), rest[n_field:]
    stages, (sums, work, dup, image) = rest[:count], rest[count:]
    b_mine = b_ref[0]
    n_pair = b_mine.shape[0]
    shape = b_mine.shape[1:]
    zero = jnp.zeros(shape, F32)
    known = coeffs[...]
    scale = 1.0 / known[:, 0:1]

    def dots(block, z, pair, spot, carry):
        return carry[0] + b_ref[block][pair] * z, carry[1] + basis[spot] * z

    first, second = over_pairs(z_blocks, dots, (zero, zero))
    h01 = lane_sum(first) * scale
    h11 = lane_sum(second)

    def remove(block, z, pair, spot, carry):
        w = z - (h01 * scale) * b_ref[block][pair] - h11 * basis[spot]
        work[spot] = w
        return carry + w * w

    h21 = jnp.sqrt(lane_sum(over_pairs(z_blocks, remove, zero)))
    unit = 1.0 / h21

    def build(block, w, pair, spot, carry):
        v = w * unit
        work[spot] = v
        spread(dup, spot, v, dof)
        return carry

    over_pairs([[work]], build, 0)

    def put(pair, values):
        image[pair] = values

    copy.wait()
    apply_rows(stages, pos, dup, terms, dof, put)

    def last(pair, carry):
        u = image[pair]
        return (
            carry[0] + b_mine[pair] * u,
            carry[1] + basis[pair] * u,
            carry[2] + work[pair] * u,
            carry[3] + u * u,
        )

    parts = lax.fori_loop(0, n_pair, last, (zero, zero, zero, zero), unroll=True)
    solved = [known[:, 0:1], known[:, 1:2], known[:, 2:3], h01, h11, h21]
    columns = [lane_sum(part) for part in parts] + solved
    if len(sums.shape) == 3 and sums.shape[1:] == shape:
        packed = place(columns, shape)
    else:
        packed = dense_rows(columns, shape, sums.shape[1])
    for block in range(sums.shape[0]):
        sums[block] = packed


def weigh(values):
    d02, h12, h22, g22, beta, h00, h10, h01, h11, h21 = values
    scale = 1.0 / beta
    h02 = d02 * scale
    g00 = h00 * h00 + h10 * h10
    g01 = h00 * h01 + h10 * h11
    g02 = h00 * h02 + h10 * h12
    g11 = h01 * h01 + h11 * h11 + h21 * h21
    g12 = h01 * h02 + h11 * h12 + h21 * h22
    inv0 = 1.0 / g00
    l10 = g01 * inv0
    l20 = g02 * inv0
    d1 = g11 - l10 * g01
    e21 = g12 - l20 * g01
    inv1 = 1.0 / d1
    l21 = e21 * inv1
    d2 = g22 - l20 * g02 - l21 * e21
    r0 = beta * h00
    r1 = beta * h01 - l10 * r0
    r2 = beta * h02 - l20 * r0 - l21 * r1
    y2 = r2 / d2
    y1 = r1 * inv1 - l21 * y2
    y0 = r0 * inv0 - l10 * y1 - l20 * y2
    return scale, y0, y1, y2


def combine_kernel(sums, b_mine, v1_mine, v2_mine, out):
    total = sums[0]
    for block in range(1, sums.shape[0]):
        total = total + sums[block]
    known = sums[0]
    values = [(total if i < 4 else known)[:, i : i + 1] for i in range(10)]
    scale, y0, y1, y2 = weigh(values)
    for pair in range(b_mine.shape[0]):
        out[pair] = (y0 * scale) * b_mine[pair] + y1 * v1_mine[pair] + y2 * v2_mine[pair]


def finish_kernel(dof, info, turned, *rest):
    out, stack, factor = rest[-3:]
    n_sub, per_part, rhs, lanes = turned.shape
    shares = rest[:n_sub]
    per_row = lanes // rhs
    n_rows = info.shape[1]
    first = [info[quarter] for quarter in range(n_sub)]
    total = list(first)
    for block in range(1, info.shape[0] // n_sub):
        for quarter in range(n_sub):
            total[quarter] = total[quarter] + info[block * n_sub + quarter]
    known = [jnp.concatenate([f[r : r + 1] for f in first], axis=0) for r in range(n_rows)]
    added = [jnp.concatenate([t[r : r + 1] for t in total], axis=0) for r in range(n_rows)]
    values = []
    for index in range(10):
        source = (added if index < 4 else known)[index // per_row]
        shift = rhs * (index % per_row)
        values.append(pltpu.roll(source, lanes - shift, 1) if shift else source)
    scale, y0, y1, y2 = weigh(values)
    h00, h10, h01, h11, h21 = values[5:]
    gamma = y2 / h21
    both = (y1 - gamma * h11) / h10
    coeffs = [(y0 - both * h00 - gamma * h01) * scale, both * scale, gamma]
    flipped = jnp.concatenate(coeffs, axis=0)
    spare = -flipped.shape[0] % 8
    if spare:
        flipped = jnp.concatenate([flipped, jnp.zeros((spare, lanes), F32)], axis=0)
    flipped = flipped.T
    for index in range(3 * n_sub):
        factor[index] = jnp.broadcast_to(flipped[:rhs, index : index + 1], (rhs, lanes))
    for k in range(n_sub):
        quarter = lax.axis_index("sub") ^ k
        alpha, beta, gamma = (factor[part * n_sub + quarter] for part in range(3))
        start = pl.multiple_of(quarter * rhs, 8)
        for pair in range(per_part):
            mixed = alpha * turned[quarter, pair] + beta * shares[k][0, pair]
            stack[pair, pl.ds(start, rhs), :] = mixed + gamma * shares[k][1, pair]
    for pair in range(per_part):
        both = stack[pair].T
        out[2 * pair] = both[:dof]
        out[2 * pair + 1] = both[dof:]


def per_device(coarse_op, right_side, owner_map, neighbor_table):
    nz = lax.axis_size("z")
    n_sub = lax.axis_size("sub")
    per_dev, dof, width = coarse_op.shape
    terms = width // dof
    hops = terms - 1
    rhs = right_side.shape[2] // n_sub
    n_loc = n_sub * per_dev
    n_own = n_loc // 2
    me_z, me_c, me_s = lax.axis_index("z"), lax.axis_index("core"), lax.axis_index("sub")
    ids = jnp.stack([me_z, me_c, me_s]).astype(jnp.int32)
    even = per_dev % 2 == 0
    lanes = 2 * dof
    field = (n_own, rhs, lanes)

    relay = n_sub == 4 and per_dev % 4 == 0 and terms % 2 == 1
    order = jnp.arange(n_sub, dtype=jnp.int32) ^ me_s
    hops_to = [[(s, s ^ k) for s in range(n_sub)] for k in range(n_sub)]
    half = per_dev // 2
    if relay:
        halves = [jax.ShapeDtypeStruct((half // 2, dof, 2 * width), F32)] * 2
        parts = per_dev // 2
        op_low, op_high = pl.pallas_call(
            functools.partial(pack_kernel, dof),
            out_shape=halves,
            in_specs=[HBM],
            out_specs=[VMEM] * 2,
            scratch_shapes=[
                pltpu.VMEM((parts, 2, dof, width), F32),
                pltpu.SemaphoreType.DMA((parts,)),
            ],
            compiler_params=SMALL,
            name="pack",
        )(pltpu.with_memory_space_constraint(coarse_op, pltpu.HBM))
        turned, kept = pl.pallas_call(
            turn_right_kernel,
            out_shape=[jax.ShapeDtypeStruct((n_sub, half, rhs, lanes), F32)] * 2,
            in_specs=[VMEM],
            out_specs=[VMEM] * 2,
            compiler_params=SMALL,
            name="pack_right",
        )(right_side)
        x_high = lax.ppermute(op_high, "sub", hops_to[1])
        y_low = lax.ppermute(op_low, "sub", hops_to[2])
        x_low = lax.ppermute(op_low, "sub", hops_to[1])
        y_high = lax.ppermute(op_high, "sub", hops_to[2])

    positions = pl.pallas_call(
        functools.partial(position_kernel, (per_dev, n_sub, nz, hops)),
        out_shape=jax.ShapeDtypeStruct((n_loc * terms,), jnp.int32),
        in_specs=[SMEM, SMEM, SMEM],
        out_specs=SMEM,
        scratch_shapes=[pltpu.SMEM((owner_map.shape[0],), jnp.int32)],
        compiler_params=SMALL,
        name="positions",
    )(ids, owner_map, neighbor_table.reshape(-1))

    if not relay:
        turned = right_side.reshape(per_dev, dof, n_sub, rhs).transpose(2, 0, 3, 1)
    if even and not relay:
        turned = turned.reshape(n_sub, per_dev // 2, 2, rhs, dof).transpose(0, 1, 3, 2, 4)
        turned = turned.reshape(n_sub, per_dev // 2, rhs, lanes)
    if not relay:
        kept = turned
    mine = lax.all_to_all(turned, "sub", split_axis=0, concat_axis=0, tiled=True)
    mine = mine[order]
    if not even:
        mine = mine.reshape(n_own, 2, rhs, dof).transpose(0, 2, 1, 3)
    b_mine = mine.reshape(field)

    swap = [(c, c ^ 1) for c in range(CORES)]

    def step_z(own, offset):
        return lax.ppermute(own, "z", [(z, z ^ offset) for z in range(nz)])

    def gather(own):
        if nz == 4:
            cross = step_z(own, 2)
            near = step_z(own, 1)
            parts = [own, near, cross, step_z(cross, 1)]
        else:
            parts = [own] + [step_z(own, offset) for offset in range(1, nz)]
        for index in range(nz):
            parts.append(lax.ppermute(parts[index], "core", swap))
        return parts

    if relay:
        d_low = lax.ppermute(y_low, "sub", hops_to[1])
        d_high = lax.ppermute(x_high, "sub", hops_to[2])
        stages = [[op_low, op_high, x_low, x_high, y_low, y_high], [d_low, d_high]]
    if not relay:
        every = lax.all_gather(coarse_op, "sub", axis=0)[order]
        stages = [[every.reshape(n_own, 2 * dof, width)]]
    b_parts = gather(b_mine)
    n_field = len(b_parts)
    dup = (CORES * nz * n_loc, rhs, lanes)
    full = (CORES * nz * n_own,) + field[1:]
    small = jax.ShapeDtypeStruct(field[1:], F32)
    own_shape = jax.ShapeDtypeStruct(field, F32)
    sends = n_sub if even else 0
    share = [jax.ShapeDtypeStruct((2, per_dev // 2, rhs, lanes), F32)] * sends

    def split_shape(pairs):
        return jax.ShapeDtypeStruct((pairs, width, 4 * dof), BF16)

    ops = stages[0]
    done = sum(op.shape[0] for op in ops)
    z1, split, spread_b = pl.pallas_call(
        functools.partial(first_kernel, n_field, len(ops), dof, terms),
        out_shape=[
            jax.ShapeDtypeStruct((done,) + field[1:], F32),
            split_shape(done),
            jax.ShapeDtypeStruct(dup, F32),
        ],
        in_specs=[SMEM] + [VMEM] * n_field + [ANY] * len(ops),
        out_specs=[VMEM] * 3,
        scratch_shapes=[pltpu.VMEM(op.shape, F32) for op in ops]
        + [pltpu.SemaphoreType.DMA((len(ops),))],
        compiler_params=PARAMS,
        name="first",
    )(positions, *b_parts, *ops)
    splits, chunks = [split], 1
    z1_parts = gather(z1)
    if relay:
        ops, chunks = stages[1], 2
        late, split = pl.pallas_call(
            functools.partial(more_kernel, done, dof, terms),
            out_shape=[
                jax.ShapeDtypeStruct((n_own - done,) + field[1:], F32),
                split_shape(n_own - done),
            ],
            in_specs=[ANY, VMEM] + [VMEM] * len(ops),
            out_specs=[VMEM] * 2,
            scratch_shapes=[pltpu.SMEM(positions.shape, jnp.int32), pltpu.SemaphoreType.DMA],
            compiler_params=PARAMS,
            name="more",
        )(positions, spread_b, *ops)
        z1_parts = z1_parts + gather(late)
        splits.append(split)
    count = len(splits)
    links = [pltpu.SMEM(positions.shape, jnp.int32), pltpu.SemaphoreType.DMA]

    z2, basis, coeffs, *shares = pl.pallas_call(
        functools.partial(second_kernel, n_field, chunks, count, sends, dof, terms),
        out_shape=[own_shape, jax.ShapeDtypeStruct(full, F32), small] + share,
        in_specs=[ANY] + [VMEM] * ((1 + chunks) * n_field + count),
        out_specs=[VMEM] * (3 + sends),
        scratch_shapes=[pltpu.VMEM(dup, F32)] + links,
        compiler_params=PARAMS,
        name="second",
    )(positions, *b_parts, *z1_parts, *splits)
    z2_parts = gather(z2)
    shares[1:] = [lax.ppermute(shares[k], "sub", hops_to[k]) for k in range(1, sends)]
    z2_parts, shares = lax.optimization_barrier((z2_parts, shares))

    axes = ("z", "core", "sub") if even else ("z", "core")
    copies = nz * CORES * (n_sub if even else 1)
    note = (pl.cdiv(10 * rhs, lanes), lanes) if even else field[1:]
    keep = [] if even else [jax.ShapeDtypeStruct(full, F32)]
    sums, *work = pl.pallas_call(
        functools.partial(third_kernel, n_field, count, dof, terms),
        out_shape=[jax.ShapeDtypeStruct((copies,) + note, F32)] + keep,
        in_specs=[ANY] + [VMEM] * (2 + 2 * n_field + count),
        out_specs=[VMEM] * (1 + len(keep)),
        scratch_shapes=[pltpu.VMEM(full, F32)] * (1 - len(keep))
        + [pltpu.VMEM(dup, F32), pltpu.VMEM(field, F32)]
        + links,
        compiler_params=PARAMS,
        name="third",
    )(positions, basis, coeffs, *b_parts, *z2_parts, *splits)
    sums = lax.all_to_all(sums, axes, split_axis=0, concat_axis=0, tiled=True)

    if even:
        return pl.pallas_call(
            functools.partial(finish_kernel, dof),
            out_shape=jax.ShapeDtypeStruct(right_side.shape, F32),
            in_specs=[VMEM] * (2 + sends),
            out_specs=VMEM,
            scratch_shapes=[
                pltpu.VMEM((per_dev // 2, n_sub * rhs, lanes), F32),
                pltpu.VMEM((3 * n_sub, rhs, lanes), F32),
            ],
            compiler_params=SMALL,
            name="finish",
        )(sums, kept, *shares)
    result = pl.pallas_call(
        combine_kernel,
        out_shape=own_shape,
        in_specs=[VMEM] * 4,
        out_specs=VMEM,
        compiler_params=SMALL,
            name="combine",
    )(sums, b_mine, basis[:n_own], work[0][:n_own])
    result = result.reshape(n_own, rhs, 2, dof).transpose(0, 2, 1, 3)
    result = result.reshape(n_sub, per_dev, rhs, dof)[order]
    result = lax.all_to_all(result, "sub", split_axis=0, concat_axis=0, tiled=True)
    return result.transpose(1, 3, 0, 2).reshape(right_side.shape)


def solution(mesh):
    n_grp, n_sub = mesh.shape["grp"], mesh.shape["sub"]
    inner = Mesh(mesh.devices.reshape(n_grp // CORES, CORES, n_sub), ("z", "core", "sub"))
    split = P(("z", "core", "sub"), None, None)

    return jax.shard_map(
        per_device,
        mesh=inner,
        in_specs=(split, split, P(), P()),
        out_specs=split,
        check_vma=False,
    )
```

```python
import functools

import jax
import jax.numpy as jnp
from jax import lax
from jax.experimental import pallas as pl
from jax.experimental.pallas import tpu as pltpu
from jax.sharding import Mesh
from jax.sharding import PartitionSpec as P


F32 = jnp.float32
BF16 = jnp.bfloat16
CORES = 2
VMEM = pl.BlockSpec(memory_space=pltpu.VMEM)
SMEM = pl.BlockSpec(memory_space=pltpu.SMEM)
HBM = pl.BlockSpec(memory_space=pltpu.HBM)
ANY = pl.BlockSpec(memory_space=pl.ANY)
PARAMS = pltpu.CompilerParams(vmem_limit_bytes=20 * 1024 * 1024)
SMALL = pltpu.CompilerParams(vmem_limit_bytes=4 * 1024 * 1024)


def divide(value, size):
    if size & (size - 1):
        return lax.div(value, jnp.int32(size))
    return lax.shift_right_logical(value, jnp.int32(size.bit_length() - 1))


def remain(value, size):
    if size & (size - 1):
        return lax.rem(value, jnp.int32(size))
    return value & (size - 1)


def low_half(shape, dof):
    return lax.broadcasted_iota(jnp.int32, shape, 1) < dof


def lane_sum(values):
    return jnp.sum(values, axis=1, keepdims=True)


def split_bf16(values):
    high = values.astype(BF16)
    return high, (values - high.astype(F32)).astype(BF16)


def place(columns, shape):
    lane = lax.broadcasted_iota(jnp.int32, shape, 1)
    packed = jnp.zeros(shape, F32)
    for index, column in enumerate(columns):
        packed = jnp.where(lane == index, column, packed)
    return packed


def dense_rows(columns, shape, rows):
    size, lanes = shape
    per_row = lanes // size
    flipped = place(columns, shape).T
    lane = lax.broadcasted_iota(jnp.int32, (1, lanes), 1)
    wide = jnp.concatenate([flipped] * per_row, axis=1)
    packed = []
    for row in range(rows):
        line = jnp.zeros((1, lanes), F32)
        for inner in range(per_row):
            index = row * per_row + inner
            if index < len(columns):
                line = jnp.where(divide(lane, size) == inner, wide[index : index + 1], line)
        packed.append(line)
    return jnp.concatenate(packed, axis=0)


def position_kernel(geometry, ids, owner, table, out, where):
    per_dev, n_sub, nz, hops = geometry
    me_z, me_c, me_s = ids[0], ids[1], ids[2]
    sites = owner.shape[0]

    def locate(slot):
        dev = divide(slot, per_dev)
        grp = divide(dev, n_sub)
        block = (remain(grp, CORES) ^ me_c) * nz + (divide(grp, CORES) ^ me_z)
        return (block * n_sub + (remain(dev, n_sub) ^ me_s)) * per_dev + remain(slot, per_dev)

    def fill(slot, carry):
        where[owner[slot]] = locate(slot)
        return carry

    lax.fori_loop(0, sites, fill, 0, unroll=8)

    def look(local, carry):
        dev = (me_z * CORES + me_c) * n_sub + (divide(local, per_dev) ^ me_s)
        slot = dev * per_dev + remain(local, per_dev)
        base = owner[slot] * hops
        out[local * (hops + 1)] = locate(slot)
        for hop in range(hops):
            out[local * (hops + 1) + 1 + hop] = where[table[base + hop]]
        return carry

    lax.fori_loop(0, n_sub * per_dev, look, 0, unroll=2)


def pack_kernel(dof, op, low, high, held, sems):
    half = op.shape[0] // 2
    count = sems.shape[0]
    size = op.shape[0] // count
    sources = [op.at[pl.ds(size * index, size)] for index in range(count)]
    copies = start_copies(sources, [held.at[index] for index in range(count)], sems)
    main = op.shape[2] - dof
    for index in range(count):
        copies[index].wait()
        for inner in range(size // 2):
            even, odd = held[index, 2 * inner], held[index, 2 * inner + 1]
            pair = (size * index) // 2 + inner
            target, pair = (low, pair) if pair < half // 2 else (high, pair - half // 2)
            target[pair, :, :main] = even[:, :main]
            target[pair, :, main : 2 * main] = odd[:, :main]
            target[pair, :, 2 * main :] = jnp.concatenate([even[:, main:], odd[:, main:]], axis=1)


def turn_right_kernel(right, turned, kept):
    n_sub, per_part, rhs = turned.shape[0], turned.shape[1], turned.shape[2]
    for pair in range(per_part):
        both = jnp.concatenate([right[2 * pair], right[2 * pair + 1]], axis=0).T
        for quarter in range(n_sub):
            turned[quarter, pair] = both[quarter * rhs : (quarter + 1) * rhs]
            kept[quarter, pair] = both[quarter * rhs : (quarter + 1) * rhs]


def spread(dup, pair, values, dof):
    mask = low_half(values.shape, dof)
    rolled = pltpu.roll(values, dof, 1)
    dup[2 * pair] = jnp.where(mask, values, rolled)
    dup[2 * pair + 1] = jnp.where(mask, rolled, values)


def site_vector(local, pos, dup, terms, dof):
    mask = low_half((dup.shape[1], 2 * dof), dof)
    tiles = []
    for first in range(0, terms - 1, 2):
        left = dup[pos[local * terms + first]]
        right = dup[pos[local * terms + first + 1]]
        tiles.append(jnp.where(mask, left, right))
    if terms % 2:
        tiles.append(dup[pos[local * terms + terms - 1]][:, :dof])
    return list(split_bf16(jnp.concatenate(tiles, axis=1)))


def row_pairs(op, pair, dof):
    if op.shape[1] == 2 * dof:
        return op[pair, :dof], op[pair, dof:]
    main = op.shape[2] // 2 - dof
    rows = op[pair]
    tail = rows[:, 2 * main :]
    even = jnp.concatenate([rows[:, :main], tail[:, :dof]], axis=1)
    odd = jnp.concatenate([rows[:, main : 2 * main], tail[:, dof:]], axis=1)
    return even, odd


def to_columns(even, odd):
    width, lanes = even.shape[1], 2 * even.shape[0]
    pieces = []
    for start in range(0, width, lanes):
        stop = min(start + lanes, width)
        pieces.append(jnp.concatenate([even[:, start:stop], odd[:, start:stop]], axis=0).T)
    return jnp.concatenate(split_bf16(jnp.concatenate(pieces, axis=0)), axis=1)


def pair_product(columns, local, pos, dup, terms, dof):
    rows, lanes = dup.shape[1], 2 * dof
    vectors = [v for i in range(2) for v in site_vector(local + i, pos, dup, terms, dof)]
    product = lax.dot_general(
        jnp.concatenate(vectors, axis=0),
        columns,
        (((1,), (0,)), ((), ())),
        preferred_element_type=F32,
    )
    product = product[:, :lanes] + product[:, lanes:]
    even = product[:rows] + product[rows : 2 * rows]
    odd = product[2 * rows : 3 * rows] + product[3 * rows :]
    return jnp.where(low_half(even.shape, dof), even, odd)


def apply_rows(stages, pos, dup, terms, dof, put):
    base = 0
    for stage in stages:
        for pair in range(stage.shape[0]):
            columns = stage[pair]
            put(base + pair, pair_product(columns, 2 * (base + pair), pos, dup, terms, dof))
        base += stage.shape[0]


def start_copies(sources, targets, sems):
    copies = [
        pltpu.make_async_copy(source, target, sems.at[index])
        for index, (source, target) in enumerate(zip(sources, targets))
    ]
    for copy in copies:
        copy.start()
    return copies


def over_pairs(blocks, step, init):
    spot = 0
    for block, chunks in enumerate(blocks):
        start = 0
        for chunk in chunks:

            def body(pair, carry, block=block, chunk=chunk, start=start, spot=spot):
                return step(block, chunk[pair], start + pair, spot + pair, carry)

            init = lax.fori_loop(0, chunk.shape[0], body, init, unroll=True)
            start += chunk.shape[0]
            spot += chunk.shape[0]
    return init


def in_blocks(refs, chunks):
    size = len(refs) // chunks
    return [[refs[chunk * size + block] for chunk in range(chunks)] for block in range(size)]


def share_out(chunks, values, shares):
    first = [(chunk, pair) for chunk in chunks for pair in range(chunk.shape[0])]
    for index, share in enumerate(shares):
        for inner in range(share.shape[1]):
            spot = index * share.shape[1] + inner
            chunk, pair = first[spot]
            share[0, inner] = chunk[pair]
            share[1, inner] = values[spot]


def first_kernel(n_field, count, dof, terms, pos, *rest):
    fields, ops, rest = rest[:n_field], rest[n_field : n_field + count], rest[n_field + count :]
    out, split, dup = rest[:3]
    held = ops

    def build(block, value, pair, spot, carry):
        spread(dup, spot, value, dof)
        return carry

    over_pairs(in_blocks(fields, 1), build, 0)

    def put(pair, values):
        out[pair] = values

    base = 0
    for op in held:
        for inner in range(op.shape[0]):
            columns = to_columns(*row_pairs(op, inner, dof))
            split[base] = columns
            put(base, pair_product(columns, 2 * base, pos, dup, terms, dof))
            base += 1


def more_kernel(base, dof, terms, links, dup, *rest):
    ops, (out, split, pos, sem) = rest[:-4], rest[-4:]
    copy = pltpu.make_async_copy(links, pos, sem)
    copy.start()
    done = 0
    for op in ops:
        for inner in range(op.shape[0]):
            split[done] = to_columns(*row_pairs(op, inner, dof))
            done += 1
    copy.wait()
    for pair in range(done):
        local = 2 * (base + pair)
        out[pair] = pair_product(split[pair], local, pos, dup, terms, dof)


def second_kernel(n_field, chunks, count, sends, dof, terms, links, *rest):
    rest, (pos, sem) = rest[:-2], rest[-2:]
    copy = pltpu.make_async_copy(links, pos, sem)
    copy.start()
    b_ref, rest = rest[:n_field], rest[n_field:]
    z_blocks, rest = in_blocks(rest[: chunks * n_field], chunks), rest[chunks * n_field :]
    stages, (out, basis, coeffs) = rest[:count], rest[count : count + 3]
    shares, dup = rest[count + 3 : count + 3 + sends], rest[count + 3 + sends]
    shape = b_ref[0].shape[1:]
    zero = jnp.zeros(shape, F32)

    def dots(block, z, pair, spot, carry):
        b = b_ref[block][pair]
        return carry[0] + b * b, carry[1] + b * z

    norm, cross = over_pairs(z_blocks, dots, (zero, zero))
    beta = jnp.sqrt(lane_sum(norm))
    scale = 1.0 / beta
    h00 = lane_sum(cross) * scale * scale

    def remove(block, z, pair, spot, carry):
        w = z * scale - (h00 * scale) * b_ref[block][pair]
        basis[spot] = w
        return carry + w * w

    h10 = jnp.sqrt(lane_sum(over_pairs(z_blocks, remove, zero)))
    unit = 1.0 / h10

    def build(block, w, pair, spot, carry):
        v = w * unit
        basis[spot] = v
        spread(dup, spot, v, dof)
        return carry

    over_pairs([[basis]], build, 0)
    coeffs[...] = place([beta, h00, h10], shape)

    def put(pair, values):
        out[pair] = values

    copy.wait()
    apply_rows(stages, pos, dup, terms, dof, put)
    share_out(z_blocks[0], out, shares)


def third_kernel(n_field, count, dof, terms, links, basis, coeffs, *rest):
    rest, (pos, sem) = rest[:-2], rest[-2:]
    copy = pltpu.make_async_copy(links, pos, sem)
    copy.start()
    b_ref, rest = rest[:n_field], rest[n_field:]
    z_blocks, rest = in_blocks(rest[:n_field], 1), rest[n_field:]
    stages, (sums, work, dup, image) = rest[:count], rest[count:]
    b_mine = b_ref[0]
    n_pair = b_mine.shape[0]
    shape = b_mine.shape[1:]
    zero = jnp.zeros(shape, F32)
    known = coeffs[...]
    scale = 1.0 / known[:, 0:1]

    def dots(block, z, pair, spot, carry):
        return carry[0] + b_ref[block][pair] * z, carry[1] + basis[spot] * z

    first, second = over_pairs(z_blocks, dots, (zero, zero))
    h01 = lane_sum(first) * scale
    h11 = lane_sum(second)

    def remove(block, z, pair, spot, carry):
        w = z - (h01 * scale) * b_ref[block][pair] - h11 * basis[spot]
        work[spot] = w
        return carry + w * w

    h21 = jnp.sqrt(lane_sum(over_pairs(z_blocks, remove, zero)))
    unit = 1.0 / h21

    def build(block, w, pair, spot, carry):
        v = w * unit
        work[spot] = v
        spread(dup, spot, v, dof)
        return carry

    over_pairs([[work]], build, 0)

    def put(pair, values):
        image[pair] = values

    copy.wait()
    apply_rows(stages, pos, dup, terms, dof, put)

    def last(pair, carry):
        u = image[pair]
        return (
            carry[0] + b_mine[pair] * u,
            carry[1] + basis[pair] * u,
            carry[2] + work[pair] * u,
            carry[3] + u * u,
        )

    parts = lax.fori_loop(0, n_pair, last, (zero, zero, zero, zero), unroll=True)
    solved = [known[:, 0:1], known[:, 1:2], known[:, 2:3], h01, h11, h21]
    columns = [lane_sum(part) for part in parts] + solved
    if len(sums.shape) == 3 and sums.shape[1:] == shape:
        packed = place(columns, shape)
    else:
        packed = dense_rows(columns, shape, sums.shape[1])
    for block in range(sums.shape[0]):
        sums[block] = packed


def weigh(values):
    d02, h12, h22, g22, beta, h00, h10, h01, h11, h21 = values
    scale = 1.0 / beta
    h02 = d02 * scale
    g00 = h00 * h00 + h10 * h10
    g01 = h00 * h01 + h10 * h11
    g02 = h00 * h02 + h10 * h12
    g11 = h01 * h01 + h11 * h11 + h21 * h21
    g12 = h01 * h02 + h11 * h12 + h21 * h22
    inv0 = 1.0 / g00
    l10 = g01 * inv0
    l20 = g02 * inv0
    d1 = g11 - l10 * g01
    e21 = g12 - l20 * g01
    inv1 = 1.0 / d1
    l21 = e21 * inv1
    d2 = g22 - l20 * g02 - l21 * e21
    r0 = beta * h00
    r1 = beta * h01 - l10 * r0
    r2 = beta * h02 - l20 * r0 - l21 * r1
    y2 = r2 / d2
    y1 = r1 * inv1 - l21 * y2
    y0 = r0 * inv0 - l10 * y1 - l20 * y2
    return scale, y0, y1, y2


def combine_kernel(sums, b_mine, v1_mine, v2_mine, out):
    total = sums[0]
    for block in range(1, sums.shape[0]):
        total = total + sums[block]
    known = sums[0]
    values = [(total if i < 4 else known)[:, i : i + 1] for i in range(10)]
    scale, y0, y1, y2 = weigh(values)
    for pair in range(b_mine.shape[0]):
        out[pair] = (y0 * scale) * b_mine[pair] + y1 * v1_mine[pair] + y2 * v2_mine[pair]


def finish_kernel(dof, info, turned, *rest):
    out, stack, factor = rest[-3:]
    n_sub, per_part, rhs, lanes = turned.shape
    shares = rest[:n_sub]
    per_row = lanes // rhs
    n_rows = info.shape[1]
    first = [info[quarter] for quarter in range(n_sub)]
    total = list(first)
    for block in range(1, info.shape[0] // n_sub):
        for quarter in range(n_sub):
            total[quarter] = total[quarter] + info[block * n_sub + quarter]
    known = [jnp.concatenate([f[r : r + 1] for f in first], axis=0) for r in range(n_rows)]
    added = [jnp.concatenate([t[r : r + 1] for t in total], axis=0) for r in range(n_rows)]
    values = []
    for index in range(10):
        source = (added if index < 4 else known)[index // per_row]
        shift = rhs * (index % per_row)
        values.append(pltpu.roll(source, lanes - shift, 1) if shift else source)
    scale, y0, y1, y2 = weigh(values)
    h00, h10, h01, h11, h21 = values[5:]
    gamma = y2 / h21
    both = (y1 - gamma * h11) / h10
    coeffs = [(y0 - both * h00 - gamma * h01) * scale, both * scale, gamma]
    flipped = jnp.concatenate(coeffs, axis=0)
    spare = -flipped.shape[0] % 8
    if spare:
        flipped = jnp.concatenate([flipped, jnp.zeros((spare, lanes), F32)], axis=0)
    flipped = flipped.T
    for index in range(3 * n_sub):
        factor[index] = jnp.broadcast_to(flipped[:rhs, index : index + 1], (rhs, lanes))
    for k in range(n_sub):
        quarter = lax.axis_index("sub") ^ k
        alpha, beta, gamma = (factor[part * n_sub + quarter] for part in range(3))
        start = pl.multiple_of(quarter * rhs, 8)
        for pair in range(per_part):
            mixed = alpha * turned[quarter, pair] + beta * shares[k][0, pair]
            stack[pair, pl.ds(start, rhs), :] = mixed + gamma * shares[k][1, pair]
    for pair in range(per_part):
        both = stack[pair].T
        out[2 * pair] = both[:dof]
        out[2 * pair + 1] = both[dof:]


def per_device(coarse_op, right_side, owner_map, neighbor_table):
    nz = lax.axis_size("z")
    n_sub = lax.axis_size("sub")
    per_dev, dof, width = coarse_op.shape
    terms = width // dof
    hops = terms - 1
    rhs = right_side.shape[2] // n_sub
    n_loc = n_sub * per_dev
    n_own = n_loc // 2
    me_z, me_c, me_s = lax.axis_index("z"), lax.axis_index("core"), lax.axis_index("sub")
    ids = jnp.stack([me_z, me_c, me_s]).astype(jnp.int32)
    even = per_dev % 2 == 0
    lanes = 2 * dof
    field = (n_own, rhs, lanes)

    relay = n_sub == 4 and per_dev % 4 == 0 and terms % 2 == 1
    order = jnp.arange(n_sub, dtype=jnp.int32) ^ me_s
    hops_to = [[(s, s ^ k) for s in range(n_sub)] for k in range(n_sub)]
    half = per_dev // 2
    if relay:
        halves = [jax.ShapeDtypeStruct((half // 2, dof, 2 * width), F32)] * 2
        parts = per_dev // 2
        op_low, op_high = pl.pallas_call(
            functools.partial(pack_kernel, dof),
            out_shape=halves,
            in_specs=[HBM],
            out_specs=[VMEM] * 2,
            scratch_shapes=[
                pltpu.VMEM((parts, 2, dof, width), F32),
                pltpu.SemaphoreType.DMA((parts,)),
            ],
            compiler_params=SMALL,
            name="pack",
        )(pltpu.with_memory_space_constraint(coarse_op, pltpu.HBM))
        turned, kept = pl.pallas_call(
            turn_right_kernel,
            out_shape=[jax.ShapeDtypeStruct((n_sub, half, rhs, lanes), F32)] * 2,
            in_specs=[VMEM],
            out_specs=[VMEM] * 2,
            compiler_params=SMALL,
            name="pack_right",
        )(right_side)
        x_high = lax.ppermute(op_high, "sub", hops_to[1])
        y_low = lax.ppermute(op_low, "sub", hops_to[2])
        x_low = lax.ppermute(op_low, "sub", hops_to[1])
        y_high = lax.ppermute(op_high, "sub", hops_to[2])

    positions = pl.pallas_call(
        functools.partial(position_kernel, (per_dev, n_sub, nz, hops)),
        out_shape=jax.ShapeDtypeStruct((n_loc * terms,), jnp.int32),
        in_specs=[SMEM, SMEM, SMEM],
        out_specs=SMEM,
        scratch_shapes=[pltpu.SMEM((owner_map.shape[0],), jnp.int32)],
        compiler_params=SMALL,
        name="positions",
    )(ids, owner_map, neighbor_table.reshape(-1))

    if not relay:
        turned = right_side.reshape(per_dev, dof, n_sub, rhs).transpose(2, 0, 3, 1)
    if even and not relay:
        turned = turned.reshape(n_sub, per_dev // 2, 2, rhs, dof).transpose(0, 1, 3, 2, 4)
        turned = turned.reshape(n_sub, per_dev // 2, rhs, lanes)
    if not relay:
        kept = turned
    mine = lax.all_to_all(turned, "sub", split_axis=0, concat_axis=0, tiled=True)
    mine = mine[order]
    if not even:
        mine = mine.reshape(n_own, 2, rhs, dof).transpose(0, 2, 1, 3)
    b_mine = mine.reshape(field)

    swap = [(c, c ^ 1) for c in range(CORES)]

    def step_z(own, offset):
        return lax.ppermute(own, "z", [(z, z ^ offset) for z in range(nz)])

    def gather(own):
        if nz == 4:
            cross = step_z(own, 2)
            near = step_z(own, 1)
            parts = [own, near, cross, step_z(cross, 1)]
        else:
            parts = [own] + [step_z(own, offset) for offset in range(1, nz)]
        for index in range(nz):
            parts.append(lax.ppermute(parts[index], "core", swap))
        return parts

    if relay:
        d_low = lax.ppermute(y_low, "sub", hops_to[1])
        d_high = lax.ppermute(x_high, "sub", hops_to[2])
        stages = [[op_low, op_high, x_low, x_high, y_low, y_high], [d_low, d_high]]
    if not relay:
        every = lax.all_gather(coarse_op, "sub", axis=0)[order]
        stages = [[every.reshape(n_own, 2 * dof, width)]]
    b_parts = gather(b_mine)
    n_field = len(b_parts)
    dup = (CORES * nz * n_loc, rhs, lanes)
    full = (CORES * nz * n_own,) + field[1:]
    small = jax.ShapeDtypeStruct(field[1:], F32)
    own_shape = jax.ShapeDtypeStruct(field, F32)
    sends = n_sub if even else 0
    share = [jax.ShapeDtypeStruct((2, per_dev // 2, rhs, lanes), F32)] * sends

    def split_shape(pairs):
        return jax.ShapeDtypeStruct((pairs, width, 4 * dof), BF16)

    ops = stages[0]
    done = sum(op.shape[0] for op in ops)
    z1, split, spread_b = pl.pallas_call(
        functools.partial(first_kernel, n_field, len(ops), dof, terms),
        out_shape=[
            jax.ShapeDtypeStruct((done,) + field[1:], F32),
            split_shape(done),
            jax.ShapeDtypeStruct(dup, F32),
        ],
        in_specs=[SMEM] + [VMEM] * n_field + [VMEM] * len(ops),
        out_specs=[VMEM] * 3,
        compiler_params=PARAMS,
        name="first",
    )(positions, *b_parts, *ops)
    splits, chunks = [split], 1
    z1_parts = gather(z1)
    if relay:
        ops, chunks = stages[1], 2
        late, split = pl.pallas_call(
            functools.partial(more_kernel, done, dof, terms),
            out_shape=[
                jax.ShapeDtypeStruct((n_own - done,) + field[1:], F32),
                split_shape(n_own - done),
            ],
            in_specs=[ANY, VMEM] + [VMEM] * len(ops),
            out_specs=[VMEM] * 2,
            scratch_shapes=[pltpu.SMEM(positions.shape, jnp.int32), pltpu.SemaphoreType.DMA],
            compiler_params=PARAMS,
            name="more",
        )(positions, spread_b, *ops)
        z1_parts = z1_parts + gather(late)
        splits.append(split)
    count = len(splits)
    links = [pltpu.SMEM(positions.shape, jnp.int32), pltpu.SemaphoreType.DMA]

    z2, basis, coeffs, *shares = pl.pallas_call(
        functools.partial(second_kernel, n_field, chunks, count, sends, dof, terms),
        out_shape=[own_shape, jax.ShapeDtypeStruct(full, F32), small] + share,
        in_specs=[ANY] + [VMEM] * ((1 + chunks) * n_field + count),
        out_specs=[VMEM] * (3 + sends),
        scratch_shapes=[pltpu.VMEM(dup, F32)] + links,
        compiler_params=PARAMS,
        name="second",
    )(positions, *b_parts, *z1_parts, *splits)
    z2_parts = gather(z2)
    shares[1:] = [lax.ppermute(shares[k], "sub", hops_to[k]) for k in range(1, sends)]
    z2_parts, shares = lax.optimization_barrier((z2_parts, shares))

    axes = ("z", "core", "sub") if even else ("z", "core")
    copies = nz * CORES * (n_sub if even else 1)
    note = (pl.cdiv(10 * rhs, lanes), lanes) if even else field[1:]
    keep = [] if even else [jax.ShapeDtypeStruct(full, F32)]
    sums, *work = pl.pallas_call(
        functools.partial(third_kernel, n_field, count, dof, terms),
        out_shape=[jax.ShapeDtypeStruct((copies,) + note, F32)] + keep,
        in_specs=[ANY] + [VMEM] * (2 + 2 * n_field + count),
        out_specs=[VMEM] * (1 + len(keep)),
        scratch_shapes=[pltpu.VMEM(full, F32)] * (1 - len(keep))
        + [pltpu.VMEM(dup, F32), pltpu.VMEM(field, F32)]
        + links,
        compiler_params=PARAMS,
        name="third",
    )(positions, basis, coeffs, *b_parts, *z2_parts, *splits)
    sums = lax.all_to_all(sums, axes, split_axis=0, concat_axis=0, tiled=True)

    if even:
        return pl.pallas_call(
            functools.partial(finish_kernel, dof),
            out_shape=jax.ShapeDtypeStruct(right_side.shape, F32),
            in_specs=[VMEM] * (2 + sends),
            out_specs=VMEM,
            scratch_shapes=[
                pltpu.VMEM((per_dev // 2, n_sub * rhs, lanes), F32),
                pltpu.VMEM((3 * n_sub, rhs, lanes), F32),
            ],
            compiler_params=SMALL,
            name="finish",
        )(sums, kept, *shares)
    result = pl.pallas_call(
        combine_kernel,
        out_shape=own_shape,
        in_specs=[VMEM] * 4,
        out_specs=VMEM,
        compiler_params=SMALL,
            name="combine",
    )(sums, b_mine, basis[:n_own], work[0][:n_own])
    result = result.reshape(n_own, rhs, 2, dof).transpose(0, 2, 1, 3)
    result = result.reshape(n_sub, per_dev, rhs, dof)[order]
    result = lax.all_to_all(result, "sub", split_axis=0, concat_axis=0, tiled=True)
    return result.transpose(1, 3, 0, 2).reshape(right_side.shape)


def solution(mesh):
    n_grp, n_sub = mesh.shape["grp"], mesh.shape["sub"]
    inner = Mesh(mesh.devices.reshape(n_grp // CORES, CORES, n_sub), ("z", "core", "sub"))
    split = P(("z", "core", "sub"), None, None)

    return jax.shard_map(
        per_device,
        mesh=inner,
        in_specs=(split, split, P(), P()),
        out_specs=split,
        check_vma=False,
    )
```
